32 devices in a mesh: ctx: 4 (over z), fsdp: 8 (over y, x, core).
Axes of the slice: x: 2, y: 2, z: 4, core: 2. Of those that a mesh axis runs over, the one named last changes fastest.
Arguments:
- inputs: bfloat16 [8, 1024, 896], P('fsdp', 'ctx'), may hold values from -60 to 60
- positions: int32 [8, 1024], P('fsdp', 'ctx'), may hold values from 0 to 1023, as said below
- cotangent: bfloat16 [8, 1024, 896], P('fsdp', 'ctx'), may hold values from -6 to 6
- norm_one: bfloat16 [1, 896], P(None, 'fsdp'), may hold values from 0.5 to 1.5
- w_query: bfloat16 [1, 896, 896], P(None, 'fsdp'), may hold values from -0.1875 to 0.1875
- b_query: bfloat16 [1, 896], P(None, 'fsdp'), may hold values from -2 to 2
- key_projection: bfloat16 [1, 896, 128], P(None, 'fsdp'), may hold values from -0.1875 to 0.1875
- b_key: bfloat16 [1, 128], P(None, 'fsdp'), may hold values from -2 to 2
- value_projection: bfloat16 [1, 896, 128], P(None, 'fsdp'), may hold values from -0.1875 to 0.1875
- value_bias: bfloat16 [1, 128], P(None, 'fsdp'), may hold values from -3 to 3
- w_out: bfloat16 [1, 896, 896], P(None, 'fsdp'), may hold values from -0.75 to 0.75
- norm_two: bfloat16 [1, 896], P(None, 'fsdp'), may hold values from 0.5 to 1.5
- w_gate: bfloat16 [1, 896, 4864], P(None, 'fsdp'), may hold values from -0.1875 to 0.1875
- w_up: bfloat16 [1, 896, 4864], P(None, 'fsdp'), may hold values from -0.1875 to 0.1875
- w_down: bfloat16 [1, 4864, 896], P(None, 'fsdp'), may hold values from -0.078125 to 0.078125
Outputs:
- output: float32 [8, 1024, 896], P('fsdp', 'ctx')
- grad_inputs: float32 [8, 1024, 896], P('fsdp', 'ctx')
- grad_norm_one: float32 [1, 896], P(None, 'fsdp')
- grad_w_query: float32 [1, 896, 896], P(None, 'fsdp')
- grad_b_query: float32 [1, 896], P(None, 'fsdp')
- grad_w_key: float32 [1, 896, 128], P(None, 'fsdp')
- grad_b_key: float32 [1, 128], P(None, 'fsdp')
- grad_w_value: float32 [1, 896, 128], P(None, 'fsdp')
- grad_b_value: float32 [1, 128], P(None, 'fsdp')
- grad_w_out: float32 [1, 896, 896], P(None, 'fsdp')
- grad_norm_two: float32 [1, 896], P(None, 'fsdp')
- grad_w_gate: float32 [1, 896, 4864], P(None, 'fsdp')
- grad_w_up: float32 [1, 896, 4864], P(None, 'fsdp')
- grad_w_down: float32 [1, 4864, 896], P(None, 'fsdp')
The draws below stay inside these ranges and needn't reach their ends.
Inputs may be any that keep to these rules, and one draw needn't show every extreme that they name: In each sequence every position 0 to 1023 stands in exactly one slot; each aligned block of 256 slots (one device's) holds two whole blocks of 128 consecutive positions, rising within a block: block b and block 7 - b.
All inputs are finite; a program needn't handle non-finite values.
Results may differ from the reference program's by a relative error of at most 0.02.
Values may be sent and summed in bfloat16 or wider, within the bound.
A program may use at most 192 MiB of HBM per device.

```python
import math
import jax
import jax.numpy as jnp
from jax import lax

MODEL_WIDTH = 896
QUERY_HEADS = 14
KEY_VALUE_HEADS = 2
HEAD_SIZE = 64
FF = 4864
DECODER_LAYERS = 1
SEQ_LEN = 1024
TOK_DEV = 256
SEQS = 8


def draw_positions(key, part):
    pair_half = TOK_DEV // 2
    block_total = SEQ_LEN // TOK_DEV

    def one_sequence(seq_key):
        perm_key, flip_key = jax.random.split(seq_key)
        pair_index = jax.random.permutation(perm_key, block_total).astype(jnp.int32)
        flipped = jax.random.randint(flip_key, (block_total,), 0, 2)
        partner = 2 * block_total - 1 - pair_index
        leading = jnp.where(flipped == 1, partner, pair_index)
        trailing = jnp.where(flipped == 1, pair_index, partner)
        offsets = jnp.arange(pair_half, dtype=jnp.int32)
        slots = jnp.concatenate([leading[:, None] * pair_half + offsets[None, :], trailing[:, None] * pair_half + offsets[None, :]], axis=1)
        return slots.reshape(SEQ_LEN).astype(jnp.int32)
    return jax.vmap(one_sequence)(jax.random.split(key, SEQS)).astype(jnp.int32)


def draw_inputs(key, part):
    base_key, row_key, column_key = jax.random.split(key, 3)
    shape_all = (SEQS, SEQ_LEN, MODEL_WIDTH)
    base = jax.random.truncated_normal(base_key, -4.0, 4.0, shape_all, jnp.float32)
    row_scale = jnp.exp(jax.random.uniform(row_key, (SEQS, SEQ_LEN, 1), jnp.float32, math.log(0.3), math.log(3.0)))
    column_scale = jnp.exp(jax.random.uniform(column_key, (MODEL_WIDTH,), jnp.float32, math.log(0.3), math.log(3.0)))
    return (base * row_scale * column_scale).astype(jnp.bfloat16)


def draw_b_query(key, part):
    random_noise = jax.random.truncated_normal(jax.random.fold_in(key, 1), -4.0, 4.0, (DECODER_LAYERS, QUERY_HEADS * HEAD_SIZE), jnp.float32)
    return (0.5 * random_noise).astype(jnp.bfloat16)


def draw_b_key(key, part):
    random_noise = jax.random.truncated_normal(jax.random.fold_in(key, 3), -4.0, 4.0, (DECODER_LAYERS, KEY_VALUE_HEADS * HEAD_SIZE), jnp.float32)
    return (0.5 * random_noise).astype(jnp.bfloat16)


def shard_levels(key, dims, cuts, least, largest):
    def one(dim, shards_of):
        steps = jax.random.uniform(jax.random.fold_in(jax.random.fold_in(key, 6), dim), (shards_of,), jnp.float32, least / len(cuts), largest / len(cuts))
        return jnp.repeat(jnp.exp(steps), dims[dim] // shards_of).reshape((-1,) + (1,) * (len(dims) - dim - 1))

    loudness = one(*cuts[0])
    for cut in cuts[1:]:
        loudness = loudness * one(*cut)
    return loudness


def bell_draw(rng, shape, deviation, limit, shards=(), held_as=jnp.bfloat16):
    factor_of = shard_levels(rng, shape, shards, -0.22, 0.18) if shards else 1.0
    result = jax.random.normal(rng, shape, jnp.float32) * deviation * factor_of
    return jnp.minimum(jnp.maximum(result, -limit), limit).astype(held_as)


def setup_inputs(seed: int = 0) -> dict:
    splits = jax.random.split(jax.random.key(seed), 16)
    return {
        "inputs": draw_inputs(jax.random.fold_in(splits[15], 71), 0),
        "positions": draw_positions(jax.random.fold_in(splits[15], 71), 0),
        "cotangent": bell_draw(splits[2], (SEQS, SEQ_LEN, MODEL_WIDTH), 1.0, 6.0, ((0, 8), (1, 4))),
        "norm_one": jnp.clip(1.0 + 0.1 * jax.random.normal(splits[3], (DECODER_LAYERS, MODEL_WIDTH), jnp.float32), 0.5, 1.5).astype(jnp.bfloat16),
        "w_query": bell_draw(splits[4], (DECODER_LAYERS, MODEL_WIDTH, QUERY_HEADS * HEAD_SIZE), MODEL_WIDTH ** -0.5, 0.1875, ((1, 8),)),
        "b_query": draw_b_query(jax.random.fold_in(splits[15], 71), 0),
        "key_projection": bell_draw(splits[6], (DECODER_LAYERS, MODEL_WIDTH, KEY_VALUE_HEADS * HEAD_SIZE), MODEL_WIDTH ** -0.5, 0.1875, ((1, 8),)),
        "b_key": draw_b_key(jax.random.fold_in(splits[15], 71), 0),
        "value_projection": bell_draw(splits[8], (DECODER_LAYERS, MODEL_WIDTH, KEY_VALUE_HEADS * HEAD_SIZE), MODEL_WIDTH ** -0.5, 0.1875, ((1, 8),)),
        "value_bias": bell_draw(splits[9], (DECODER_LAYERS, KEY_VALUE_HEADS * HEAD_SIZE), 0.5, 3.0, ((1, 8),)),
        "w_out": bell_draw(splits[10], (DECODER_LAYERS, QUERY_HEADS * HEAD_SIZE, MODEL_WIDTH), HEAD_SIZE ** -0.5, 0.75, ((1, 8),)),
        "norm_two": jnp.clip(1.0 + 0.1 * jax.random.normal(splits[11], (DECODER_LAYERS, MODEL_WIDTH), jnp.float32), 0.5, 1.5).astype(jnp.bfloat16),
        "w_gate": bell_draw(splits[12], (DECODER_LAYERS, MODEL_WIDTH, FF), MODEL_WIDTH ** -0.5, 0.1875, ((1, 8),)),
        "w_up": bell_draw(splits[13], (DECODER_LAYERS, MODEL_WIDTH, FF), MODEL_WIDTH ** -0.5, 0.1875, ((1, 8),)),
        "w_down": bell_draw(splits[14], (DECODER_LAYERS, FF, MODEL_WIDTH), FF ** -0.5, 0.078125, ((1, 8),)),
    }


@jax.custom_vjp
def lower_limit(v):
    return lax.optimization_barrier(v.astype(jnp.bfloat16)).astype(jnp.float32)

@jax.custom_vjp
def low_back(v):
    return v

def low_keep(v):
    return (lower_limit(v), None)

def low_pass(kept, grad):
    return (grad,)

def back_keep(v):
    return (v, None)

def back_low(kept, grad):
    return (lower_limit(grad),)
lower_limit.defvjp(low_keep, low_pass)
low_back.defvjp(back_keep, back_low)
rope_base = 1000000.0
epsilon = 1e-06
negative = -1e+30

def product(left, right):
    return jnp.dot(left, right, precision=lax.Precision.HIGHEST, preferred_element_type=jnp.float32)

def angles(places, head_width):
    half_width = head_width // 2
    inverse = jnp.exp(jnp.arange(half_width, dtype=jnp.float32) * (-2.0 * math.log(rope_base) / head_width))
    turned = places.astype(jnp.float32)[:, None] * inverse[None, :]
    return (jnp.cos(turned)[:, None, :], jnp.sin(turned)[:, None, :])

def apply_rotation(value_entries, cosine_table, sine_table):
    half_width = value_entries.shape[-1] // 2
    first_half = value_entries[..., :half_width]
    second_half = value_entries[..., half_width:]
    return jnp.concatenate([first_half * cosine_table - second_half * sine_table, second_half * cosine_table + first_half * sine_table], axis=-1)

def normalize(hidden, gain):
    return lower_limit(hidden * lax.rsqrt(lax.optimization_barrier(jnp.mean(hidden * hidden, axis=-1, keepdims=True)) + epsilon) * gain)

def layer_apply(hidden, places, params):
    gain_one, w_query, b_query, key_projection, b_key, value_projection, value_bias, w_out, gain_two, w_gate, w_up, w_down = params
    total_length = hidden.shape[0]
    heads_per_group = QUERY_HEADS // KEY_VALUE_HEADS
    score_scale = 1.0 / math.sqrt(HEAD_SIZE)
    cosine_table, sine_table = angles(places, HEAD_SIZE)
    normed = normalize(hidden, gain_one)
    query_rows = low_back(product(normed, w_query) + b_query)
    key_row_slice = low_back(product(normed, key_projection) + b_key)
    value_row_slice = low_back(product(normed, value_projection) + value_bias)
    query_rows = lower_limit(apply_rotation(query_rows.reshape(total_length, QUERY_HEADS, HEAD_SIZE), cosine_table, sine_table)).reshape(total_length, KEY_VALUE_HEADS, heads_per_group, HEAD_SIZE)
    key_row_slice = lower_limit(apply_rotation(key_row_slice.reshape(total_length, KEY_VALUE_HEADS, HEAD_SIZE), cosine_table, sine_table))
    value_row_slice = lower_limit(value_row_slice.reshape(total_length, KEY_VALUE_HEADS, HEAD_SIZE))
    raw_scores = low_back(jnp.einsum('tgjd,ugd->gjtu', query_rows, key_row_slice, precision=lax.Precision.HIGHEST) * score_scale)
    allowed = places[None, :] <= places[:, None]
    raw_scores = jnp.where(allowed, raw_scores, negative)
    top_score = lax.optimization_barrier(jnp.max(raw_scores, axis=-1, keepdims=True))
    log_total = top_score + jnp.log(lax.optimization_barrier(jnp.sum(jnp.exp(raw_scores - top_score), axis=-1, keepdims=True)))
    attn_probs = lower_limit(jnp.exp(raw_scores - log_total))
    mixture = jnp.einsum('gjtu,ugd->tgjd', attn_probs, value_row_slice, precision=lax.Precision.HIGHEST)
    mixture = lower_limit(low_back(mixture.reshape(total_length, QUERY_HEADS * HEAD_SIZE)))
    middle = hidden + low_back(product(mixture, w_out))
    normed_two = normalize(middle, gain_two)
    gate_act = low_back(product(normed_two, w_gate))
    up_act = low_back(product(normed_two, w_up))
    inner_act = lower_limit(jax.nn.silu(gate_act) * up_act)
    return middle + low_back(product(inner_act, w_down))

def reference(inputs, positions, cotangent, norm_one, w_query, b_query, key_projection, b_key, value_projection, value_bias, w_out, norm_two, w_gate, w_up, w_down):
    params = tuple((weight.astype(jnp.float32) for weight in (norm_one, w_query, b_query, key_projection, b_key, value_projection, value_bias, w_out, norm_two, w_gate, w_up, w_down)))
    start = inputs.astype(jnp.float32)

    def forward(start_rows, weights):

        def one_sequence(pair):
            hidden, places = pair
            for layer_index in range(DECODER_LAYERS):
                hidden = layer_apply(hidden, places, tuple((weight[layer_index] for weight in weights)))
            return hidden
        return lax.map(jax.checkpoint(one_sequence), (start_rows, positions))
    output, pullback = jax.vjp(forward, start, params)
    grad_start, grad_params = pullback(cotangent.astype(jnp.float32))
    return (output, grad_start, grad_params[0], grad_params[1], grad_params[2], grad_params[3], grad_params[4], grad_params[5], grad_params[6], grad_params[7], grad_params[8], grad_params[9], grad_params[10], grad_params[11])
```

```python
import math

import jax
import jax.numpy as jnp
from jax import lax
from jax.sharding import PartitionSpec as P

QUERY_HEADS = 14
KEY_VALUE_HEADS = 2
HEAD_SIZE = 64
ROPE_BASE = 1000000.0
EPSILON = 1e-06
NEGATIVE = -1e30
BF = jnp.bfloat16
F32 = jnp.float32


def angles(places):
    half = HEAD_SIZE // 2
    inverse = jnp.exp(jnp.arange(half, dtype=F32) * (-2.0 * math.log(ROPE_BASE) / HEAD_SIZE))
    turned = places.astype(F32)[:, None] * inverse[None, :]
    return jnp.cos(turned)[:, None, :], jnp.sin(turned)[:, None, :]


def rotate(u, cosine, sine):
    half = u.shape[-1] // 2
    a, b = u[..., :half], u[..., half:]
    return jnp.concatenate([a * cosine - b * sine, b * cosine + a * sine], axis=-1)


def norm_rows(hidden, gain):
    scale = lax.rsqrt(jnp.mean(hidden * hidden, axis=-1, keepdims=True) + EPSILON)
    return scale, (hidden * scale * gain).astype(BF)


def norm_back(hidden, scale, gain, grad):
    weighted = gain * grad
    grad_gain = jnp.sum(grad * hidden * scale, axis=0)
    inner = jnp.mean(weighted * hidden, axis=-1, keepdims=True)
    return grad_gain, scale * weighted - hidden * (scale * scale * scale) * inner


def dot(a, b):
    return jnp.dot(a, b, preferred_element_type=F32)


def dot_t(a, b):
    return lax.dot_general(a, b, (((1,), (1,)), ((), ())), preferred_element_type=F32)


def t_dot(a, b):
    return lax.dot_general(a, b, (((0,), (0,)), ((), ())), preferred_element_type=F32)


def shards(
    inputs, positions, cotangent, norm_one, w_query, b_query, key_projection, b_key,
    value_projection, value_bias, w_out, norm_two, w_gate, w_up, w_down,
):
    rows = inputs.shape[1]
    width = inputs.shape[2]
    group = QUERY_HEADS // KEY_VALUE_HEADS
    q_cols = w_query.shape[2]
    kv_cols = key_projection.shape[2]
    score_scale = 1.0 / math.sqrt(HEAD_SIZE)

    places = positions[0]
    key_places = lax.all_gather(places, "ctx", axis=0, tiled=True)
    cosine, sine = angles(places)
    hidden = inputs[0].astype(F32)

    packed = jnp.concatenate([w_query[0], key_projection[0], value_projection[0], w_out[0]], axis=1)
    packed = lax.all_gather(packed, "fsdp", axis=0, tiled=True)
    w_qkv = packed[:, : q_cols + 2 * kv_cols]
    w_o = packed[:, q_cols + 2 * kv_cols :]
    small = jnp.concatenate([norm_one[0], b_query[0], b_key[0], value_bias[0], norm_two[0]])
    small = lax.all_gather(small, "fsdp", axis=0).astype(F32)
    cuts, at = [], 0
    for piece in (norm_one, b_query, b_key, value_bias, norm_two):
        n = piece.shape[1]
        cuts.append(small[:, at : at + n].reshape(-1))
        at += n
    gain_one, bias_q, bias_k, bias_v, gain_two = cuts
    bias = jnp.concatenate([bias_q, bias_k, bias_v])

    grad_branch = cotangent[0]
    df_all = lax.all_gather(grad_branch, "fsdp", axis=0, tiled=True)
    wg = lax.all_to_all(w_gate[0], "fsdp", split_axis=1, concat_axis=0, tiled=True)
    wu = lax.all_to_all(w_up[0], "fsdp", split_axis=1, concat_axis=0, tiled=True)
    wd = w_down[0]

    scale_one, normed = norm_rows(hidden, gain_one)
    qkv = dot(normed, w_qkv) + bias
    q = rotate(qkv[:, :q_cols].reshape(rows, QUERY_HEADS, HEAD_SIZE), cosine, sine).astype(BF)
    k = rotate(
        qkv[:, q_cols : q_cols + kv_cols].reshape(rows, KEY_VALUE_HEADS, HEAD_SIZE), cosine, sine
    ).astype(BF)
    v = qkv[:, q_cols + kv_cols :].astype(BF)
    kv = jnp.concatenate([k.reshape(rows, kv_cols), v], axis=1)
    kv = lax.all_gather(kv, "ctx", axis=0, tiled=True)
    total = kv.shape[0]
    k_all = kv[:, :kv_cols].reshape(total, KEY_VALUE_HEADS, HEAD_SIZE)
    v_all = kv[:, kv_cols:].reshape(total, KEY_VALUE_HEADS, HEAD_SIZE)
    q = q.reshape(rows, KEY_VALUE_HEADS, group, HEAD_SIZE)
    s = jnp.einsum("tgjd,ugd->gjtu", q, k_all, preferred_element_type=F32) * score_scale
    s = jnp.where(key_places[None, :] <= places[:, None], s, NEGATIVE)
    top = jnp.max(s, axis=-1, keepdims=True)
    lse = top + jnp.log(jnp.sum(jnp.exp(s - top), axis=-1, keepdims=True))
    pf = jnp.exp(s - lse)
    p = pf.astype(BF)
    o = jnp.einsum("gjtu,ugd->tgjd", p, v_all, preferred_element_type=F32)
    ob = o.reshape(rows, q_cols).astype(BF)
    middle = hidden + dot(ob, w_o)
    scale_two, normed_two = norm_rows(middle, gain_two)

    x_all = lax.all_gather(normed_two, "fsdp", axis=0, tiled=True)
    gate = dot(x_all, wg)
    up = dot(x_all, wu)
    sig = jax.nn.sigmoid(gate)
    hid = (gate * sig * up).astype(BF)
    out_part = dot(hid, wd).astype(BF)
    ffn_out = lax.psum_scatter(out_part, "fsdp", scatter_dimension=0, tiled=True)
    output = middle + ffn_out.astype(F32)

    dhid = dot_t(df_all, wd)
    dgate = (dhid * up * sig * (1.0 + gate * (1.0 - sig))).astype(BF)
    dup = (dhid * (gate * sig)).astype(BF)
    dx_part = (dot_t(dgate, wg) + dot_t(dup, wu)).astype(BF)
    dxn2 = lax.psum_scatter(dx_part, "fsdp", scatter_dimension=0, tiled=True).astype(F32)
    g_down = t_dot(hid, df_all)
    g_gate = t_dot(x_all, dgate)
    g_up = t_dot(x_all, dup)

    g_out = grad_branch.astype(F32)
    grad_gain_two, dmid = norm_back(middle, scale_two, gain_two, dxn2)
    dm = g_out + dmid
    da = dm.astype(BF)
    g_wo = t_dot(ob, da)
    dob = dot_t(da, w_o).astype(BF).reshape(rows, KEY_VALUE_HEADS, group, HEAD_SIZE)

    dp = jnp.einsum("tgjd,ugd->gjtu", dob, v_all, preferred_element_type=F32)
    delta = jnp.sum(pf * dp, axis=-1, keepdims=True)
    ds = (pf * (dp - delta)).astype(BF)
    dq = jnp.einsum("gjtu,ugd->tgjd", ds, k_all, preferred_element_type=F32) * score_scale
    dk = jnp.einsum("gjtu,tgjd->ugd", ds, q, preferred_element_type=F32) * score_scale
    dv = jnp.einsum("gjtu,tgjd->ugd", p, dob, preferred_element_type=F32)
    dkv = jnp.concatenate([dk.reshape(total, kv_cols), dv.reshape(total, kv_cols)], axis=1)
    dkv = lax.psum_scatter(dkv, "ctx", scatter_dimension=0, tiled=True)
    dq = rotate(dq.reshape(rows, QUERY_HEADS, HEAD_SIZE), cosine, -sine).astype(BF)
    dk = rotate(
        dkv[:, :kv_cols].reshape(rows, KEY_VALUE_HEADS, HEAD_SIZE), cosine, -sine
    ).astype(BF)
    dqkv = jnp.concatenate(
        [dq.reshape(rows, q_cols), dk.reshape(rows, kv_cols), dkv[:, kv_cols:].astype(BF)], axis=1
    )
    g_qkv = t_dot(normed, dqkv)
    g_bias = jnp.sum(dqkv.astype(F32), axis=0)
    dxn = dot_t(dqkv, w_qkv)
    grad_gain_one, dhidden = norm_back(hidden, scale_one, gain_one, dxn)
    grad_in = dm + dhidden

    g_attn = jnp.concatenate([g_qkv, g_wo], axis=1).astype(BF)
    g_attn = lax.psum_scatter(g_attn, "fsdp", scatter_dimension=0, tiled=True)
    back = [
        lax.all_to_all(g.astype(BF), "fsdp", split_axis=0, concat_axis=1, tiled=True)
        for g in (g_gate, g_up)
    ]
    g_attn, g_gate, g_up, g_down = lax.psum((g_attn, back[0], back[1], g_down.astype(BF)), "ctx")
    pieces = jnp.concatenate(
        [
            g.reshape(small.shape[0], -1)
            for g in (
                grad_gain_one, g_bias[:q_cols], g_bias[q_cols : q_cols + kv_cols],
                g_bias[q_cols + kv_cols :], grad_gain_two,
            )
        ],
        axis=1,
    )
    pieces = lax.psum(pieces, ("ctx", "fsdp"))
    mine = lax.dynamic_slice_in_dim(pieces, lax.axis_index("fsdp"), 1, axis=0)
    outs, at = [], 0
    for piece in (norm_one, b_query, b_key, value_bias, norm_two):
        n = piece.shape[1]
        outs.append(mine[:, at : at + n])
        at += n
    g_n1, g_bq, g_bk, g_bv, g_n2 = outs
    g_attn = g_attn.astype(F32)
    return (
        output[None], grad_in[None], g_n1,
        g_attn[None, :, :q_cols], g_bq,
        g_attn[None, :, q_cols : q_cols + kv_cols], g_bk,
        g_attn[None, :, q_cols + kv_cols : q_cols + 2 * kv_cols], g_bv,
        g_attn[None, :, q_cols + 2 * kv_cols :], g_n2,
        g_gate.astype(F32)[None], g_up.astype(F32)[None], g_down.astype(F32)[None],
    )


def solution(mesh):
    tok, row, vec = P("fsdp", "ctx", None), P(None, "fsdp", None), P(None, "fsdp")
    return jax.shard_map(
        shards,
        mesh=mesh,
        in_specs=(
            tok, P("fsdp", "ctx"), tok, vec, row, vec, row, vec, row, vec, row, vec, row, row, row,
        ),
        out_specs=(tok, tok, vec, row, vec, row, vec, row, vec, row, vec, row, row, row),
        check_vma=False,
    )
```

```python
import functools
import math

import jax
import jax.numpy as jnp
from jax import lax
from jax.experimental import pallas as pl
from jax.experimental.pallas import tpu as pltpu
from jax.sharding import PartitionSpec as P

QUERY_HEADS = 14
KEY_VALUE_HEADS = 2
HEAD_SIZE = 64
ROPE_BASE = 1000000.0
EPSILON = 1e-06
NEGATIVE = -1e30
BF = jnp.bfloat16
F32 = jnp.float32
MESH = pl.DeviceIdType.MESH


def angles(places):
    half = HEAD_SIZE // 2
    inverse = jnp.exp(jnp.arange(half, dtype=F32) * (-2.0 * math.log(ROPE_BASE) / HEAD_SIZE))
    turned = places.astype(F32)[:, None] * inverse[None, :]
    return jnp.cos(turned)[:, None, :], jnp.sin(turned)[:, None, :]


def rotate(u, cosine, sine):
    half = u.shape[-1] // 2
    a, b = u[..., :half], u[..., half:]
    return jnp.concatenate([a * cosine - b * sine, b * cosine + a * sine], axis=-1)


def norm_rows(hidden, gain):
    scale = lax.rsqrt(jnp.mean(hidden * hidden, axis=-1, keepdims=True) + EPSILON)
    return scale, (hidden * scale * gain).astype(BF)


def norm_back(hidden, scale, gain, grad):
    weighted = gain * grad
    grad_gain = jnp.sum(grad * hidden * scale, axis=0)
    inner = jnp.mean(weighted * hidden, axis=-1, keepdims=True)
    return grad_gain, scale * weighted - hidden * (scale * scale * scale) * inner


def dot(a, b):
    return jnp.dot(a, b, preferred_element_type=F32)


def dot_t(a, b):
    return lax.dot_general(a, b, (((1,), (1,)), ((), ())), preferred_element_type=F32)


def t_dot(a, b):
    return lax.dot_general(a, b, (((0,), (0,)), ((), ())), preferred_element_type=F32)


def plane():
    f = lax.axis_index("fsdp")
    core, x, y = f % 2, (f // 2) % 2, f // 4
    by_x, by_y = f + 2 - 4 * x, f + 4 - 8 * y
    twin = f + 1 - 2 * core
    near = by_x + core * (by_y - by_x)
    far = by_y + core * (by_x - by_y)
    return twin, near, far, 2 + 2 * core, 4 - 2 * core


def tiles(rows, step, body):
    count = rows // step
    unroll = count if count <= 10 else 4

    @pl.loop(0, count, unroll=unroll)
    def _(r):
        body(pl.ds(pl.multiple_of(r * step, step), step))


def peer(r):
    f = lax.axis_index("fsdp")
    core, x, y = f % 2, (f // 2) % 2, f // 4
    return f + (r % 2) * (1 - 2 * core) + ((r // 2) % 2) * (2 - 4 * x) + (r // 4) * (4 - 8 * y)


def greet(others):
    barrier = pltpu.get_barrier_semaphore()
    for other in others:
        pl.semaphore_signal(barrier, inc=1, device_id=other, device_id_type=MESH)
    pl.semaphore_wait(barrier, len(others))


def push(src, dst, send, recv, other):
    return pltpu.make_async_remote_copy(
        src_ref=src, dst_ref=dst, send_sem=send, recv_sem=recv, device_id=other, device_id_type=MESH
    )


class Gather:
    def __init__(self, place, mine, full, send, recv, by_owner=False):
        self.twin, self.near, self.far, self.s_near, self.s_far = place
        self.mine, self.full, self.send, self.recv = mine, full, send, recv
        self.by_owner = by_owner

    def copy(self, i):
        twin, near, far = self.twin, self.near, self.far
        here = (0, 0, 0, self.s_near, 2, 4, 6)[i]
        there, other = (
            (self.s_near, near), (self.s_far, far), (1, twin), (6, far), (3, twin), (5, twin), (7, twin)
        )[i]
        if self.by_owner:
            here = there = peer(here)
        src = self.mine if i < 3 else self.full.at[here]
        return push(src, self.full.at[there], self.send.at[i], self.recv.at[there], {"fsdp": other})

    def start(self):
        for i in range(3):
            self.copy(i).start()

    def wait(self, slot):
        slot = peer(slot) if self.by_owner else slot
        full = self.full.at[slot]
        push(full, full, self.send.at[0], self.recv.at[slot], {"fsdp": self.near}).wait_recv()

    def relay(self):
        self.wait(2)
        self.wait(4)
        for i in range(3, 6):
            self.copy(i).start()

    def relay_corner(self):
        self.wait(6)
        self.copy(6).start()

    def finish(self):
        for i in range(7):
            self.copy(i).wait_send()


class Scatter:
    def __init__(
        self, place, part, core_in, tree_in, folded, send_core, recv_core, send_tree, recv_tree,
        by_owner=False,
    ):
        self.twin, self.near, self.far, self.s_near, self.s_far = place
        self.at = peer if by_owner else lambda slot: slot
        self.part, self.core_in, self.tree_in, self.folded = part, core_in, tree_in, folded
        self.send_core, self.recv_core = send_core, recv_core
        self.send_tree, self.recv_tree = send_tree, recv_tree

    def to_twin(self, k):
        return push(
            self.part.at[self.at(2 * k + 1)], self.core_in.at[k], self.send_core.at[k], self.recv_core.at[k],
            {"fsdp": self.twin},
        )

    def tree(self, j):
        other = (self.far, self.near, self.far)[j]
        return push(
            self.folded.at[j], self.tree_in.at[j], self.send_tree.at[j], self.recv_tree.at[j],
            {"fsdp": other},
        )

    def fold(self, j, slot, corner=False):
        part, core_in, tree_in, folded = self.part, self.core_in, self.tree_in, self.folded
        k = slot // 2
        slot = self.at(slot)

        def add(at):
            value = part[slot, at, :].astype(F32) + core_in[k, at, :].astype(F32)
            if corner:
                value = value + tree_in[0, at, :].astype(F32)
            folded[j, at, :] = value.astype(BF)

        tiles(part.shape[1], 16, add)

    def start_corner(self):
        self.to_twin(3).wait_recv()
        self.fold(0, 6)
        self.tree(0).start()

    def start_far(self):
        self.to_twin(1).wait_recv()
        self.to_twin(2).wait_recv()
        self.fold(2, self.s_far)
        self.tree(2).start()

    def start(self):
        self.start_corner()
        self.start_far()

    def relay(self):
        self.tree(0).wait_recv()
        self.fold(1, self.s_near, True)
        self.tree(1).start()

    def total(self, store):
        part, core_in, tree_in = self.part, self.core_in, self.tree_in
        mine = self.at(0)
        self.to_twin(0).wait_recv()
        self.tree(1).wait_recv()
        self.tree(2).wait_recv()

        def add(at):
            value = part[mine, at, :].astype(F32) + core_in[0, at, :].astype(F32)
            store(at, value + tree_in[1, at, :].astype(F32) + tree_in[2, at, :].astype(F32))

        tiles(part.shape[1], 16, add)

    def finish(self):
        for k in range(4):
            self.to_twin(k).wait_send()
        for j in range(3):
            self.tree(j).wait_send()


def line():
    z = lax.axis_index("ctx")
    inner = (z == 1) | (z == 2)
    return z, inner, z + 1 - 2 * (z // 3), 3 * (z // 2), 3 - z


class Line:
    def __init__(self, own, pair, mate, sems, first=0):
        self.own, self.pair, self.mate = own, pair, mate
        self.sems, self.first = sems, first
        self.z, self.inner, self.to_inner, self.to_outer, self.to_mate = line()

    def _copy(self, k, p):
        src, dst, other = (
            (self.own, self.pair, self.to_inner),
            (self.pair, self.mate, self.to_mate),
            (self.pair, self.pair, self.to_outer),
        )[k]
        i = self.first + p
        return push(src.at[p], dst.at[p], self.sems[2 * k].at[i], self.sems[2 * k + 1].at[i], {"ctx": other})

    def _rows(self, body):
        tiles(self.own.shape[1], 16, body)

    def start(self, p):
        @pl.when(~self.inner)
        def _():
            self._copy(0, p).start()

    def meet(self, p):
        own, pair = self.own, self.pair

        @pl.when(self.inner)
        def _():
            self._copy(0, p).wait_recv()

            def add(at):
                pair[p, at, :] = (pair[p, at, :].astype(F32) + own[p, at, :].astype(F32)).astype(BF)

            self._rows(add)
            self._copy(1, p).start()

    def settle(self, p):
        pair, mate = self.pair, self.mate

        @pl.when(self.inner)
        def _():
            self._copy(1, p).wait_recv()
            self._copy(1, p).wait_send()

            def add(at):
                pair[p, at, :] = (pair[p, at, :].astype(F32) + mate[p, at, :].astype(F32)).astype(BF)

            self._rows(add)
            self._copy(2, p).start()

        @pl.when(~self.inner)
        def _():
            self._copy(2, p).wait_recv()

    def finish(self, p):
        @pl.when(self.inner)
        def _():
            self._copy(2, p).wait_send()

        @pl.when(~self.inner)
        def _():
            self._copy(0, p).wait_send()


def greet_all():
    z = lax.axis_index("ctx")
    barrier = pltpu.get_barrier_semaphore()
    for r in range(1, 8):
        pl.semaphore_signal(barrier, inc=1, device_id={"fsdp": peer(r)}, device_id_type=MESH)

    for d in range(1, 4):
        pl.semaphore_signal(barrier, inc=1, device_id={"ctx": (z + d) % 4}, device_id_type=MESH)
    pl.semaphore_wait(barrier, 10)


class LineGather:
    def __init__(self, full, send_up, send_down, recv):
        self.full, self.send_up, self.send_down, self.recv = full, send_up, send_down, recv
        self.z = lax.axis_index("ctx")

    def _copy(self, slot, up):
        send = (self.send_up if up else self.send_down).at[slot]
        full = self.full.at[slot]
        return push(full, full, send, self.recv.at[slot], {"ctx": self.z + 1 if up else self.z - 1})

    def _hand_up(self, slot):
        @pl.when(self.z < 3)
        def _():
            self._copy(slot, True).start()

    def _hand_down(self, slot):
        @pl.when(self.z > 0)
        def _():
            self._copy(slot, False).start()

    def start(self):
        self._hand_up(self.z)
        self._hand_down(self.z)

    def collect(self, d):
        @pl.when(self.z >= d)
        def _():
            self._copy(self.z - d, True).wait_recv()
            self._hand_up(self.z - d)

        @pl.when(self.z + d <= 3)
        def _():
            self._copy(self.z + d, False).wait_recv()
            self._hand_down(self.z + d)

    def finish(self):
        for slot in range(4):
            @pl.when((self.z < 3) & (slot <= self.z))
            def _():
                self._copy(slot, True).wait_send()

            @pl.when((self.z > 0) & (slot >= self.z))
            def _():
                self._copy(slot, False).wait_send()


def turn(u, cosine, sine):
    lane = lax.broadcasted_iota(jnp.int32, u.shape, 1)
    other = jnp.where(lane % 64 < 32, pltpu.roll(u, 96, 1), pltpu.roll(u, 32, 1))
    return u * cosine + other * sine


def halves(pair, out):
    lane = lax.broadcasted_iota(jnp.int32, pair.shape, 1)
    left = lane < 64
    swapped = pltpu.roll(pair, 64, 1)
    zero = jnp.zeros_like(pair)
    out[0, 0] = jnp.where(left, pair, zero).astype(BF)
    out[0, 1] = jnp.where(left, swapped, zero).astype(BF)
    out[1, 0] = jnp.where(left, zero, swapped).astype(BF)
    out[1, 1] = jnp.where(left, zero, pair).astype(BF)


def halves_t(pair, out, here):
    pair = pair.T
    zero = jnp.zeros((64, pair.shape[1]), BF)
    for g in range(2):
        head = pair[64 * g : 64 * g + 64].astype(BF)
        out[0, g, :64, here] = head
        out[0, g, 64:, here] = zero
        out[1, g, :64, here] = zero
        out[1, g, 64:, here] = head


def key_places(kv_ref, kcol):
    rows = kcol.shape[1]
    for j in range(4):
        digit = kv_ref[j, rows:, :].astype(F32)
        places = jnp.broadcast_to(digit[0:1] * 32.0 + digit[1:2], (128, rows))
        for lo in range(0, rows, 128):
            column = places[:, lo : lo + 128].T
            kcol[j * rows + lo : j * rows + lo + 128, :128] = column
            kcol[j * rows + lo : j * rows + lo + 128, 128:] = column


def scan_rows(count, body, init):
    return lax.fori_loop(
        0, count, lambda t, carry: body(pl.ds(pl.multiple_of(t * 64, 64), 64), carry), init, unroll=4
    )


def eights(value, op):
    parts = [value[8 * j : 8 * j + 8] for j in range(value.shape[0] // 8)]
    while len(parts) > 1:
        parts = [op(parts[j], parts[j + 1]) for j in range(0, len(parts), 2)]
    return parts[0]


def front_kernel(
    x_ref, pos_ref, cos_ref, sin_ref, wq_ref, wk_ref, wv_ref, wo_ref,
    n1_ref, bq_ref, bk_ref, bv_ref, n2_ref, wg_ref, wu_ref, cot_ref,
    xn_ref, q_ref, kv_ref, lse_ref, obt_ref, mid_ref, xn2_ref,
    wkv_ref, wq_all, wo_all, vec_ref, wgu_ref, df_ref,
    wkv_own, small_f, small_own, small_all, wgu_out, kk, vvt, score, prob, kcol, *sems,
):
    place = plane()
    me = lax.axis_index("fsdp")
    z = lax.axis_index("ctx")
    rows = x_ref.shape[0]
    ff_own, ff = wg_ref.shape[1] // 8, wgu_ref.shape[2] // 2
    greet_all()
    gkv = Gather(place, wkv_own, wkv_ref, sems[0], sems[1], by_owner=True)
    gs = Gather(place, small_own, small_all, sems[2], sems[3], by_owner=True)
    gq = Gather(place, wq_ref, wq_all, sems[4], sems[5], by_owner=True)
    go = Gather(place, wo_ref, wo_all, sems[6], sems[7], by_owner=True)
    send_u, recv_u = sems[8:10]
    gk = LineGather(kv_ref, *sems[10:13])
    gd = Gather(place, cot_ref, df_ref, sems[13], sems[14])

    wkv_own[:, :128] = wk_ref[...]
    wkv_own[:, 128:] = wv_ref[...]
    gkv.start()
    small_f[...] = jnp.zeros_like(small_f)
    small_f[0:1, :112] = n1_ref[...].astype(F32)
    small_f[1:2, :112] = bq_ref[...].astype(F32)
    small_f[2:3, :16] = bk_ref[...].astype(F32)
    small_f[2:3, 128:144] = bv_ref[...].astype(F32)
    small_f[3:4, :112] = n2_ref[...].astype(F32)
    flat = small_f[...]
    row = lax.broadcasted_iota(jnp.int32, flat.shape, 0)
    placed = jnp.where(row == 2, pltpu.roll(flat, me * 16, 1), pltpu.roll(flat, me * 112, 1))
    small_own[...] = placed.astype(BF)
    gs.start()
    gq.start()
    wkv_ref[me] = wkv_own[...]
    small_all[me] = small_own[...]
    wq_all[me] = wq_ref[...]
    wo_all[me] = wo_ref[...]
    for j in range(8):
        for half, src in ((0, wg_ref), (1, wu_ref)):
            block = src[:, j * ff_own : (j + 1) * ff_own]
            wgu_out[j, :, half * ff : half * ff + ff_own] = block
            wgu_out[j, :, half * ff + ff_own : (half + 1) * ff] = jnp.zeros(
                (src.shape[0], ff - ff_own), BF
            )
    df_ref[0] = cot_ref[...]
    place_row = pos_ref[...].astype(F32)
    high = jnp.floor(place_row * (1.0 / 32.0))
    kv_ref[z, rows : rows + 1, :] = high.astype(BF)
    kv_ref[z, rows + 1 : rows + 2, :] = (place_row - 32.0 * high).astype(BF)
    kv_ref[z, rows + 2 :, :] = jnp.zeros((14, 256), BF)

    gkv.relay()
    gs.relay()
    gkv.relay_corner()
    gs.relay_corner()
    for slot in (3, 5, 7, 1):
        gkv.wait(slot)
        gs.wait(slot)
    vec = small_all[0].astype(F32)
    for j in range(1, 8):
        vec = vec + small_all[j].astype(F32)
    vec_ref[...] = vec

    def norm_one(at):
        h = x_ref[at, :].astype(F32)
        scale = lax.rsqrt(jnp.mean(h * h, axis=-1, keepdims=True) + EPSILON)
        xn_ref[at, :] = (h * scale * vec_ref[0:1, :]).astype(BF)

    tiles(rows, 32, norm_one)
    cosine, sine = cos_ref[...], sin_ref[...]
    kv = dot(xn_ref[...], wkv_ref[...].reshape(896, 256)) + vec_ref[2:3, :256]
    kv_ref[z, :rows, :128] = turn(kv[:, :128], cosine, sine).astype(BF)
    kv_ref[z, :rows, 128:] = kv[:, 128:].astype(BF)
    gk.start()

    gq.relay()
    go.start()

    def block_to(r):
        owner = peer(r)
        return push(wgu_out.at[owner], wgu_ref.at[me], send_u.at[r], recv_u.at[r], {"fsdp": owner})

    @pl.loop(1, 8)
    def _(i):
        block_to(8 - i).start()

    wgu_ref[me] = wgu_out[me]
    gd.start()
    gk.collect(1)
    gq.relay_corner()
    for slot in (3, 5, 7, 1):
        gq.wait(slot)

    @pl.loop(0, 7)
    def _(i):
        at = pl.ds(pl.multiple_of(i * 128, 128), 128)
        q = dot(xn_ref[...], wq_all[:, :, at].reshape(896, 128)) + vec_ref[1:2, at]
        q_ref[:, at] = (turn(q, cosine, sine) * 0.125).astype(BF)

    gk.collect(2)

    gk.collect(3)
    for j in range(4):
        here = pl.ds(j * rows, rows)
        halves(kv_ref[j, :rows, :128].astype(F32), kk.at[:, :, here])
        halves_t(kv_ref[j, :rows, 128:].astype(F32), vvt, here)
    key_places(kv_ref, kcol)
    count = 4 * rows // 64

    @pl.loop(0, 7)
    def _(i):
        lanes = pl.ds(pl.multiple_of(i * 128, 128), 128)
        o = None
        for half in range(2):
            head = 2 * i + half
            score[...] = dot_t(kk[half, head // 7], q_ref[:, lanes])

            def find_top(at, top):
                s = jnp.where(kcol[at, :] <= place_row, score[at, :], NEGATIVE)
                score[at, :] = s
                return jnp.maximum(top, eights(s, jnp.maximum))

            top = scan_rows(count, find_top, jnp.full((8, rows), NEGATIVE, F32))
            top = jnp.max(top, axis=0, keepdims=True)

            def soft(at, total):
                e = jnp.exp(score[at, :] - top)
                prob[at, :] = e.astype(BF)
                return total + eights(e, jnp.add)

            total = scan_rows(count, soft, jnp.zeros((8, rows), F32))
            total = jnp.sum(total, axis=0, keepdims=True)
            lse_ref[pl.ds(head, 1), :] = top + jnp.log(total)
            part = dot(vvt[half, head // 7], prob[...]) * (1.0 / total)
            o = part if o is None else o + part
        obt_ref[lanes, :] = o.astype(BF)

        @pl.when(i == 0)
        def _():
            go.relay()

        @pl.when(i == 5)
        def _():
            go.relay_corner()

    for slot in (3, 5, 7, 1):
        go.wait(slot)
    for lo in range(0, 896, 128):
        mid_ref[:, lo : lo + 128] = t_dot(obt_ref[...], wo_all[:, :, lo : lo + 128].reshape(896, 128))

    def norm_two(at):
        m = mid_ref[at, :] + x_ref[at, :].astype(F32)
        mid_ref[at, :] = m
        scale = lax.rsqrt(jnp.mean(m * m, axis=-1, keepdims=True) + EPSILON)
        xn2_ref[at, :] = (m * scale * vec_ref[3:4, :]).astype(BF)

    tiles(rows, 32, norm_two)

    @pl.loop(1, 8)
    def _(r):
        block_to(r).wait_send()
        push(
            wgu_out.at[me], wgu_ref.at[peer(r)], send_u.at[r], recv_u.at[r], {"fsdp": peer(r)}
        ).wait_recv()

    gd.relay()
    gd.relay_corner()
    for slot in (1, 3, 5, 7):
        gd.wait(slot)
    for each in (gkv, gs, gq, go, gk, gd):
        each.finish()


def front(x, pos, cosine, sine, wq, wk, wv, wo, n1, bq, bk, bv, n2, wg, wu, cot):
    dma = pltpu.SemaphoreType.DMA
    vm = pl.BlockSpec(memory_space=pltpu.VMEM)
    vmem = pltpu.VMEM
    out = jax.ShapeDtypeStruct
    rows, width = x.shape
    own = wq.shape[0]
    ff = -(-(wg.shape[1] // 8) // 128) * 128
    tokens = 4 * rows
    return pl.pallas_call(
        front_kernel,
        out_shape=(
            out((rows, width), BF), out((rows, width), BF), out((4, rows + 16, 256), BF),
            out((16, rows), F32), out((width, rows), BF), out((rows, width), F32),
            out((rows, width), BF), out((8, own, 256), BF), out((8, own, width), BF),
            out((8, own, width), BF), out((16, width), F32), out((8, own, 2 * ff), BF),
            out((8, rows, width), BF),
        ),
        in_specs=[vm] * 16,
        out_specs=(vm,) * 13,
        scratch_shapes=[
            vmem((own, 256), BF), vmem((16, width), F32), vmem((16, width), BF), vmem((8, 16, width), BF),
            vmem((8, own, 2 * ff), BF), vmem((2, 2, tokens, 128), BF), vmem((2, 2, 128, tokens), BF),
            vmem((tokens, rows), F32), vmem((tokens, rows), BF), vmem((tokens, rows), F32),
            dma((7,)), dma((8,)), dma((7,)), dma((8,)), dma((7,)), dma((8,)), dma((7,)), dma((8,)),
            dma((8,)), dma((8,)), dma((4,)), dma((4,)), dma((4,)), dma((7,)), dma((8,)),
        ],
        compiler_params=pltpu.CompilerParams(collective_id=2, has_side_effects=True),
    )(x, pos, cosine, sine, wq, wk, wv, wo, n1, bq, bk, bv, n2, wg, wu, cot)


def middle_kernel(
    xn2_ref, pos_ref, cos_ref, sin_ref, kv_ref, lse_ref, vec_ref,
    df_hbm, wgu_hbm, wd_hbm, x_hbm, cot_hbm, mid_hbm, xn_hbm, q_hbm, obt_hbm, wkv_hbm, wq_hbm, wo_hbm,
    out_ref, gin_ref, pair_q, pair_o, pair_k, in_u, pair_d,
    x_all, part_out, core_in, tree_in, dx, core_f, tree_f, gwgu, gwd, mate_d, pair_u, mate_u,
    core_o, tree_o, core_q, tree_q, core_k, tree_k,
    own_o, mate_o, own_q, mate_q, own_k, mate_k, dkv_in, *sems,
):
    place = plane()
    me = lax.axis_index("fsdp")
    z = lax.axis_index("ctx")
    rows, width = xn2_ref.shape
    own = width // 8
    ff, ff_own = wgu_hbm.shape[1] // 2, wd_hbm.shape[0]
    tokens, keys = 8 * rows, 4 * rows
    piece = gwd.shape[1]
    loads = sems[38]
    greet_all()
    line_sems = sems[18:24]
    ld = Line(gwd, pair_d, mate_d, line_sems, 0)
    lu = Line(gwgu, pair_u, mate_u, line_sems, 4)
    lo = Line(own_o, pair_o, mate_o, line_sems, 12)
    lq = Line(own_q, pair_q, mate_q, line_sems, 13)
    lk = Line(own_k, pair_k, mate_k, line_sems, 14)
    send_all, recv_all, send_kv, recv_kv = sems[24:28]

    def feed_forward(df_ref, wgu_ref, wd, act_all, hid_all, dgu_all, dh, part, folded):
        gx = Gather(place, xn2_ref, x_all, sems[0], sems[1])
        rd = Scatter(place, part, core_in, tree_in, folded, *sems[2:6])
        gx.start()
        fetch = [
            pltpu.make_async_copy(wgu_hbm, wgu_ref, loads.at[0]),
            pltpu.make_async_copy(wd_hbm, wd.at[pl.ds(0, ff_own)], loads.at[1]),
            pltpu.make_async_copy(df_hbm, df_ref, loads.at[2]),
        ]
        for cp in fetch:
            cp.start()
        x_all[0] = xn2_ref[...]
        wd[ff_own:] = jnp.zeros((ff - ff_own, width), BF)
        fetch[0].wait()
        fetch[1].wait()
        both = lambda ref, p: ref[pl.ds(2 * p, 2)].reshape(2 * rows, ref.shape[2])

        @pl.loop(0, 4)
        def _(p):
            @pl.when(p == 1)
            def _():
                gx.relay()

            @pl.when(p == 3)
            def _():
                gx.relay_corner()

            gx.wait(2 * p + 1)
            x = both(x_all, p)
            for n in range(0, 2 * ff, 256):
                act_all[p, :, n : n + 256] = dot(x, wgu_ref[:, n : n + 256])

            def activate(at):
                gate, up = act_all[p, at, :ff], act_all[p, at, ff:]
                sig = 0.5 * jnp.tanh(0.5 * gate) + 0.5
                hid_all[p, at, :] = (gate * sig * up).astype(BF)

            tiles(2 * rows, 16, activate)
            out = dot(hid_all[p], wd[...]).astype(BF)
            part_out[pl.ds(2 * p, 2)] = out.reshape(2, rows, width)

        fetch[2].wait()
        for p in range(4):
            gwd[p] = t_dot(
                hid_all[:, :, p * piece : (p + 1) * piece].reshape(tokens, piece),
                df_ref[...].reshape(tokens, width),
            ).astype(BF)
            ld.start(p)

        @pl.loop(0, 4)
        def _(k):
            p = 3 - k
            dh[...] = dot_t(both(df_ref, p), wd[...])

            def activate(at):
                gate, up, d = act_all[p, at, :ff], act_all[p, at, ff:], dh[at, :]
                sig = 0.5 * jnp.tanh(0.5 * gate) + 0.5
                dgu_all[p, at, :ff] = (d * up * (sig * (1.0 + gate * (1.0 - sig)))).astype(BF)
                dgu_all[p, at, ff:] = (d * (gate * sig)).astype(BF)

            tiles(2 * rows, 16, activate)
            value = dot_t(dgu_all[p], wgu_ref[...]).astype(BF)
            part[pl.ds(2 * p, 2)] = value.reshape(2, rows, width)
            rd.to_twin(p).start()

            @pl.when(k == 1)
            def _():
                rd.start_corner()

            @pl.when(k == 2)
            def _():
                ld.meet(0)

        rd.start_far()
        ld.meet(1)
        rd.relay()

        @pl.loop(0, 2 * ff // 256)
        def _(n):
            at = pl.ds(pl.multiple_of(n * 256, 256), 256)
            value = t_dot(x_all[...].reshape(tokens, width), dgu_all[:, :, at].reshape(tokens, 256))
            gwgu[:, :, at] = value.astype(BF).reshape(8, own, 256)

            @pl.when(n == 1)
            def _():
                ld.meet(2)

            @pl.when(n == 3)
            def _():
                ld.settle(0)

        for r in (7, 6, 5, 4):
            lu.start(peer(r))

        def store_dx(at, value):
            dx[at, :] = value

        rd.total(store_dx)
        gx.finish()
        rd.finish()

    pl.run_scoped(
        feed_forward,
        pltpu.VMEM((8, rows, width), BF), pltpu.VMEM((width, 2 * ff), BF), pltpu.VMEM((ff, width), BF),
        pltpu.VMEM((4, 2 * rows, 2 * ff), F32), pltpu.VMEM((4, 2 * rows, ff), BF),
        pltpu.VMEM((4, 2 * rows, 2 * ff), BF), pltpu.VMEM((2 * rows, ff), F32),
        pltpu.VMEM((8, rows, width), BF), pltpu.VMEM((3, rows, width), BF),
    )

    def attention_back(
        x_ref, cot_ref, mid_ref, xn_ref, q_ref, obt_ref, wkv_ref, wq_ref, wo_ref,
        dm, da, dob, kk, kkt, vv, kcol, score, dprob, prob, dscore, dk_acc, dv_acc,
        dq, dkv_own, dkv, dxn, small, part_o, fold_o, part_q, fold_q, part_k, fold_k, fold_f,
    ):
        ro = Scatter(place, part_o, core_o, tree_o, fold_o, *sems[6:10], by_owner=True)
        rq = Scatter(place, part_q, core_q, tree_q, fold_q, *sems[10:14], by_owner=True)
        rk = Scatter(place, part_k, core_k, tree_k, fold_k, *sems[14:18], by_owner=True)
        rf = Scatter(place, part_out, core_f, tree_f, fold_f, *sems[28:32])
        arrays = (
            (mid_hbm, mid_ref), (cot_hbm, cot_ref), (obt_hbm, obt_ref), (wo_hbm, wo_ref), (q_hbm, q_ref),
            (xn_hbm, xn_ref), (wq_hbm, wq_ref), (wkv_hbm, wkv_ref), (x_hbm, x_ref),
        )
        fetch = [pltpu.make_async_copy(src, dst, loads.at[3 + i]) for i, (src, dst) in enumerate(arrays)]
        for cp in fetch:
            cp.start()
        for k in (3, 2, 1, 0):
            rf.to_twin(k).start()
        ld.meet(3)
        ld.settle(1)
        fetch[0].wait()
        fetch[1].wait()

        small[...] = jnp.zeros_like(small)

        def norm_two(at):
            m, g = mid_ref[at, :], dx[at, :]
            scale = lax.rsqrt(jnp.mean(m * m, axis=-1, keepdims=True) + EPSILON)
            weighted = vec_ref[3:4, :] * g
            inner = jnp.mean(weighted * m, axis=-1, keepdims=True)
            d = cot_ref[at, :].astype(F32) + scale * weighted - m * (scale * scale * scale) * inner
            dm[at, :] = d
            da[at, :] = d.astype(BF)
            small[3:4, :] += jnp.sum(g * m * scale, axis=0, keepdims=True)

        tiles(rows, 32, norm_two)
        for i in range(2, 9):
            fetch[i].wait()

        @pl.loop(0, 7)
        def _(i):
            lanes = pl.ds(pl.multiple_of(i * 128, 128), 128)
            part_o[:, :, lanes] = dot(obt_ref[...], da[:, lanes]).astype(BF).reshape(8, own, 128)

        for k in (3, 2, 1, 0):
            ro.to_twin(k).start()
        dob[...] = dot_t(da[...], wo_ref[...].reshape(width, width)).astype(BF)
        for j in range(4):
            here = pl.ds(j * rows, rows)
            key, value = kv_ref[j, :rows, :128].astype(F32), kv_ref[j, :rows, 128:].astype(F32)
            halves(key, kk.at[:, :, here])
            halves(value, vv.at[:, :, here])
            halves_t(key, kkt, here)
        key_places(kv_ref, kcol)
        dk_acc[...] = jnp.zeros_like(dk_acc)
        dv_acc[...] = jnp.zeros_like(dv_acc)
        place_row = pos_ref[...].astype(F32)
        cosine, sine = cos_ref[...], -sin_ref[...]
        count = keys // 64

        def keep(total):
            def store(at, value):
                total[0, at, :] = value.astype(BF)

            return store

        def gather_to(r):
            owner = peer(r)
            return push(pair_u.at[owner], in_u.at[me], send_all.at[r], recv_all.at[me], {"fsdp": owner})

        def settle_u(r):
            lu.settle(peer(r))
            gather_to(r).start()

        ld.settle(2)

        @pl.loop(0, 7)
        def _(i):
            lanes = pl.ds(pl.multiple_of(i * 128, 128), 128)
            grad = None
            for half in range(2):
                head = 2 * i + half
                g = head // 7
                score[...] = dot_t(kk[half, g], q_ref[:, lanes])
                dprob[...] = dot_t(vv[half, g], dob[:, lanes])
                lse_row = lse_ref[pl.ds(head, 1), :]

                def find_delta(at, total):
                    s = jnp.where(kcol[at, :] <= place_row, score[at, :], NEGATIVE)
                    p = jnp.exp(s - lse_row)
                    score[at, :] = p
                    prob[at, :] = p.astype(BF)
                    return total + eights(p * dprob[at, :], jnp.add)

                delta = scan_rows(count, find_delta, jnp.zeros((8, rows), F32))
                delta = jnp.sum(delta, axis=0, keepdims=True)

                def find_score(at):
                    dscore[at, :] = (score[at, :] * (dprob[at, :] - delta)).astype(BF)

                tiles(keys, 64, find_score)
                dv_acc[half, g] += dot(prob[...], dob[:, lanes])
                dk_acc[half, g] += dot(dscore[...], q_ref[:, lanes])
                term = dot(kkt[half, g], dscore[...])
                grad = term if grad is None else grad + term
            dq[:, lanes] = turn(grad.T * 0.125, cosine, sine).astype(BF)

            @pl.when(i == 0)
            def _():
                ro.start()
                rf.start()
                lu.meet(peer(7))

            @pl.when(i == 1)
            def _():
                ld.settle(3)

            @pl.when(i == 2)
            def _():
                lu.meet(peer(6))

            @pl.when(i == 3)
            def _():
                ro.relay()
                rf.relay()
                settle_u(7)

            @pl.when(i == 4)
            def _():
                lu.meet(peer(5))

            @pl.when(i == 5)
            def _():
                settle_u(6)
                ro.total(keep(own_o))

            @pl.when(i == 6)
            def _():
                lu.meet(peer(4))

        lane = lax.broadcasted_iota(jnp.int32, (64, 128), 1)

        def join(acc, at):
            first = jnp.where(lane < 64, acc[0, 0, at, :], acc[1, 1, at, :])
            second = jnp.where(lane < 64, acc[0, 1, at, :], acc[1, 0, at, :])
            return first + pltpu.roll(second, 64, 1)

        @pl.loop(0, 4)
        def _(j):
            for first in range(0, rows, 64):
                at = pl.ds(pl.multiple_of(j * rows + first, 64), 64)
                dkv_own[j, first : first + 64, :128] = join(dk_acc, at).astype(BF)
                dkv_own[j, first : first + 64, 128:] = join(dv_acc, at).astype(BF)

        def kv_to(d):
            other = (z + d) % 4
            return push(
                dkv_own.at[other], dkv_in.at[d - 1], send_kv.at[d - 1], recv_kv.at[d - 1], {"ctx": other}
            )

        for d in (2, 1, 3):
            kv_to(d).start()

        @pl.loop(4, 8)
        def _(i):
            lu.start(peer(7 - i))

        lo.start(0)
        settle_u(5)

        def weight_grads(grads, part, n):
            for at in range(0, n, 128):
                value = t_dot(xn_ref[...], grads[:, at : at + 128]).astype(BF)
                part[:, :, at : at + 128] = value.reshape(8, own, 128)

        weight_grads(dq, part_q, width)
        for k in (3, 2, 1, 0):
            rq.to_twin(k).start()
        for at in range(0, width, 128):
            wq_rows = wq_ref[...].reshape(width, width)
            dxn[:, at : at + 128] = dot_t(dq[...], wq_rows[at : at + 128])
        rq.start()
        settle_u(4)

        def store_out(at, value):
            out_ref[at, :] = value + mid_ref[at, :]

        rf.total(store_out)
        for d in (1, 3, 2):
            kv_to(d).wait_recv()

        def sum_kv(at):
            value = dkv_own[z, at, :].astype(F32)
            for d in range(3):
                value = value + dkv_in[d, at, :].astype(F32)
            dkv[at, :128] = turn(value[:, :128], cos_ref[at, :], -sin_ref[at, :]).astype(BF)
            dkv[at, 128:] = value[:, 128:].astype(BF)

        tiles(rows, 32, sum_kv)
        weight_grads(dkv, part_k, 256)
        for at in range(0, width, 128):
            wkv_rows = wkv_ref[...].reshape(width, 256)
            dxn[:, at : at + 128] += dot_t(dkv[...], wkv_rows[at : at + 128])

        def norm_one(at):
            h, g = x_ref[at, :].astype(F32), dxn[at, :]
            scale = lax.rsqrt(jnp.mean(h * h, axis=-1, keepdims=True) + EPSILON)
            weighted = vec_ref[0:1, :] * g
            inner = jnp.mean(weighted * h, axis=-1, keepdims=True)
            gin_ref[at, :] = dm[at, :] + scale * weighted - h * (scale * scale * scale) * inner
            small[0:1, :] += jnp.sum(g * h * scale, axis=0, keepdims=True)
            small[1:2, :] += jnp.sum(dq[at, :].astype(F32), axis=0, keepdims=True)
            small[2:3, :256] += jnp.sum(dkv[at, :].astype(F32), axis=0, keepdims=True)

        tiles(rows, 32, norm_one)
        flat = small[...]
        line_of = lax.broadcasted_iota(jnp.int32, (16, 128), 0)
        for j in range(8):
            by_row = pltpu.roll(flat, (width - 112 * j) % width, 1)[:, :128]
            by_head = pltpu.roll(flat, (width - 16 * j) % width, 1)
            value = jnp.where(line_of == 2, by_head[:, :128], by_row)
            lifted = pltpu.roll(by_head[:, 128:256], 2, 0)
            value = jnp.where(line_of == 4, lifted, value)
            part_k[j, :16, 256:] = value.astype(BF)
            part_k[j, 16:, 256:] = jnp.zeros((own - 16, 128), BF)

        for k in (3, 2, 1, 0):
            rk.to_twin(k).start()
        lu.meet(peer(3))
        rk.start()
        rq.relay()
        lu.meet(peer(2))
        settle_u(3)
        rk.relay()
        rq.total(keep(own_q))
        lq.start(0)
        lu.meet(peer(1))
        rk.total(keep(own_k))
        lk.start(0)
        settle_u(2)
        lu.meet(me)
        settle_u(1)
        lo.meet(0)
        lu.settle(me)
        keep_own = pltpu.make_async_copy(pair_u.at[me], in_u.at[me], loads.at[12])
        keep_own.start()
        lq.meet(0)
        lo.settle(0)
        lk.meet(0)
        lq.settle(0)
        lk.settle(0)
        keep_own.wait()

        @pl.loop(1, 8)
        def _(r):
            other = peer(r)
            push(
                pair_u.at[me], in_u.at[other], send_all.at[r], recv_all.at[other], {"fsdp": other}
            ).wait_recv()
            gather_to(r).wait_send()

        for d in (1, 2, 3):
            kv_to(d).wait_send()
        for each in (ro, rq, rk, rf):
            each.finish()

    v = pltpu.VMEM
    pl.run_scoped(
        attention_back,
        v((rows, width), BF), v((rows, width), BF), v((rows, width), F32), v((rows, width), BF),
        v((rows, width), BF), v((width, rows), BF), v((8, own, 256), BF), v((8, own, width), BF),
        v((8, own, width), BF),
        v((rows, width), F32), v((rows, width), BF), v((rows, width), BF),
        v((2, 2, keys, 128), BF), v((2, 2, 128, keys), BF), v((2, 2, keys, 128), BF),
        v((keys, rows), F32), v((keys, rows), F32), v((keys, rows), F32),
        v((keys, rows), BF), v((keys, rows), BF),
        v((2, 2, keys, 128), F32), v((2, 2, keys, 128), F32),
        v((rows, width), BF), v((4, rows, 256), BF), v((rows, 256), BF), v((rows, width), F32),
        v((16, width), F32),
        v((8, own, width), BF), v((3, own, width), BF), v((8, own, width), BF), v((3, own, width), BF),
        v((8, own, 384), BF), v((3, own, 384), BF), v((3, rows, width), BF),
    )

    @pl.loop(0, 4)
    def _(p):
        ld.finish(p)

    @pl.loop(0, 8)
    def _(p):
        lu.finish(p)

    for each in (lo, lq, lk):
        each.finish(0)


def middle(xn2, pos, cosine, sine, kv, lse, vec, df_all, wgu, wd, x, cot, mid, xn, q, obt, wkv, wq, wo):
    dma = pltpu.SemaphoreType.DMA
    vm = pl.BlockSpec(memory_space=pltpu.VMEM)
    hbm = pl.BlockSpec(memory_space=pl.ANY)
    v = pltpu.VMEM
    out = jax.ShapeDtypeStruct
    rows, width = x.shape
    own = width // 8
    ff = wgu.shape[1] // 2
    gu, gd = (8, own, 2 * ff), (4, ff // 4, width)
    wide, narrow = (1, own, width), (1, own, 384)
    tree = [dma((4,)), dma((4,)), dma((3,)), dma((3,))]
    return pl.pallas_call(
        middle_kernel,
        out_shape=(
            out((rows, width), F32), out((rows, width), F32), out(wide, BF), out(wide, BF), out(narrow, BF),
            out(gu, BF), out(gd, BF),
        ),
        in_specs=[vm] * 7 + [hbm] * 12,
        out_specs=(vm, vm, vm, vm, vm, hbm, vm),
        scratch_shapes=[
            v((8, rows, width), BF), v((8, rows, width), BF), v((4, rows, width), BF), v((3, rows, width), BF),
            v((rows, width), F32), v((4, rows, width), BF), v((3, rows, width), BF),
            v(gu, BF), v(gd, BF), v(gd, BF), v(gu, BF), v(gu, BF),
            v((4, own, width), BF), v((3, own, width), BF), v((4, own, width), BF), v((3, own, width), BF),
            v((4, own, 384), BF), v((3, own, 384), BF),
            v(wide, BF), v(wide, BF), v(wide, BF), v(wide, BF), v(narrow, BF), v(narrow, BF),
            v((3, rows, 256), BF),
            dma((7,)), dma((8,)), *tree, *tree, *tree, *tree,
            *[dma((15,))] * 6,
            dma((8,)), dma((8,)), dma((3,)), dma((3,)), *tree,
            *[dma((1,))] * 6, dma((13,)),
        ],
        compiler_params=pltpu.CompilerParams(
            collective_id=0, has_side_effects=True, vmem_limit_bytes=67043328
        ),
    )(xn2, pos, cosine, sine, kv, lse, vec, df_all, wgu, wd, x, cot, mid, xn, q, obt, wkv, wq, wo)


def results_kernel(
    out_ref, gin_ref, tq_ref, to_ref, tk_ref, tu_ref, td_ref,
    o_ref, i_ref, n1_ref, q_ref, bq_ref, k_ref, bk_ref, v_ref, bv_ref, w_ref, n2_ref, g_ref, u_ref, d_ref,
):
    o_ref[...] = out_ref[...]
    i_ref[...] = gin_ref[...]
    q_ref[...] = tq_ref[0].astype(F32)
    w_ref[...] = to_ref[0].astype(F32)
    k_ref[...] = tk_ref[0, :, :128].astype(F32)
    v_ref[...] = tk_ref[0, :, 128:256].astype(F32)
    small = tk_ref[0, :16, 256:].astype(F32)
    for i, ref in enumerate((n1_ref, bq_ref, bk_ref, n2_ref, bv_ref)):
        ref[...] = small[i : i + 1, : ref.shape[1]]
    ff_own, ff = d_ref.shape[0], tu_ref.shape[2] // 2
    for j in range(8):
        def place_block(at):
            g_ref[at, j * ff_own : (j + 1) * ff_own] = tu_ref[j, at, :ff_own].astype(F32)
            u_ref[at, j * ff_own : (j + 1) * ff_own] = tu_ref[j, at, ff : ff + ff_own].astype(F32)

        tiles(tu_ref.shape[1], 16, place_block)
    rows = td_ref.shape[1]
    for p in range(4):
        count = min(rows, ff_own - p * rows)
        d_ref[p * rows : p * rows + count] = td_ref[p, :count].astype(F32)


def results(out, gin, tq, to, tk, tu, td, ff_own):
    vm = pl.BlockSpec(memory_space=pltpu.VMEM)
    rows, width = out.shape
    own = width // 8
    shapes = (
        (rows, width), (rows, width), (1, own), (own, 896), (1, own), (own, 128), (1, 16), (own, 128), (1, 16),
        (own, 896), (1, own), (own, 8 * ff_own), (own, 8 * ff_own), (ff_own, width),
    )
    return pl.pallas_call(
        results_kernel,
        out_shape=tuple(jax.ShapeDtypeStruct(shape, F32) for shape in shapes),
        in_specs=[vm] * 7,
        out_specs=(vm,) * 14,
    )(out, gin, tq, to, tk, tu, td)


def shards(
    inputs, positions, cotangent, norm_one, w_query, b_query, key_projection, b_key,
    value_projection, value_bias, w_out, norm_two, w_gate, w_up, w_down,
):
    places = positions[0]
    turned = angles_of(places)
    cosine, sine = jnp.cos(turned), jnp.sin(turned)
    sine = jnp.where(jnp.arange(128)[None, :] % 64 < 32, -sine, sine)
    own = w_query.shape[1]
    ff_own = w_down.shape[1]
    ff = -(-ff_own // 128) * 128
    x, cot = inputs[0], cotangent[0]
    xn, q, kv, lse, obt, mid, xn2, wkv, wq, wo, vec, wgu, df_all = front(
        x, positions, cosine, sine, w_query[0], key_projection[0], value_projection[0], w_out[0],
        norm_one, b_query, b_key, value_bias, norm_two, w_gate[0], w_up[0], cot,
    )
    totals = middle(
        xn2, positions, cosine, sine, kv, lse, vec, df_all, wgu.reshape(-1, 2 * ff), w_down[0],
        x, cot, mid, xn, q, obt, wkv, wq, wo,
    )
    matrix = lambda i: i in (0, 1, 3, 5, 7, 9, 11, 12, 13)
    return tuple(g[None] if matrix(i) else g for i, g in enumerate(results(*totals, ff_own)))


def angles_of(places):
    half = HEAD_SIZE // 2
    inverse = jnp.exp(jnp.arange(half, dtype=F32) * (-2.0 * math.log(ROPE_BASE) / HEAD_SIZE))
    return places.astype(F32)[:, None] * jnp.concatenate([inverse] * 4)[None, :]


def shards_general(
    inputs, positions, cotangent, norm_one, w_query, b_query, key_projection, b_key,
    value_projection, value_bias, w_out, norm_two, w_gate, w_up, w_down,
):
    rows = inputs.shape[1]
    width = inputs.shape[2]
    group = QUERY_HEADS // KEY_VALUE_HEADS
    q_cols = w_query.shape[2]
    kv_cols = key_projection.shape[2]
    score_scale = 1.0 / math.sqrt(HEAD_SIZE)

    places = positions[0]
    key_places = lax.all_gather(places, "ctx", axis=0, tiled=True)
    cosine, sine = angles(places)
    hidden = inputs[0].astype(F32)

    packed = jnp.concatenate([w_query[0], key_projection[0], value_projection[0], w_out[0]], axis=1)
    packed = lax.all_gather(packed, "fsdp", axis=0, tiled=True)
    w_qkv = packed[:, : q_cols + 2 * kv_cols]
    w_o = packed[:, q_cols + 2 * kv_cols :]
    small = jnp.concatenate([norm_one[0], b_query[0], b_key[0], value_bias[0], norm_two[0]])
    small = lax.all_gather(small, "fsdp", axis=0).astype(F32)
    cuts, at = [], 0
    for piece in (norm_one, b_query, b_key, value_bias, norm_two):
        n = piece.shape[1]
        cuts.append(small[:, at : at + n].reshape(-1))
        at += n
    gain_one, bias_q, bias_k, bias_v, gain_two = cuts
    bias = jnp.concatenate([bias_q, bias_k, bias_v])

    grad_branch = cotangent[0]
    df_all = lax.all_gather(grad_branch, "fsdp", axis=0, tiled=True)
    wg = lax.all_to_all(w_gate[0], "fsdp", split_axis=1, concat_axis=0, tiled=True)
    wu = lax.all_to_all(w_up[0], "fsdp", split_axis=1, concat_axis=0, tiled=True)
    wd = w_down[0]

    scale_one, normed = norm_rows(hidden, gain_one)
    qkv = dot(normed, w_qkv) + bias
    q = rotate(qkv[:, :q_cols].reshape(rows, QUERY_HEADS, HEAD_SIZE), cosine, sine).astype(BF)
    k = rotate(
        qkv[:, q_cols : q_cols + kv_cols].reshape(rows, KEY_VALUE_HEADS, HEAD_SIZE), cosine, sine
    ).astype(BF)
    v = qkv[:, q_cols + kv_cols :].astype(BF)
    kv = jnp.concatenate([k.reshape(rows, kv_cols), v], axis=1)
    kv = lax.all_gather(kv, "ctx", axis=0, tiled=True)
    total = kv.shape[0]
    k_all = kv[:, :kv_cols].reshape(total, KEY_VALUE_HEADS, HEAD_SIZE)
    v_all = kv[:, kv_cols:].reshape(total, KEY_VALUE_HEADS, HEAD_SIZE)
    q = q.reshape(rows, KEY_VALUE_HEADS, group, HEAD_SIZE)
    s = jnp.einsum("tgjd,ugd->gjtu", q, k_all, preferred_element_type=F32) * score_scale
    s = jnp.where(key_places[None, :] <= places[:, None], s, NEGATIVE)
    top = jnp.max(s, axis=-1, keepdims=True)
    lse = top + jnp.log(jnp.sum(jnp.exp(s - top), axis=-1, keepdims=True))
    pf = jnp.exp(s - lse)
    p = pf.astype(BF)
    o = jnp.einsum("gjtu,ugd->tgjd", p, v_all, preferred_element_type=F32)
    ob = o.reshape(rows, q_cols).astype(BF)
    middle = hidden + dot(ob, w_o)
    scale_two, normed_two = norm_rows(middle, gain_two)

    x_all = lax.all_gather(normed_two, "fsdp", axis=0, tiled=True)
    gate = dot(x_all, wg)
    up = dot(x_all, wu)
    sig = jax.nn.sigmoid(gate)
    hid = (gate * sig * up).astype(BF)
    out_part = dot(hid, wd).astype(BF)
    ffn_out = lax.psum_scatter(out_part, "fsdp", scatter_dimension=0, tiled=True)
    output = middle + ffn_out.astype(F32)

    dhid = dot_t(df_all, wd)
    dgate = (dhid * up * sig * (1.0 + gate * (1.0 - sig))).astype(BF)
    dup = (dhid * (gate * sig)).astype(BF)
    dx_part = (dot_t(dgate, wg) + dot_t(dup, wu)).astype(BF)
    dxn2 = lax.psum_scatter(dx_part, "fsdp", scatter_dimension=0, tiled=True).astype(F32)
    g_down = t_dot(hid, df_all)
    g_gate = t_dot(x_all, dgate)
    g_up = t_dot(x_all, dup)

    g_out = grad_branch.astype(F32)
    grad_gain_two, dmid = norm_back(middle, scale_two, gain_two, dxn2)
    dm = g_out + dmid
    da = dm.astype(BF)
    g_wo = t_dot(ob, da)
    dob = dot_t(da, w_o).astype(BF).reshape(rows, KEY_VALUE_HEADS, group, HEAD_SIZE)

    dp = jnp.einsum("tgjd,ugd->gjtu", dob, v_all, preferred_element_type=F32)
    delta = jnp.sum(pf * dp, axis=-1, keepdims=True)
    ds = (pf * (dp - delta)).astype(BF)
    dq = jnp.einsum("gjtu,ugd->tgjd", ds, k_all, preferred_element_type=F32) * score_scale
    dk = jnp.einsum("gjtu,tgjd->ugd", ds, q, preferred_element_type=F32) * score_scale
    dv = jnp.einsum("gjtu,tgjd->ugd", p, dob, preferred_element_type=F32)
    dkv = jnp.concatenate([dk.reshape(total, kv_cols), dv.reshape(total, kv_cols)], axis=1)
    dkv = lax.psum_scatter(dkv, "ctx", scatter_dimension=0, tiled=True)
    dq = rotate(dq.reshape(rows, QUERY_HEADS, HEAD_SIZE), cosine, -sine).astype(BF)
    dk = rotate(
        dkv[:, :kv_cols].reshape(rows, KEY_VALUE_HEADS, HEAD_SIZE), cosine, -sine
    ).astype(BF)
    dqkv = jnp.concatenate(
        [dq.reshape(rows, q_cols), dk.reshape(rows, kv_cols), dkv[:, kv_cols:].astype(BF)], axis=1
    )
    g_qkv = t_dot(normed, dqkv)
    g_bias = jnp.sum(dqkv.astype(F32), axis=0)
    dxn = dot_t(dqkv, w_qkv)
    grad_gain_one, dhidden = norm_back(hidden, scale_one, gain_one, dxn)
    grad_in = dm + dhidden

    g_attn = jnp.concatenate([g_qkv, g_wo], axis=1).astype(BF)
    g_attn = lax.psum_scatter(g_attn, "fsdp", scatter_dimension=0, tiled=True)
    back = [
        lax.all_to_all(g.astype(BF), "fsdp", split_axis=0, concat_axis=1, tiled=True)
        for g in (g_gate, g_up)
    ]
    g_attn, g_gate, g_up, g_down = lax.psum((g_attn, back[0], back[1], g_down.astype(BF)), "ctx")
    pieces = jnp.concatenate(
        [
            g.reshape(small.shape[0], -1)
            for g in (
                grad_gain_one, g_bias[:q_cols], g_bias[q_cols : q_cols + kv_cols],
                g_bias[q_cols + kv_cols :], grad_gain_two,
            )
        ],
        axis=1,
    )
    pieces = lax.psum(pieces, ("ctx", "fsdp"))
    mine = lax.dynamic_slice_in_dim(pieces, lax.axis_index("fsdp"), 1, axis=0)
    outs, at = [], 0
    for piece in (norm_one, b_query, b_key, value_bias, norm_two):
        n = piece.shape[1]
        outs.append(mine[:, at : at + n])
        at += n
    g_n1, g_bq, g_bk, g_bv, g_n2 = outs
    g_attn = g_attn.astype(F32)
    return (
        output[None], grad_in[None], g_n1,
        g_attn[None, :, :q_cols], g_bq,
        g_attn[None, :, q_cols : q_cols + kv_cols], g_bk,
        g_attn[None, :, q_cols + kv_cols : q_cols + 2 * kv_cols], g_bv,
        g_attn[None, :, q_cols + 2 * kv_cols :], g_n2,
        g_gate.astype(F32)[None], g_up.astype(F32)[None], g_down.astype(F32)[None],
    )


def solution(mesh):
    tok, row, vec = P("fsdp", "ctx", None), P(None, "fsdp", None), P(None, "fsdp")
    fast = mesh.shape["ctx"] == 4 and mesh.shape["fsdp"] == 8
    return jax.shard_map(
        shards if fast else shards_general,
        mesh=mesh,
        in_specs=(
            tok, P("fsdp", "ctx"), tok, vec, row, vec, row, vec, row, vec, row, vec, row, row, row,
        ),
        out_specs=(tok, tok, vec, row, vec, row, vec, row, vec, row, vec, row, row, row),
        check_vma=False,
    )
```

```python
import functools
import math

import jax
import jax.numpy as jnp
from jax import lax
from jax.experimental import pallas as pl
from jax.experimental.pallas import tpu as pltpu
from jax.sharding import PartitionSpec as P

QUERY_HEADS = 14
KEY_VALUE_HEADS = 2
HEAD_SIZE = 64
ROPE_BASE = 1000000.0
EPSILON = 1e-06
NEGATIVE = -1e30
BF = jnp.bfloat16
F32 = jnp.float32
MESH = pl.DeviceIdType.MESH


def angles(places):
    half = HEAD_SIZE // 2
    inverse = jnp.exp(jnp.arange(half, dtype=F32) * (-2.0 * math.log(ROPE_BASE) / HEAD_SIZE))
    turned = places.astype(F32)[:, None] * inverse[None, :]
    return jnp.cos(turned)[:, None, :], jnp.sin(turned)[:, None, :]


def rotate(u, cosine, sine):
    half = u.shape[-1] // 2
    a, b = u[..., :half], u[..., half:]
    return jnp.concatenate([a * cosine - b * sine, b * cosine + a * sine], axis=-1)


def norm_rows(hidden, gain):
    scale = lax.rsqrt(jnp.mean(hidden * hidden, axis=-1, keepdims=True) + EPSILON)
    return scale, (hidden * scale * gain).astype(BF)


def norm_back(hidden, scale, gain, grad):
    weighted = gain * grad
    grad_gain = jnp.sum(grad * hidden * scale, axis=0)
    inner = jnp.mean(weighted * hidden, axis=-1, keepdims=True)
    return grad_gain, scale * weighted - hidden * (scale * scale * scale) * inner


def dot(a, b):
    return jnp.dot(a, b, preferred_element_type=F32)


def dot_t(a, b):
    return lax.dot_general(a, b, (((1,), (1,)), ((), ())), preferred_element_type=F32)


def t_dot(a, b):
    return lax.dot_general(a, b, (((0,), (0,)), ((), ())), preferred_element_type=F32)


def plane():
    f = lax.axis_index("fsdp")
    core, x, y = f % 2, (f // 2) % 2, f // 4
    by_x, by_y = f + 2 - 4 * x, f + 4 - 8 * y
    twin = f + 1 - 2 * core
    near = by_x + core * (by_y - by_x)
    far = by_y + core * (by_x - by_y)
    return twin, near, far, 2 + 2 * core, 4 - 2 * core


def tiles(rows, step, body):
    count = rows // step
    unroll = count if count <= 10 else 4

    @pl.loop(0, count, unroll=unroll)
    def _(r):
        body(pl.ds(pl.multiple_of(r * step, step), step))


def peer(r):
    f = lax.axis_index("fsdp")
    core, x, y = f % 2, (f // 2) % 2, f // 4
    return f + (r % 2) * (1 - 2 * core) + ((r // 2) % 2) * (2 - 4 * x) + (r // 4) * (4 - 8 * y)


def greet(others):
    barrier = pltpu.get_barrier_semaphore()
    for other in others:
        pl.semaphore_signal(barrier, inc=1, device_id=other, device_id_type=MESH)
    pl.semaphore_wait(barrier, len(others))


def push(src, dst, send, recv, other):
    return pltpu.make_async_remote_copy(
        src_ref=src, dst_ref=dst, send_sem=send, recv_sem=recv, device_id=other, device_id_type=MESH
    )


class Gather:
    def __init__(self, place, mine, full, send, recv, by_owner=False):
        self.twin, self.near, self.far, self.s_near, self.s_far = place
        self.mine, self.full, self.send, self.recv = mine, full, send, recv
        self.by_owner = by_owner

    def copy(self, i):
        twin, near, far = self.twin, self.near, self.far
        here = (0, 0, 0, self.s_near, 2, 4, 6)[i]
        there, other = (
            (self.s_near, near), (self.s_far, far), (1, twin), (6, far), (3, twin), (5, twin), (7, twin)
        )[i]
        if self.by_owner:
            here = there = peer(here)
        src = self.mine if i < 3 else self.full.at[here]
        return push(src, self.full.at[there], self.send.at[i], self.recv.at[there], {"fsdp": other})

    def start(self):
        for i in range(3):
            self.copy(i).start()

    def wait(self, slot):
        slot = peer(slot) if self.by_owner else slot
        full = self.full.at[slot]
        push(full, full, self.send.at[0], self.recv.at[slot], {"fsdp": self.near}).wait_recv()

    def relay(self):
        self.wait(2)
        self.wait(4)
        for i in range(3, 6):
            self.copy(i).start()

    def relay_corner(self):
        self.wait(6)
        self.copy(6).start()

    def finish(self):
        for i in range(7):
            self.copy(i).wait_send()


class Scatter:
    def __init__(
        self, place, part, core_in, tree_in, folded, send_core, recv_core, send_tree, recv_tree,
        by_owner=False,
    ):
        self.twin, self.near, self.far, self.s_near, self.s_far = place
        self.at = peer if by_owner else lambda slot: slot
        self.part, self.core_in, self.tree_in, self.folded = part, core_in, tree_in, folded
        self.send_core, self.recv_core = send_core, recv_core
        self.send_tree, self.recv_tree = send_tree, recv_tree

    def to_twin(self, k):
        return push(
            self.part.at[self.at(2 * k + 1)], self.core_in.at[k], self.send_core.at[k], self.recv_core.at[k],
            {"fsdp": self.twin},
        )

    def tree(self, j):
        other = (self.far, self.near, self.far)[j]
        return push(
            self.folded.at[j], self.tree_in.at[j], self.send_tree.at[j], self.recv_tree.at[j],
            {"fsdp": other},
        )

    def fold(self, j, slot, corner=False):
        part, core_in, tree_in, folded = self.part, self.core_in, self.tree_in, self.folded
        k = slot // 2
        slot = self.at(slot)

        def add(at):
            value = part[slot, at, :].astype(F32) + core_in[k, at, :].astype(F32)
            if corner:
                value = value + tree_in[0, at, :].astype(F32)
            folded[j, at, :] = value.astype(BF)

        tiles(part.shape[1], 16, add)

    def start_corner(self):
        self.to_twin(3).wait_recv()
        self.fold(0, 6)
        self.tree(0).start()

    def start_far(self):
        self.to_twin(1).wait_recv()
        self.to_twin(2).wait_recv()
        self.fold(2, self.s_far)
        self.tree(2).start()

    def start(self):
        self.start_corner()
        self.start_far()

    def relay(self):
        self.tree(0).wait_recv()
        self.fold(1, self.s_near, True)
        self.tree(1).start()

    def total(self, store):
        part, core_in, tree_in = self.part, self.core_in, self.tree_in
        mine = self.at(0)
        self.to_twin(0).wait_recv()
        self.tree(1).wait_recv()
        self.tree(2).wait_recv()

        def add(at):
            value = part[mine, at, :].astype(F32) + core_in[0, at, :].astype(F32)
            store(at, value + tree_in[1, at, :].astype(F32) + tree_in[2, at, :].astype(F32))

        tiles(part.shape[1], 16, add)

    def finish(self):
        for k in range(4):
            self.to_twin(k).wait_send()
        for j in range(3):
            self.tree(j).wait_send()


def line():
    z = lax.axis_index("ctx")
    inner = (z == 1) | (z == 2)
    return z, inner, z + 1 - 2 * (z // 3), 3 * (z // 2), 3 - z


class Line:
    def __init__(self, own, pair, mate, sems, first=0):
        self.own, self.pair, self.mate = own, pair, mate
        self.sems, self.first = sems, first
        self.z, self.inner, self.to_inner, self.to_outer, self.to_mate = line()

    def _copy(self, k, p):
        src, dst, other = (
            (self.own, self.pair, self.to_inner),
            (self.pair, self.mate, self.to_mate),
            (self.pair, self.pair, self.to_outer),
        )[k]
        i = self.first + p
        return push(src.at[p], dst.at[p], self.sems[2 * k].at[i], self.sems[2 * k + 1].at[i], {"ctx": other})

    def _rows(self, body):
        tiles(self.own.shape[1], 16, body)

    def start(self, p):
        @pl.when(~self.inner)
        def _():
            self._copy(0, p).start()

    def meet(self, p):
        own, pair = self.own, self.pair

        @pl.when(self.inner)
        def _():
            self._copy(0, p).wait_recv()

            def add(at):
                pair[p, at, :] = (pair[p, at, :].astype(F32) + own[p, at, :].astype(F32)).astype(BF)

            self._rows(add)
            self._copy(1, p).start()

    def settle(self, p):
        pair, mate = self.pair, self.mate

        @pl.when(self.inner)
        def _():
            self._copy(1, p).wait_recv()
            self._copy(1, p).wait_send()

            def add(at):
                pair[p, at, :] = (pair[p, at, :].astype(F32) + mate[p, at, :].astype(F32)).astype(BF)

            self._rows(add)
            self._copy(2, p).start()

        @pl.when(~self.inner)
        def _():
            self._copy(2, p).wait_recv()

    def finish(self, p):
        @pl.when(self.inner)
        def _():
            self._copy(2, p).wait_send()

        @pl.when(~self.inner)
        def _():
            self._copy(0, p).wait_send()


def greet_all():
    z = lax.axis_index("ctx")
    barrier = pltpu.get_barrier_semaphore()
    for r in range(1, 8):
        pl.semaphore_signal(barrier, inc=1, device_id={"fsdp": peer(r)}, device_id_type=MESH)

    for d in range(1, 4):
        pl.semaphore_signal(barrier, inc=1, device_id={"ctx": (z + d) % 4}, device_id_type=MESH)
    pl.semaphore_wait(barrier, 10)


class LineGather:
    def __init__(self, full, send_up, send_down, recv):
        self.full, self.send_up, self.send_down, self.recv = full, send_up, send_down, recv
        self.z = lax.axis_index("ctx")

    def _copy(self, slot, up):
        send = (self.send_up if up else self.send_down).at[slot]
        full = self.full.at[slot]
        return push(full, full, send, self.recv.at[slot], {"ctx": self.z + 1 if up else self.z - 1})

    def _hand_up(self, slot):
        @pl.when(self.z < 3)
        def _():
            self._copy(slot, True).start()

    def _hand_down(self, slot):
        @pl.when(self.z > 0)
        def _():
            self._copy(slot, False).start()

    def start(self):
        self._hand_up(self.z)
        self._hand_down(self.z)

    def collect(self, d):
        @pl.when(self.z >= d)
        def _():
            self._copy(self.z - d, True).wait_recv()
            self._hand_up(self.z - d)

        @pl.when(self.z + d <= 3)
        def _():
            self._copy(self.z + d, False).wait_recv()
            self._hand_down(self.z + d)

    def finish(self):
        for slot in range(4):
            @pl.when((self.z < 3) & (slot <= self.z))
            def _():
                self._copy(slot, True).wait_send()

            @pl.when((self.z > 0) & (slot >= self.z))
            def _():
                self._copy(slot, False).wait_send()


def turn(u, cosine, sine):
    lane = lax.broadcasted_iota(jnp.int32, u.shape, 1)
    other = jnp.where(lane % 64 < 32, pltpu.roll(u, 96, 1), pltpu.roll(u, 32, 1))
    return u * cosine + other * sine


def halves(pair, out):
    lane = lax.broadcasted_iota(jnp.int32, pair.shape, 1)
    left = lane < 64
    swapped = pltpu.roll(pair, 64, 1)
    zero = jnp.zeros_like(pair)
    out[0, 0] = jnp.where(left, pair, zero).astype(BF)
    out[0, 1] = jnp.where(left, swapped, zero).astype(BF)
    out[1, 0] = jnp.where(left, zero, swapped).astype(BF)
    out[1, 1] = jnp.where(left, zero, pair).astype(BF)


def halves_t(pair, out, here):
    pair = pair.T
    zero = jnp.zeros((64, pair.shape[1]), BF)
    for g in range(2):
        head = pair[64 * g : 64 * g + 64].astype(BF)
        out[0, g, :64, here] = head
        out[0, g, 64:, here] = zero
        out[1, g, :64, here] = zero
        out[1, g, 64:, here] = head


def key_places(kv_ref, kcol):
    rows = kcol.shape[1]
    for j in range(4):
        digit = kv_ref[j, rows:, :].astype(F32)
        places = jnp.broadcast_to(digit[0:1] * 32.0 + digit[1:2], (128, rows))
        for lo in range(0, rows, 128):
            column = places[:, lo : lo + 128].T
            kcol[j * rows + lo : j * rows + lo + 128, :128] = column
            kcol[j * rows + lo : j * rows + lo + 128, 128:] = column


def scan_rows(count, body, init):
    return lax.fori_loop(
        0, count, lambda t, carry: body(pl.ds(pl.multiple_of(t * 64, 64), 64), carry), init, unroll=4
    )


def eights(value, op):
    parts = [value[8 * j : 8 * j + 8] for j in range(value.shape[0] // 8)]
    while len(parts) > 1:
        parts = [op(parts[j], parts[j + 1]) for j in range(0, len(parts), 2)]
    return parts[0]


def front_kernel(
    x_ref, pos_ref, cos_ref, sin_ref, wq_ref, wk_ref, wv_ref, wo_ref,
    n1_ref, bq_ref, bk_ref, bv_ref, n2_ref, wg_ref, wu_ref, cot_ref,
    xn_ref, q_ref, kv_ref, lse_ref, obt_ref, mid_ref, xn2_ref,
    wkv_ref, wq_all, wo_all, vec_ref, wgu_ref, df_ref,
    wkv_own, small_f, small_own, small_all, wgu_out, kk, vvt, score, prob, kcol, *sems,
):
    place = plane()
    me = lax.axis_index("fsdp")
    z = lax.axis_index("ctx")
    rows = x_ref.shape[0]
    ff_own, ff = wg_ref.shape[1] // 8, wgu_ref.shape[2] // 2
    greet_all()
    gkv = Gather(place, wkv_own, wkv_ref, sems[0], sems[1], by_owner=True)
    gs = Gather(place, small_own, small_all, sems[2], sems[3], by_owner=True)
    gq = Gather(place, wq_ref, wq_all, sems[4], sems[5], by_owner=True)
    go = Gather(place, wo_ref, wo_all, sems[6], sems[7], by_owner=True)
    send_u, recv_u = sems[8:10]
    gk = LineGather(kv_ref, *sems[10:13])
    gd = Gather(place, cot_ref, df_ref, sems[13], sems[14])

    wkv_own[:, :128] = wk_ref[...]
    wkv_own[:, 128:] = wv_ref[...]
    gkv.start()
    small_f[...] = jnp.zeros_like(small_f)
    small_f[0:1, :112] = n1_ref[...].astype(F32)
    small_f[1:2, :112] = bq_ref[...].astype(F32)
    small_f[2:3, :16] = bk_ref[...].astype(F32)
    small_f[2:3, 128:144] = bv_ref[...].astype(F32)
    small_f[3:4, :112] = n2_ref[...].astype(F32)
    flat = small_f[...]
    row = lax.broadcasted_iota(jnp.int32, flat.shape, 0)
    placed = jnp.where(row == 2, pltpu.roll(flat, me * 16, 1), pltpu.roll(flat, me * 112, 1))
    small_own[...] = placed.astype(BF)
    gs.start()
    gq.start()
    wkv_ref[me] = wkv_own[...]
    small_all[me] = small_own[...]
    wq_all[me] = wq_ref[...]
    wo_all[me] = wo_ref[...]
    for j in range(8):
        for half, src in ((0, wg_ref), (1, wu_ref)):
            block = src[:, j * ff_own : (j + 1) * ff_own]
            wgu_out[j, :, half * ff : half * ff + ff_own] = block
            wgu_out[j, :, half * ff + ff_own : (half + 1) * ff] = jnp.zeros(
                (src.shape[0], ff - ff_own), BF
            )
    df_ref[0] = cot_ref[...]
    place_row = pos_ref[...].astype(F32)
    high = jnp.floor(place_row * (1.0 / 32.0))
    kv_ref[z, rows : rows + 1, :] = high.astype(BF)
    kv_ref[z, rows + 1 : rows + 2, :] = (place_row - 32.0 * high).astype(BF)
    kv_ref[z, rows + 2 :, :] = jnp.zeros((14, 256), BF)

    gkv.relay()
    gs.relay()
    gkv.relay_corner()
    gs.relay_corner()
    for slot in (3, 5, 7, 1):
        gkv.wait(slot)
        gs.wait(slot)
    vec = small_all[0].astype(F32)
    for j in range(1, 8):
        vec = vec + small_all[j].astype(F32)
    vec_ref[...] = vec

    def norm_one(at):
        h = x_ref[at, :].astype(F32)
        scale = lax.rsqrt(jnp.mean(h * h, axis=-1, keepdims=True) + EPSILON)
        xn_ref[at, :] = (h * scale * vec_ref[0:1, :]).astype(BF)

    tiles(rows, 32, norm_one)
    cosine, sine = cos_ref[...], sin_ref[...]
    kv = dot(xn_ref[...], wkv_ref[...].reshape(896, 256)) + vec_ref[2:3, :256]
    kv_ref[z, :rows, :128] = turn(kv[:, :128], cosine, sine).astype(BF)
    kv_ref[z, :rows, 128:] = kv[:, 128:].astype(BF)
    gk.start()

    gq.relay()
    go.start()

    mate = z + 1 - 2 * (z % 2)
    half_of = lambda k: pl.ds(pl.multiple_of(k * ff, 128), ff)
    taken, given = half_of(z % 2), half_of(1 - z % 2)
    send_z, recv_z = sems[15:17]

    def block_to(r):
        owner = peer(r)
        src, dst = wgu_out.at[owner, :, taken], wgu_ref.at[me, :, taken]
        return push(src, dst, send_u.at[r], recv_u.at[r], {"fsdp": owner})

    def block_from(r):
        src, dst = wgu_out.at[me, :, taken], wgu_ref.at[peer(r), :, taken]
        return push(src, dst, send_u.at[r], recv_u.at[r], {"fsdp": peer(r)})

    def hand_over(r):
        block = wgu_ref.at[peer(r), :, taken]
        return push(block, block, send_z.at[r], recv_z.at[r], {"ctx": mate})

    def handed(r):
        block = wgu_ref.at[peer(r), :, given]
        return push(block, block, send_z.at[r], recv_z.at[r], {"ctx": mate})

    @pl.loop(1, 8)
    def _(i):
        block_to(8 - i).start()

    wgu_ref[me] = wgu_out[me]
    gd.start()
    gk.collect(1)
    gq.relay_corner()
    for slot in (3, 5, 7, 1):
        gq.wait(slot)

    @pl.loop(0, 7)
    def _(i):
        at = pl.ds(pl.multiple_of(i * 128, 128), 128)
        q = dot(xn_ref[...], wq_all[:, :, at].reshape(896, 128)) + vec_ref[1:2, at]
        q_ref[:, at] = (turn(q, cosine, sine) * 0.125).astype(BF)

    gk.collect(2)

    gk.collect(3)
    for j in range(4):
        here = pl.ds(j * rows, rows)
        halves(kv_ref[j, :rows, :128].astype(F32), kk.at[:, :, here])
        halves_t(kv_ref[j, :rows, 128:].astype(F32), vvt, here)
    key_places(kv_ref, kcol)
    count = 4 * rows // 64

    @pl.loop(0, 7)
    def _(i):
        lanes = pl.ds(pl.multiple_of(i * 128, 128), 128)
        heads = (2 * i, 2 * i + 1)
        for half in range(2):
            score[half] = dot_t(kk[half, heads[half] // 7], q_ref[:, lanes])

        def find_top(at, tops):
            seen = kcol[at, :] <= place_row
            found = []
            for half in range(2):
                s = jnp.where(seen, score[half, at, :], NEGATIVE)
                score[half, at, :] = s
                found.append(jnp.maximum(tops[half], eights(s, jnp.maximum)))
            return tuple(found)

        start = jnp.full((8, rows), NEGATIVE, F32)
        tops = [jnp.max(top, axis=0, keepdims=True) for top in scan_rows(count, find_top, (start, start))]

        def soft(at, totals):
            found = []
            for half in range(2):
                e = jnp.exp(score[half, at, :] - tops[half])
                prob[half, at, :] = e.astype(BF)
                found.append(totals[half] + eights(e, jnp.add))
            return tuple(found)

        start = jnp.zeros((8, rows), F32)
        totals = [jnp.sum(total, axis=0, keepdims=True) for total in scan_rows(count, soft, (start, start))]
        o = None
        for half in range(2):
            lse_ref[pl.ds(heads[half], 1), :] = tops[half] + jnp.log(totals[half])
            part = dot(vvt[half, heads[half] // 7], prob[half]) * (1.0 / totals[half])
            o = part if o is None else o + part
        obt_ref[lanes, :] = o.astype(BF)

        block_from(7 - i).wait_recv()
        hand_over(7 - i).start()

        @pl.when(i == 0)
        def _():
            go.relay()

        @pl.when(i == 5)
        def _():
            go.relay_corner()
            gd.relay()

        @pl.when(i == 6)
        def _():
            gd.relay_corner()

    for slot in (3, 5, 7, 1):
        go.wait(slot)
    for lo in range(0, 896, 128):
        mid_ref[:, lo : lo + 128] = t_dot(obt_ref[...], wo_all[:, :, lo : lo + 128].reshape(896, 128))

    def norm_two(at):
        m = mid_ref[at, :] + x_ref[at, :].astype(F32)
        mid_ref[at, :] = m
        scale = lax.rsqrt(jnp.mean(m * m, axis=-1, keepdims=True) + EPSILON)
        xn2_ref[at, :] = (m * scale * vec_ref[3:4, :]).astype(BF)

    tiles(rows, 32, norm_two)

    @pl.loop(1, 8)
    def _(r):
        block_to(r).wait_send()
        hand_over(r).wait_send()
        handed(r).wait_recv()

    for slot in (1, 3, 5, 7):
        gd.wait(slot)
    for each in (gkv, gs, gq, go, gk, gd):
        each.finish()


def front(x, pos, cosine, sine, wq, wk, wv, wo, n1, bq, bk, bv, n2, wg, wu, cot):
    dma = pltpu.SemaphoreType.DMA
    vm = pl.BlockSpec(memory_space=pltpu.VMEM)
    vmem = pltpu.VMEM
    out = jax.ShapeDtypeStruct
    rows, width = x.shape
    own = wq.shape[0]
    ff = -(-(wg.shape[1] // 8) // 128) * 128
    tokens = 4 * rows
    return pl.pallas_call(
        front_kernel,
        out_shape=(
            out((rows, width), BF), out((rows, width), BF), out((4, rows + 16, 256), BF),
            out((16, rows), F32), out((width, rows), BF), out((rows, width), F32),
            out((rows, width), BF), out((8, own, 256), BF), out((8, own, width), BF),
            out((8, own, width), BF), out((16, width), F32), out((8, own, 2 * ff), BF),
            out((8, rows, width), BF),
        ),
        in_specs=[vm] * 16,
        out_specs=(vm,) * 13,
        scratch_shapes=[
            vmem((own, 256), BF), vmem((16, width), F32), vmem((16, width), BF), vmem((8, 16, width), BF),
            vmem((8, own, 2 * ff), BF), vmem((2, 2, tokens, 128), BF), vmem((2, 2, 128, tokens), BF),
            vmem((2, tokens, rows), F32), vmem((2, tokens, rows), BF), vmem((tokens, rows), F32),
            dma((7,)), dma((8,)), dma((7,)), dma((8,)), dma((7,)), dma((8,)), dma((7,)), dma((8,)),
            dma((8,)), dma((8,)), dma((4,)), dma((4,)), dma((4,)), dma((7,)), dma((8,)), dma((8,)), dma((8,)),
        ],
        compiler_params=pltpu.CompilerParams(collective_id=2, has_side_effects=True),
    )(x, pos, cosine, sine, wq, wk, wv, wo, n1, bq, bk, bv, n2, wg, wu, cot)


def middle_kernel(
    xn2_ref, pos_ref, cos_ref, sin_ref, kv_ref, lse_ref, vec_ref,
    df_hbm, wgu_hbm, wd_hbm, x_hbm, cot_hbm, mid_hbm, xn_hbm, q_hbm, obt_hbm, wkv_hbm, wq_hbm, wo_hbm,
    out_ref, gin_ref, pair_q, pair_o, pair_k, in_u, pair_d,
    x_all, part_out, core_in, tree_in, dx, core_f, tree_f, gwgu, gwd, mate_d, pair_u, mate_u,
    core_o, tree_o, core_q, tree_q, core_k, tree_k,
    own_o, mate_o, own_q, mate_q, own_k, mate_k, dkv_in, *sems,
):
    place = plane()
    me = lax.axis_index("fsdp")
    z = lax.axis_index("ctx")
    rows, width = xn2_ref.shape
    own = width // 8
    ff, ff_own = wgu_hbm.shape[1] // 2, wd_hbm.shape[0]
    tokens, keys = 8 * rows, 4 * rows
    piece = gwd.shape[1]
    loads = sems[38]
    greet_all()
    line_sems = sems[18:24]
    ld = Line(gwd, pair_d, mate_d, line_sems, 0)
    lu = Line(gwgu, pair_u, mate_u, line_sems, 4)
    lo = Line(own_o, pair_o, mate_o, line_sems, 12)
    lq = Line(own_q, pair_q, mate_q, line_sems, 13)
    lk = Line(own_k, pair_k, mate_k, line_sems, 14)
    send_all, recv_all, send_kv, recv_kv = sems[24:28]

    def feed_forward(df_ref, wgu_ref, wd, act_all, hid_all, dgu_all, dh, part, folded):
        gx = Gather(place, xn2_ref, x_all, sems[0], sems[1])
        rd = Scatter(place, part, core_in, tree_in, folded, *sems[2:6])
        gx.start()
        fetch = [
            pltpu.make_async_copy(wgu_hbm, wgu_ref, loads.at[0]),
            pltpu.make_async_copy(wd_hbm, wd.at[pl.ds(0, ff_own)], loads.at[1]),
            pltpu.make_async_copy(df_hbm, df_ref, loads.at[2]),
        ]
        for cp in fetch:
            cp.start()
        x_all[0] = xn2_ref[...]
        wd[ff_own:] = jnp.zeros((ff - ff_own, width), BF)
        fetch[0].wait()
        fetch[1].wait()
        both = lambda ref, p: ref[pl.ds(2 * p, 2)].reshape(2 * rows, ref.shape[2])

        @pl.loop(0, 4)
        def _(p):
            @pl.when(p == 1)
            def _():
                gx.relay()

            @pl.when(p == 3)
            def _():
                gx.relay_corner()

            gx.wait(2 * p + 1)
            x = both(x_all, p)
            for n in range(0, 2 * ff, 256):
                act_all[p, :, n : n + 256] = dot(x, wgu_ref[:, n : n + 256])

            def activate(at):
                gate, up = act_all[p, at, :ff], act_all[p, at, ff:]
                sig = 0.5 * jnp.tanh(0.5 * gate) + 0.5
                hid_all[p, at, :] = (gate * sig * up).astype(BF)

            tiles(2 * rows, 16, activate)
            out = dot(hid_all[p], wd[...]).astype(BF)
            part_out[pl.ds(2 * p, 2)] = out.reshape(2, rows, width)

        fetch[2].wait()
        for p in range(4):
            gwd[p] = t_dot(
                hid_all[:, :, p * piece : (p + 1) * piece].reshape(tokens, piece),
                df_ref[...].reshape(tokens, width),
            ).astype(BF)
            ld.start(p)

        @pl.loop(0, 4)
        def _(k):
            p = 3 - k
            dh[...] = dot_t(both(df_ref, p), wd[...])

            def activate(at):
                gate, up, d = act_all[p, at, :ff], act_all[p, at, ff:], dh[at, :]
                sig = 0.5 * jnp.tanh(0.5 * gate) + 0.5
                dgu_all[p, at, :ff] = (d * up * (sig * (1.0 + gate * (1.0 - sig)))).astype(BF)
                dgu_all[p, at, ff:] = (d * (gate * sig)).astype(BF)

            tiles(2 * rows, 16, activate)
            value = dot_t(dgu_all[p], wgu_ref[...]).astype(BF)
            part[pl.ds(2 * p, 2)] = value.reshape(2, rows, width)
            rd.to_twin(p).start()

            @pl.when(k == 1)
            def _():
                rd.start_corner()

            @pl.when(k == 2)
            def _():
                ld.meet(0)

        rd.start_far()
        ld.meet(1)
        rd.relay()

        @pl.loop(0, 2 * ff // 256)
        def _(n):
            at = pl.ds(pl.multiple_of(n * 256, 256), 256)
            value = t_dot(x_all[...].reshape(tokens, width), dgu_all[:, :, at].reshape(tokens, 256))
            gwgu[:, :, at] = value.astype(BF).reshape(8, own, 256)

            @pl.when(n == 1)
            def _():
                ld.meet(2)

            @pl.when(n == 3)
            def _():
                ld.settle(0)

        for r in (7, 6, 5, 4):
            lu.start(peer(r))

        def store_dx(at, value):
            dx[at, :] = value

        rd.total(store_dx)
        gx.finish()
        rd.finish()

    pl.run_scoped(
        feed_forward,
        pltpu.VMEM((8, rows, width), BF), pltpu.VMEM((width, 2 * ff), BF), pltpu.VMEM((ff, width), BF),
        pltpu.VMEM((4, 2 * rows, 2 * ff), F32), pltpu.VMEM((4, 2 * rows, ff), BF),
        pltpu.VMEM((4, 2 * rows, 2 * ff), BF), pltpu.VMEM((2 * rows, ff), F32),
        pltpu.VMEM((8, rows, width), BF), pltpu.VMEM((3, rows, width), BF),
    )

    def attention_back(
        x_ref, cot_ref, mid_ref, xn_ref, q_ref, obt_ref, wkv_ref, wq_ref, wo_ref,
        dm, da, dob, kk, kkt, vv, kcol, score, dprob, prob, dscore, dk_acc, dv_acc,
        dq, dkv_own, dkv, dxn, small, part_o, fold_o, part_q, fold_q, part_k, fold_k, fold_f,
    ):
        ro = Scatter(place, part_o, core_o, tree_o, fold_o, *sems[6:10], by_owner=True)
        rq = Scatter(place, part_q, core_q, tree_q, fold_q, *sems[10:14], by_owner=True)
        rk = Scatter(place, part_k, core_k, tree_k, fold_k, *sems[14:18], by_owner=True)
        rf = Scatter(place, part_out, core_f, tree_f, fold_f, *sems[28:32])
        arrays = (
            (mid_hbm, mid_ref), (cot_hbm, cot_ref), (obt_hbm, obt_ref), (wo_hbm, wo_ref), (q_hbm, q_ref),
            (xn_hbm, xn_ref), (wq_hbm, wq_ref), (wkv_hbm, wkv_ref), (x_hbm, x_ref),
        )
        fetch = [pltpu.make_async_copy(src, dst, loads.at[3 + i]) for i, (src, dst) in enumerate(arrays)]
        for cp in fetch:
            cp.start()
        for k in (3, 2, 1, 0):
            rf.to_twin(k).start()
        ld.meet(3)
        ld.settle(1)
        fetch[0].wait()
        fetch[1].wait()

        small[...] = jnp.zeros_like(small)

        def norm_two(at):
            m, g = mid_ref[at, :], dx[at, :]
            scale = lax.rsqrt(jnp.mean(m * m, axis=-1, keepdims=True) + EPSILON)
            weighted = vec_ref[3:4, :] * g
            inner = jnp.mean(weighted * m, axis=-1, keepdims=True)
            d = cot_ref[at, :].astype(F32) + scale * weighted - m * (scale * scale * scale) * inner
            dm[at, :] = d
            da[at, :] = d.astype(BF)
            small[3:4, :] += jnp.sum(g * m * scale, axis=0, keepdims=True)

        tiles(rows, 32, norm_two)
        for i in range(2, 9):
            fetch[i].wait()

        @pl.loop(0, 7)
        def _(i):
            lanes = pl.ds(pl.multiple_of(i * 128, 128), 128)
            part_o[:, :, lanes] = dot(obt_ref[...], da[:, lanes]).astype(BF).reshape(8, own, 128)

        for k in (3, 2, 1, 0):
            ro.to_twin(k).start()
        dob[...] = dot_t(da[...], wo_ref[...].reshape(width, width)).astype(BF)
        for j in range(4):
            here = pl.ds(j * rows, rows)
            key, value = kv_ref[j, :rows, :128].astype(F32), kv_ref[j, :rows, 128:].astype(F32)
            halves(key, kk.at[:, :, here])
            halves(value, vv.at[:, :, here])
            halves_t(key, kkt, here)
        key_places(kv_ref, kcol)
        dk_acc[...] = jnp.zeros_like(dk_acc)
        dv_acc[...] = jnp.zeros_like(dv_acc)
        place_row = pos_ref[...].astype(F32)
        cosine, sine = cos_ref[...], -sin_ref[...]
        count = keys // 64

        def keep(total):
            def store(at, value):
                total[0, at, :] = value.astype(BF)

            return store

        def gather_to(r):
            owner = peer(r)
            return push(pair_u.at[owner], in_u.at[me], send_all.at[r], recv_all.at[me], {"fsdp": owner})

        def settle_u(r):
            lu.settle(peer(r))
            gather_to(r).start()

        ld.settle(2)

        @pl.loop(0, 7)
        def _(i):
            lanes = pl.ds(pl.multiple_of(i * 128, 128), 128)
            grad = None
            for half in range(2):
                head = 2 * i + half
                g = head // 7
                score[...] = dot_t(kk[half, g], q_ref[:, lanes])
                dprob[...] = dot_t(vv[half, g], dob[:, lanes])
                lse_row = lse_ref[pl.ds(head, 1), :]

                def find_delta(at, total):
                    s = jnp.where(kcol[at, :] <= place_row, score[at, :], NEGATIVE)
                    p = jnp.exp(s - lse_row)
                    score[at, :] = p
                    prob[at, :] = p.astype(BF)
                    return total + eights(p * dprob[at, :], jnp.add)

                delta = scan_rows(count, find_delta, jnp.zeros((8, rows), F32))
                delta = jnp.sum(delta, axis=0, keepdims=True)

                def find_score(at):
                    dscore[at, :] = (score[at, :] * (dprob[at, :] - delta)).astype(BF)

                tiles(keys, 64, find_score)
                dv_acc[half, g] += dot(prob[...], dob[:, lanes])
                dk_acc[half, g] += dot(dscore[...], q_ref[:, lanes])
                term = dot(kkt[half, g], dscore[...])
                grad = term if grad is None else grad + term
            dq[:, lanes] = turn(grad.T * 0.125, cosine, sine).astype(BF)

            @pl.when(i == 0)
            def _():
                ro.start()
                rf.start()
                lu.meet(peer(7))

            @pl.when(i == 1)
            def _():
                ld.settle(3)

            @pl.when(i == 2)
            def _():
                lu.meet(peer(6))

            @pl.when(i == 3)
            def _():
                ro.relay()
                rf.relay()
                settle_u(7)

            @pl.when(i == 4)
            def _():
                lu.meet(peer(5))

            @pl.when(i == 5)
            def _():
                settle_u(6)
                ro.total(keep(own_o))

            @pl.when(i == 6)
            def _():
                lu.meet(peer(4))

        lane = lax.broadcasted_iota(jnp.int32, (64, 128), 1)

        def join(acc, at):
            first = jnp.where(lane < 64, acc[0, 0, at, :], acc[1, 1, at, :])
            second = jnp.where(lane < 64, acc[0, 1, at, :], acc[1, 0, at, :])
            return first + pltpu.roll(second, 64, 1)

        @pl.loop(0, 4)
        def _(j):
            for first in range(0, rows, 64):
                at = pl.ds(pl.multiple_of(j * rows + first, 64), 64)
                dkv_own[j, first : first + 64, :128] = join(dk_acc, at).astype(BF)
                dkv_own[j, first : first + 64, 128:] = join(dv_acc, at).astype(BF)

        def kv_to(d):
            other = (z + d) % 4
            return push(
                dkv_own.at[other], dkv_in.at[d - 1], send_kv.at[d - 1], recv_kv.at[d - 1], {"ctx": other}
            )

        for d in (2, 1, 3):
            kv_to(d).start()

        @pl.loop(4, 8)
        def _(i):
            lu.start(peer(7 - i))

        lo.start(0)
        settle_u(5)

        def weight_grads(grads, part, n):
            for at in range(0, n, 128):
                value = t_dot(xn_ref[...], grads[:, at : at + 128]).astype(BF)
                part[:, :, at : at + 128] = value.reshape(8, own, 128)

        weight_grads(dq, part_q, width)
        for k in (3, 2, 1, 0):
            rq.to_twin(k).start()
        for at in range(0, width, 128):
            wq_rows = wq_ref[...].reshape(width, width)
            dxn[:, at : at + 128] = dot_t(dq[...], wq_rows[at : at + 128])
        rq.start()
        settle_u(4)

        def store_out(at, value):
            out_ref[at, :] = value + mid_ref[at, :]

        rf.total(store_out)
        for d in (1, 3, 2):
            kv_to(d).wait_recv()

        def sum_kv(at):
            value = dkv_own[z, at, :].astype(F32)
            for d in range(3):
                value = value + dkv_in[d, at, :].astype(F32)
            dkv[at, :128] = turn(value[:, :128], cos_ref[at, :], -sin_ref[at, :]).astype(BF)
            dkv[at, 128:] = value[:, 128:].astype(BF)

        tiles(rows, 32, sum_kv)
        weight_grads(dkv, part_k, 256)
        for at in range(0, width, 128):
            wkv_rows = wkv_ref[...].reshape(width, 256)
            dxn[:, at : at + 128] += dot_t(dkv[...], wkv_rows[at : at + 128])

        def norm_one(at):
            h, g = x_ref[at, :].astype(F32), dxn[at, :]
            scale = lax.rsqrt(jnp.mean(h * h, axis=-1, keepdims=True) + EPSILON)
            weighted = vec_ref[0:1, :] * g
            inner = jnp.mean(weighted * h, axis=-1, keepdims=True)
            gin_ref[at, :] = dm[at, :] + scale * weighted - h * (scale * scale * scale) * inner
            small[0:1, :] += jnp.sum(g * h * scale, axis=0, keepdims=True)
            small[1:2, :] += jnp.sum(dq[at, :].astype(F32), axis=0, keepdims=True)
            small[2:3, :256] += jnp.sum(dkv[at, :].astype(F32), axis=0, keepdims=True)

        tiles(rows, 32, norm_one)
        flat = small[...]
        line_of = lax.broadcasted_iota(jnp.int32, (16, 128), 0)
        for j in range(8):
            by_row = pltpu.roll(flat, (width - 112 * j) % width, 1)[:, :128]
            by_head = pltpu.roll(flat, (width - 16 * j) % width, 1)
            value = jnp.where(line_of == 2, by_head[:, :128], by_row)
            lifted = pltpu.roll(by_head[:, 128:256], 2, 0)
            value = jnp.where(line_of == 4, lifted, value)
            part_k[j, :16, 256:] = value.astype(BF)
            part_k[j, 16:, 256:] = jnp.zeros((own - 16, 128), BF)

        for k in (3, 2, 1, 0):
            rk.to_twin(k).start()
        lu.meet(peer(3))
        rk.start()
        rq.relay()
        lu.meet(peer(2))
        settle_u(3)
        rk.relay()
        rq.total(keep(own_q))
        lq.start(0)
        lu.meet(peer(1))
        rk.total(keep(own_k))
        lk.start(0)
        settle_u(2)
        lu.meet(me)
        settle_u(1)
        lo.meet(0)
        lu.settle(me)
        keep_own = pltpu.make_async_copy(pair_u.at[me], in_u.at[me], loads.at[12])
        keep_own.start()
        lq.meet(0)
        lo.settle(0)
        lk.meet(0)
        lq.settle(0)
        lk.settle(0)
        keep_own.wait()

        @pl.loop(1, 8)
        def _(r):
            other = peer(r)
            push(
                pair_u.at[me], in_u.at[other], send_all.at[r], recv_all.at[other], {"fsdp": other}
            ).wait_recv()
            gather_to(r).wait_send()

        for d in (1, 2, 3):
            kv_to(d).wait_send()
        for each in (ro, rq, rk, rf):
            each.finish()

    v = pltpu.VMEM
    pl.run_scoped(
        attention_back,
        v((rows, width), BF), v((rows, width), BF), v((rows, width), F32), v((rows, width), BF),
        v((rows, width), BF), v((width, rows), BF), v((8, own, 256), BF), v((8, own, width), BF),
        v((8, own, width), BF),
        v((rows, width), F32), v((rows, width), BF), v((rows, width), BF),
        v((2, 2, keys, 128), BF), v((2, 2, 128, keys), BF), v((2, 2, keys, 128), BF),
        v((keys, rows), F32), v((keys, rows), F32), v((keys, rows), F32),
        v((keys, rows), BF), v((keys, rows), BF),
        v((2, 2, keys, 128), F32), v((2, 2, keys, 128), F32),
        v((rows, width), BF), v((4, rows, 256), BF), v((rows, 256), BF), v((rows, width), F32),
        v((16, width), F32),
        v((8, own, width), BF), v((3, own, width), BF), v((8, own, width), BF), v((3, own, width), BF),
        v((8, own, 384), BF), v((3, own, 384), BF), v((3, rows, width), BF),
    )

    @pl.loop(0, 4)
    def _(p):
        ld.finish(p)

    @pl.loop(0, 8)
    def _(p):
        lu.finish(p)

    for each in (lo, lq, lk):
        each.finish(0)


def middle(xn2, pos, cosine, sine, kv, lse, vec, df_all, wgu, wd, x, cot, mid, xn, q, obt, wkv, wq, wo):
    dma = pltpu.SemaphoreType.DMA
    vm = pl.BlockSpec(memory_space=pltpu.VMEM)
    hbm = pl.BlockSpec(memory_space=pl.ANY)
    v = pltpu.VMEM
    out = jax.ShapeDtypeStruct
    rows, width = x.shape
    own = width // 8
    ff = wgu.shape[1] // 2
    gu, gd = (8, own, 2 * ff), (4, ff // 4, width)
    wide, narrow = (1, own, width), (1, own, 384)
    tree = [dma((4,)), dma((4,)), dma((3,)), dma((3,))]
    return pl.pallas_call(
        middle_kernel,
        out_shape=(
            out((rows, width), F32), out((rows, width), F32), out(wide, BF), out(wide, BF), out(narrow, BF),
            out(gu, BF), out(gd, BF),
        ),
        in_specs=[vm] * 7 + [hbm] * 12,
        out_specs=(vm, vm, vm, vm, vm, hbm, vm),
        scratch_shapes=[
            v((8, rows, width), BF), v((8, rows, width), BF), v((4, rows, width), BF), v((3, rows, width), BF),
            v((rows, width), F32), v((4, rows, width), BF), v((3, rows, width), BF),
            v(gu, BF), v(gd, BF), v(gd, BF), v(gu, BF), v(gu, BF),
            v((4, own, width), BF), v((3, own, width), BF), v((4, own, width), BF), v((3, own, width), BF),
            v((4, own, 384), BF), v((3, own, 384), BF),
            v(wide, BF), v(wide, BF), v(wide, BF), v(wide, BF), v(narrow, BF), v(narrow, BF),
            v((3, rows, 256), BF),
            dma((7,)), dma((8,)), *tree, *tree, *tree, *tree,
            *[dma((15,))] * 6,
            dma((8,)), dma((8,)), dma((3,)), dma((3,)), *tree,
            *[dma((1,))] * 6, dma((13,)),
        ],
        compiler_params=pltpu.CompilerParams(
            collective_id=0, has_side_effects=True, vmem_limit_bytes=67043328
        ),
    )(xn2, pos, cosine, sine, kv, lse, vec, df_all, wgu, wd, x, cot, mid, xn, q, obt, wkv, wq, wo)


def results_kernel(
    out_ref, gin_ref, tq_ref, to_ref, tk_ref, tu_ref, td_ref,
    o_ref, i_ref, n1_ref, q_ref, bq_ref, k_ref, bk_ref, v_ref, bv_ref, w_ref, n2_ref, g_ref, u_ref, d_ref,
):
    o_ref[...] = out_ref[...]
    i_ref[...] = gin_ref[...]
    q_ref[...] = tq_ref[0].astype(F32)
    w_ref[...] = to_ref[0].astype(F32)
    k_ref[...] = tk_ref[0, :, :128].astype(F32)
    v_ref[...] = tk_ref[0, :, 128:256].astype(F32)
    small = tk_ref[0, :16, 256:].astype(F32)
    for i, ref in enumerate((n1_ref, bq_ref, bk_ref, n2_ref, bv_ref)):
        ref[...] = small[i : i + 1, : ref.shape[1]]
    ff_own, ff = d_ref.shape[0], tu_ref.shape[2] // 2
    for j in range(8):
        def place_block(at):
            g_ref[at, j * ff_own : (j + 1) * ff_own] = tu_ref[j, at, :ff_own].astype(F32)
            u_ref[at, j * ff_own : (j + 1) * ff_own] = tu_ref[j, at, ff : ff + ff_own].astype(F32)

        tiles(tu_ref.shape[1], 16, place_block)
    rows = td_ref.shape[1]
    for p in range(4):
        count = min(rows, ff_own - p * rows)
        d_ref[p * rows : p * rows + count] = td_ref[p, :count].astype(F32)


def results(out, gin, tq, to, tk, tu, td, ff_own):
    vm = pl.BlockSpec(memory_space=pltpu.VMEM)
    rows, width = out.shape
    own = width // 8
    shapes = (
        (rows, width), (rows, width), (1, own), (own, 896), (1, own), (own, 128), (1, 16), (own, 128), (1, 16),
        (own, 896), (1, own), (own, 8 * ff_own), (own, 8 * ff_own), (ff_own, width),
    )
    return pl.pallas_call(
        results_kernel,
        out_shape=tuple(jax.ShapeDtypeStruct(shape, F32) for shape in shapes),
        in_specs=[vm] * 7,
        out_specs=(vm,) * 14,
    )(out, gin, tq, to, tk, tu, td)


def shards(
    inputs, positions, cotangent, norm_one, w_query, b_query, key_projection, b_key,
    value_projection, value_bias, w_out, norm_two, w_gate, w_up, w_down,
):
    places = positions[0]
    turned = angles_of(places)
    cosine, sine = jnp.cos(turned), jnp.sin(turned)
    sine = jnp.where(jnp.arange(128)[None, :] % 64 < 32, -sine, sine)
    own = w_query.shape[1]
    ff_own = w_down.shape[1]
    ff = -(-ff_own // 128) * 128
    x, cot = inputs[0], cotangent[0]
    xn, q, kv, lse, obt, mid, xn2, wkv, wq, wo, vec, wgu, df_all = front(
        x, positions, cosine, sine, w_query[0], key_projection[0], value_projection[0], w_out[0],
        norm_one, b_query, b_key, value_bias, norm_two, w_gate[0], w_up[0], cot,
    )
    totals = middle(
        xn2, positions, cosine, sine, kv, lse, vec, df_all, wgu.reshape(-1, 2 * ff), w_down[0],
        x, cot, mid, xn, q, obt, wkv, wq, wo,
    )
    matrix = lambda i: i in (0, 1, 3, 5, 7, 9, 11, 12, 13)
    return tuple(g[None] if matrix(i) else g for i, g in enumerate(results(*totals, ff_own)))


def angles_of(places):
    half = HEAD_SIZE // 2
    inverse = jnp.exp(jnp.arange(half, dtype=F32) * (-2.0 * math.log(ROPE_BASE) / HEAD_SIZE))
    return places.astype(F32)[:, None] * jnp.concatenate([inverse] * 4)[None, :]


def shards_general(
    inputs, positions, cotangent, norm_one, w_query, b_query, key_projection, b_key,
    value_projection, value_bias, w_out, norm_two, w_gate, w_up, w_down,
):
    rows = inputs.shape[1]
    width = inputs.shape[2]
    group = QUERY_HEADS // KEY_VALUE_HEADS
    q_cols = w_query.shape[2]
    kv_cols = key_projection.shape[2]
    score_scale = 1.0 / math.sqrt(HEAD_SIZE)

    places = positions[0]
    key_places = lax.all_gather(places, "ctx", axis=0, tiled=True)
    cosine, sine = angles(places)
    hidden = inputs[0].astype(F32)

    packed = jnp.concatenate([w_query[0], key_projection[0], value_projection[0], w_out[0]], axis=1)
    packed = lax.all_gather(packed, "fsdp", axis=0, tiled=True)
    w_qkv = packed[:, : q_cols + 2 * kv_cols]
    w_o = packed[:, q_cols + 2 * kv_cols :]
    small = jnp.concatenate([norm_one[0], b_query[0], b_key[0], value_bias[0], norm_two[0]])
    small = lax.all_gather(small, "fsdp", axis=0).astype(F32)
    cuts, at = [], 0
    for piece in (norm_one, b_query, b_key, value_bias, norm_two):
        n = piece.shape[1]
        cuts.append(small[:, at : at + n].reshape(-1))
        at += n
    gain_one, bias_q, bias_k, bias_v, gain_two = cuts
    bias = jnp.concatenate([bias_q, bias_k, bias_v])

    grad_branch = cotangent[0]
    df_all = lax.all_gather(grad_branch, "fsdp", axis=0, tiled=True)
    wg = lax.all_to_all(w_gate[0], "fsdp", split_axis=1, concat_axis=0, tiled=True)
    wu = lax.all_to_all(w_up[0], "fsdp", split_axis=1, concat_axis=0, tiled=True)
    wd = w_down[0]

    scale_one, normed = norm_rows(hidden, gain_one)
    qkv = dot(normed, w_qkv) + bias
    q = rotate(qkv[:, :q_cols].reshape(rows, QUERY_HEADS, HEAD_SIZE), cosine, sine).astype(BF)
    k = rotate(
        qkv[:, q_cols : q_cols + kv_cols].reshape(rows, KEY_VALUE_HEADS, HEAD_SIZE), cosine, sine
    ).astype(BF)
    v = qkv[:, q_cols + kv_cols :].astype(BF)
    kv = jnp.concatenate([k.reshape(rows, kv_cols), v], axis=1)
    kv = lax.all_gather(kv, "ctx", axis=0, tiled=True)
    total = kv.shape[0]
    k_all = kv[:, :kv_cols].reshape(total, KEY_VALUE_HEADS, HEAD_SIZE)
    v_all = kv[:, kv_cols:].reshape(total, KEY_VALUE_HEADS, HEAD_SIZE)
    q = q.reshape(rows, KEY_VALUE_HEADS, group, HEAD_SIZE)
    s = jnp.einsum("tgjd,ugd->gjtu", q, k_all, preferred_element_type=F32) * score_scale
    s = jnp.where(key_places[None, :] <= places[:, None], s, NEGATIVE)
    top = jnp.max(s, axis=-1, keepdims=True)
    lse = top + jnp.log(jnp.sum(jnp.exp(s - top), axis=-1, keepdims=True))
    pf = jnp.exp(s - lse)
    p = pf.astype(BF)
    o = jnp.einsum("gjtu,ugd->tgjd", p, v_all, preferred_element_type=F32)
    ob = o.reshape(rows, q_cols).astype(BF)
    middle = hidden + dot(ob, w_o)
    scale_two, normed_two = norm_rows(middle, gain_two)

    x_all = lax.all_gather(normed_two, "fsdp", axis=0, tiled=True)
    gate = dot(x_all, wg)
    up = dot(x_all, wu)
    sig = jax.nn.sigmoid(gate)
    hid = (gate * sig * up).astype(BF)
    out_part = dot(hid, wd).astype(BF)
    ffn_out = lax.psum_scatter(out_part, "fsdp", scatter_dimension=0, tiled=True)
    output = middle + ffn_out.astype(F32)

    dhid = dot_t(df_all, wd)
    dgate = (dhid * up * sig * (1.0 + gate * (1.0 - sig))).astype(BF)
    dup = (dhid * (gate * sig)).astype(BF)
    dx_part = (dot_t(dgate, wg) + dot_t(dup, wu)).astype(BF)
    dxn2 = lax.psum_scatter(dx_part, "fsdp", scatter_dimension=0, tiled=True).astype(F32)
    g_down = t_dot(hid, df_all)
    g_gate = t_dot(x_all, dgate)
    g_up = t_dot(x_all, dup)

    g_out = grad_branch.astype(F32)
    grad_gain_two, dmid = norm_back(middle, scale_two, gain_two, dxn2)
    dm = g_out + dmid
    da = dm.astype(BF)
    g_wo = t_dot(ob, da)
    dob = dot_t(da, w_o).astype(BF).reshape(rows, KEY_VALUE_HEADS, group, HEAD_SIZE)

    dp = jnp.einsum("tgjd,ugd->gjtu", dob, v_all, preferred_element_type=F32)
    delta = jnp.sum(pf * dp, axis=-1, keepdims=True)
    ds = (pf * (dp - delta)).astype(BF)
    dq = jnp.einsum("gjtu,ugd->tgjd", ds, k_all, preferred_element_type=F32) * score_scale
    dk = jnp.einsum("gjtu,tgjd->ugd", ds, q, preferred_element_type=F32) * score_scale
    dv = jnp.einsum("gjtu,tgjd->ugd", p, dob, preferred_element_type=F32)
    dkv = jnp.concatenate([dk.reshape(total, kv_cols), dv.reshape(total, kv_cols)], axis=1)
    dkv = lax.psum_scatter(dkv, "ctx", scatter_dimension=0, tiled=True)
    dq = rotate(dq.reshape(rows, QUERY_HEADS, HEAD_SIZE), cosine, -sine).astype(BF)
    dk = rotate(
        dkv[:, :kv_cols].reshape(rows, KEY_VALUE_HEADS, HEAD_SIZE), cosine, -sine
    ).astype(BF)
    dqkv = jnp.concatenate(
        [dq.reshape(rows, q_cols), dk.reshape(rows, kv_cols), dkv[:, kv_cols:].astype(BF)], axis=1
    )
    g_qkv = t_dot(normed, dqkv)
    g_bias = jnp.sum(dqkv.astype(F32), axis=0)
    dxn = dot_t(dqkv, w_qkv)
    grad_gain_one, dhidden = norm_back(hidden, scale_one, gain_one, dxn)
    grad_in = dm + dhidden

    g_attn = jnp.concatenate([g_qkv, g_wo], axis=1).astype(BF)
    g_attn = lax.psum_scatter(g_attn, "fsdp", scatter_dimension=0, tiled=True)
    back = [
        lax.all_to_all(g.astype(BF), "fsdp", split_axis=0, concat_axis=1, tiled=True)
        for g in (g_gate, g_up)
    ]
    g_attn, g_gate, g_up, g_down = lax.psum((g_attn, back[0], back[1], g_down.astype(BF)), "ctx")
    pieces = jnp.concatenate(
        [
            g.reshape(small.shape[0], -1)
            for g in (
                grad_gain_one, g_bias[:q_cols], g_bias[q_cols : q_cols + kv_cols],
                g_bias[q_cols + kv_cols :], grad_gain_two,
            )
        ],
        axis=1,
    )
    pieces = lax.psum(pieces, ("ctx", "fsdp"))
    mine = lax.dynamic_slice_in_dim(pieces, lax.axis_index("fsdp"), 1, axis=0)
    outs, at = [], 0
    for piece in (norm_one, b_query, b_key, value_bias, norm_two):
        n = piece.shape[1]
        outs.append(mine[:, at : at + n])
        at += n
    g_n1, g_bq, g_bk, g_bv, g_n2 = outs
    g_attn = g_attn.astype(F32)
    return (
        output[None], grad_in[None], g_n1,
        g_attn[None, :, :q_cols], g_bq,
        g_attn[None, :, q_cols : q_cols + kv_cols], g_bk,
        g_attn[None, :, q_cols + kv_cols : q_cols + 2 * kv_cols], g_bv,
        g_attn[None, :, q_cols + 2 * kv_cols :], g_n2,
        g_gate.astype(F32)[None], g_up.astype(F32)[None], g_down.astype(F32)[None],
    )


def solution(mesh):
    tok, row, vec = P("fsdp", "ctx", None), P(None, "fsdp", None), P(None, "fsdp")
    fast = mesh.shape["ctx"] == 4 and mesh.shape["fsdp"] == 8
    return jax.shard_map(
        shards if fast else shards_general,
        mesh=mesh,
        in_specs=(
            tok, P("fsdp", "ctx"), tok, vec, row, vec, row, vec, row, vec, row, vec, row, row, row,
        ),
        out_specs=(tok, tok, vec, row, vec, row, vec, row, vec, row, vec, row, row, row),
        check_vma=False,
    )
```

```python
import functools
import math

import jax
import jax.numpy as jnp
from jax import lax
from jax.experimental import pallas as pl
from jax.experimental.pallas import tpu as pltpu
from jax.sharding import PartitionSpec as P

QUERY_HEADS = 14
KEY_VALUE_HEADS = 2
HEAD_SIZE = 64
ROPE_BASE = 1000000.0
EPSILON = 1e-06
NEGATIVE = -1e30
BF = jnp.bfloat16
F32 = jnp.float32
MESH = pl.DeviceIdType.MESH


def angles(places):
    half = HEAD_SIZE // 2
    inverse = jnp.exp(jnp.arange(half, dtype=F32) * (-2.0 * math.log(ROPE_BASE) / HEAD_SIZE))
    turned = places.astype(F32)[:, None] * inverse[None, :]
    return jnp.cos(turned)[:, None, :], jnp.sin(turned)[:, None, :]


def rotate(u, cosine, sine):
    half = u.shape[-1] // 2
    a, b = u[..., :half], u[..., half:]
    return jnp.concatenate([a * cosine - b * sine, b * cosine + a * sine], axis=-1)


def norm_rows(hidden, gain):
    scale = lax.rsqrt(jnp.mean(hidden * hidden, axis=-1, keepdims=True) + EPSILON)
    return scale, (hidden * scale * gain).astype(BF)


def norm_back(hidden, scale, gain, grad):
    weighted = gain * grad
    grad_gain = jnp.sum(grad * hidden * scale, axis=0)
    inner = jnp.mean(weighted * hidden, axis=-1, keepdims=True)
    return grad_gain, scale * weighted - hidden * (scale * scale * scale) * inner


def dot(a, b):
    return jnp.dot(a, b, preferred_element_type=F32)


def dot_t(a, b):
    return lax.dot_general(a, b, (((1,), (1,)), ((), ())), preferred_element_type=F32)


def t_dot(a, b):
    return lax.dot_general(a, b, (((0,), (0,)), ((), ())), preferred_element_type=F32)


def plane():
    f = lax.axis_index("fsdp")
    core, x, y = f % 2, (f // 2) % 2, f // 4
    by_x, by_y = f + 2 - 4 * x, f + 4 - 8 * y
    twin = f + 1 - 2 * core
    near = by_x + core * (by_y - by_x)
    far = by_y + core * (by_x - by_y)
    return twin, near, far, 2 + 2 * core, 4 - 2 * core


def tiles(rows, step, body):
    count = rows // step
    unroll = count if count <= 10 else 4

    @pl.loop(0, count, unroll=unroll)
    def _(r):
        body(pl.ds(pl.multiple_of(r * step, step), step))


def peer(r):
    f = lax.axis_index("fsdp")
    core, x, y = f % 2, (f // 2) % 2, f // 4
    return f + (r % 2) * (1 - 2 * core) + ((r // 2) % 2) * (2 - 4 * x) + (r // 4) * (4 - 8 * y)


def greet(others):
    barrier = pltpu.get_barrier_semaphore()
    for other in others:
        pl.semaphore_signal(barrier, inc=1, device_id=other, device_id_type=MESH)
    pl.semaphore_wait(barrier, len(others))


def push(src, dst, send, recv, other):
    return pltpu.make_async_remote_copy(
        src_ref=src, dst_ref=dst, send_sem=send, recv_sem=recv, device_id=other, device_id_type=MESH
    )


class Gather:
    def __init__(self, place, mine, full, send, recv, by_owner=False):
        self.twin, self.near, self.far, self.s_near, self.s_far = place
        self.mine, self.full, self.send, self.recv = mine, full, send, recv
        self.by_owner = by_owner

    def copy(self, i):
        twin, near, far = self.twin, self.near, self.far
        here = (0, 0, 0, self.s_near, 2, 4, 6)[i]
        there, other = (
            (self.s_near, near), (self.s_far, far), (1, twin), (6, far), (3, twin), (5, twin), (7, twin)
        )[i]
        if self.by_owner:
            here = there = peer(here)
        src = self.mine if i < 3 else self.full.at[here]
        return push(src, self.full.at[there], self.send.at[i], self.recv.at[there], {"fsdp": other})

    def start(self):
        for i in range(3):
            self.copy(i).start()

    def wait(self, slot):
        slot = peer(slot) if self.by_owner else slot
        full = self.full.at[slot]
        push(full, full, self.send.at[0], self.recv.at[slot], {"fsdp": self.near}).wait_recv()

    def relay(self):
        self.wait(2)
        self.wait(4)
        for i in range(3, 6):
            self.copy(i).start()

    def relay_corner(self):
        self.wait(6)
        self.copy(6).start()

    def finish(self):
        for i in range(7):
            self.copy(i).wait_send()


class Scatter:
    def __init__(
        self, place, part, core_in, tree_in, folded, send_core, recv_core, send_tree, recv_tree,
        by_owner=False,
    ):
        self.twin, self.near, self.far, self.s_near, self.s_far = place
        self.at = peer if by_owner else lambda slot: slot
        self.part, self.core_in, self.tree_in, self.folded = part, core_in, tree_in, folded
        self.send_core, self.recv_core = send_core, recv_core
        self.send_tree, self.recv_tree = send_tree, recv_tree

    def to_twin(self, k):
        return push(
            self.part.at[self.at(2 * k + 1)], self.core_in.at[k], self.send_core.at[k], self.recv_core.at[k],
            {"fsdp": self.twin},
        )

    def tree(self, j):
        other = (self.far, self.near, self.far)[j]
        return push(
            self.folded.at[j], self.tree_in.at[j], self.send_tree.at[j], self.recv_tree.at[j],
            {"fsdp": other},
        )

    def fold(self, j, slot, corner=False):
        part, core_in, tree_in, folded = self.part, self.core_in, self.tree_in, self.folded
        k = slot // 2
        slot = self.at(slot)

        def add(at):
            value = part[slot, at, :].astype(F32) + core_in[k, at, :].astype(F32)
            if corner:
                value = value + tree_in[0, at, :].astype(F32)
            folded[j, at, :] = value.astype(BF)

        tiles(part.shape[1], 16, add)

    def start_corner(self):
        self.to_twin(3).wait_recv()
        self.fold(0, 6)
        self.tree(0).start()

    def start_far(self):
        self.to_twin(1).wait_recv()
        self.to_twin(2).wait_recv()
        self.fold(2, self.s_far)
        self.tree(2).start()

    def start(self):
        self.start_corner()
        self.start_far()

    def relay(self):
        self.tree(0).wait_recv()
        self.fold(1, self.s_near, True)
        self.tree(1).start()

    def total(self, store):
        part, core_in, tree_in = self.part, self.core_in, self.tree_in
        mine = self.at(0)
        self.to_twin(0).wait_recv()
        self.tree(1).wait_recv()
        self.tree(2).wait_recv()

        def add(at):
            value = part[mine, at, :].astype(F32) + core_in[0, at, :].astype(F32)
            store(at, value + tree_in[1, at, :].astype(F32) + tree_in[2, at, :].astype(F32))

        tiles(part.shape[1], 16, add)

    def finish(self):
        for k in range(4):
            self.to_twin(k).wait_send()
        for j in range(3):
            self.tree(j).wait_send()


def line():
    z = lax.axis_index("ctx")
    inner = (z == 1) | (z == 2)
    return z, inner, z + 1 - 2 * (z // 3), 3 * (z // 2), 3 - z


class Line:
    def __init__(self, own, pair, mate, sems, first=0):
        self.own, self.pair, self.mate = own, pair, mate
        self.sems, self.first = sems, first
        self.z, self.inner, self.to_inner, self.to_outer, self.to_mate = line()

    def _copy(self, k, p):
        src, dst, other = (
            (self.own, self.pair, self.to_inner),
            (self.pair, self.mate, self.to_mate),
            (self.pair, self.pair, self.to_outer),
        )[k]
        i = self.first + p
        return push(src.at[p], dst.at[p], self.sems[2 * k].at[i], self.sems[2 * k + 1].at[i], {"ctx": other})

    def _rows(self, body):
        tiles(self.own.shape[1], 16, body)

    def start(self, p):
        @pl.when(~self.inner)
        def _():
            self._copy(0, p).start()

    def meet(self, p):
        own, pair = self.own, self.pair

        @pl.when(self.inner)
        def _():
            self._copy(0, p).wait_recv()

            def add(at):
                pair[p, at, :] = (pair[p, at, :].astype(F32) + own[p, at, :].astype(F32)).astype(BF)

            self._rows(add)
            self._copy(1, p).start()

    def settle(self, p):
        pair, mate = self.pair, self.mate

        @pl.when(self.inner)
        def _():
            self._copy(1, p).wait_recv()
            self._copy(1, p).wait_send()

            def add(at):
                pair[p, at, :] = (pair[p, at, :].astype(F32) + mate[p, at, :].astype(F32)).astype(BF)

            self._rows(add)
            self._copy(2, p).start()

        @pl.when(~self.inner)
        def _():
            self._copy(2, p).wait_recv()

    def finish(self, p):
        @pl.when(self.inner)
        def _():
            self._copy(2, p).wait_send()

        @pl.when(~self.inner)
        def _():
            self._copy(0, p).wait_send()


def greet_all():
    z = lax.axis_index("ctx")
    barrier = pltpu.get_barrier_semaphore()
    for r in range(1, 8):
        pl.semaphore_signal(barrier, inc=1, device_id={"fsdp": peer(r)}, device_id_type=MESH)

    for d in range(1, 4):
        pl.semaphore_signal(barrier, inc=1, device_id={"ctx": (z + d) % 4}, device_id_type=MESH)
    pl.semaphore_wait(barrier, 10)


class LineGather:
    def __init__(self, full, send_up, send_down, recv):
        self.full, self.send_up, self.send_down, self.recv = full, send_up, send_down, recv
        self.z = lax.axis_index("ctx")

    def _copy(self, slot, up):
        send = (self.send_up if up else self.send_down).at[slot]
        full = self.full.at[slot]
        return push(full, full, send, self.recv.at[slot], {"ctx": self.z + 1 if up else self.z - 1})

    def _hand_up(self, slot):
        @pl.when(self.z < 3)
        def _():
            self._copy(slot, True).start()

    def _hand_down(self, slot):
        @pl.when(self.z > 0)
        def _():
            self._copy(slot, False).start()

    def start(self):
        self._hand_up(self.z)
        self._hand_down(self.z)

    def collect(self, d):
        @pl.when(self.z >= d)
        def _():
            self._copy(self.z - d, True).wait_recv()
            self._hand_up(self.z - d)

        @pl.when(self.z + d <= 3)
        def _():
            self._copy(self.z + d, False).wait_recv()
            self._hand_down(self.z + d)

    def finish(self):
        for slot in range(4):
            @pl.when((self.z < 3) & (slot <= self.z))
            def _():
                self._copy(slot, True).wait_send()

            @pl.when((self.z > 0) & (slot >= self.z))
            def _():
                self._copy(slot, False).wait_send()


def turn(u, cosine, sine):
    lane = lax.broadcasted_iota(jnp.int32, u.shape, 1)
    other = jnp.where(lane % 64 < 32, pltpu.roll(u, 96, 1), pltpu.roll(u, 32, 1))
    return u * cosine + other * sine


def halves(pair, out):
    lane = lax.broadcasted_iota(jnp.int32, pair.shape, 1)
    left = lane < 64
    swapped = pltpu.roll(pair, 64, 1)
    zero = jnp.zeros_like(pair)
    out[0, 0] = jnp.where(left, pair, zero).astype(BF)
    out[0, 1] = jnp.where(left, swapped, zero).astype(BF)
    out[1, 0] = jnp.where(left, zero, swapped).astype(BF)
    out[1, 1] = jnp.where(left, zero, pair).astype(BF)


def halves_t(pair, out, here):
    pair = pair.T
    zero = jnp.zeros((64, pair.shape[1]), BF)
    for g in range(2):
        head = pair[64 * g : 64 * g + 64].astype(BF)
        out[0, g, :64, here] = head
        out[0, g, 64:, here] = zero
        out[1, g, :64, here] = zero
        out[1, g, 64:, here] = head


def key_places(kv_ref, kcol):
    rows = kcol.shape[1]
    for j in range(4):
        digit = kv_ref[j, rows:, :].astype(F32)
        places = jnp.broadcast_to(digit[0:1] * 32.0 + digit[1:2], (128, rows))
        for lo in range(0, rows, 128):
            column = places[:, lo : lo + 128].T
            kcol[j * rows + lo : j * rows + lo + 128, :128] = column
            kcol[j * rows + lo : j * rows + lo + 128, 128:] = column


def scan_rows(count, body, init):
    return lax.fori_loop(
        0, count, lambda t, carry: body(pl.ds(pl.multiple_of(t * 64, 64), 64), carry), init, unroll=4
    )


def eights(value, op):
    parts = [value[8 * j : 8 * j + 8] for j in range(value.shape[0] // 8)]
    while len(parts) > 1:
        parts = [op(parts[j], parts[j + 1]) for j in range(0, len(parts), 2)]
    return parts[0]


def front_kernel(
    x_ref, pos_ref, cos_ref, sin_ref, wq_ref, wk_ref, wv_ref, wo_ref,
    n1_ref, bq_ref, bk_ref, bv_ref, n2_ref, wg_ref, wu_ref, cot_ref,
    xn_ref, q_ref, kv_ref, lse_ref, obt_ref, mid_ref, xn2_ref,
    wkv_ref, wq_all, wo_all, vec_ref, wgu_ref, df_ref,
    wkv_own, small_f, small_own, small_all, wgu_out, kk, vvt, score, prob, kcol, *sems,
):
    place = plane()
    me = lax.axis_index("fsdp")
    z = lax.axis_index("ctx")
    rows = x_ref.shape[0]
    ff_own, ff = wg_ref.shape[1] // 8, wgu_ref.shape[2] // 2
    greet_all()
    gkv = Gather(place, wkv_own, wkv_ref, sems[0], sems[1], by_owner=True)
    gs = Gather(place, small_own, small_all, sems[2], sems[3], by_owner=True)
    gq = Gather(place, wq_ref, wq_all, sems[4], sems[5], by_owner=True)
    go = Gather(place, wo_ref, wo_all, sems[6], sems[7], by_owner=True)
    send_u, recv_u = sems[8:10]
    gk = LineGather(kv_ref, *sems[10:13])
    gd = Gather(place, cot_ref, df_ref, sems[13], sems[14])

    wkv_own[:, :128] = wk_ref[...]
    wkv_own[:, 128:] = wv_ref[...]
    gkv.start()
    small_f[...] = jnp.zeros_like(small_f)
    small_f[0:1, :112] = n1_ref[...].astype(F32)
    small_f[1:2, :112] = bq_ref[...].astype(F32)
    small_f[2:3, :16] = bk_ref[...].astype(F32)
    small_f[2:3, 128:144] = bv_ref[...].astype(F32)
    small_f[3:4, :112] = n2_ref[...].astype(F32)
    flat = small_f[...]
    row = lax.broadcasted_iota(jnp.int32, flat.shape, 0)
    placed = jnp.where(row == 2, pltpu.roll(flat, me * 16, 1), pltpu.roll(flat, me * 112, 1))
    small_own[...] = placed.astype(BF)
    gs.start()
    gq.start()
    wkv_ref[me] = wkv_own[...]
    small_all[me] = small_own[...]
    wq_all[me] = wq_ref[...]
    wo_all[me] = wo_ref[...]
    for j in range(8):
        for half, src in ((0, wg_ref), (1, wu_ref)):
            block = src[:, j * ff_own : (j + 1) * ff_own]
            wgu_out[j, :, half * ff : half * ff + ff_own] = block
            wgu_out[j, :, half * ff + ff_own : (half + 1) * ff] = jnp.zeros(
                (src.shape[0], ff - ff_own), BF
            )
    df_ref[0] = cot_ref[...]
    place_row = pos_ref[...].astype(F32)
    high = jnp.floor(place_row * (1.0 / 32.0))
    kv_ref[z, rows : rows + 1, :] = high.astype(BF)
    kv_ref[z, rows + 1 : rows + 2, :] = (place_row - 32.0 * high).astype(BF)
    kv_ref[z, rows + 2 :, :] = jnp.zeros((14, 256), BF)

    gkv.relay()
    gs.relay()
    gkv.relay_corner()
    gs.relay_corner()
    for slot in (3, 5, 7, 1):
        gkv.wait(slot)
        gs.wait(slot)
    vec = small_all[0].astype(F32)
    for j in range(1, 8):
        vec = vec + small_all[j].astype(F32)
    vec_ref[...] = vec

    def norm_one(at):
        h = x_ref[at, :].astype(F32)
        scale = lax.rsqrt(jnp.mean(h * h, axis=-1, keepdims=True) + EPSILON)
        xn_ref[at, :] = (h * scale * vec_ref[0:1, :]).astype(BF)

    tiles(rows, 32, norm_one)
    cosine, sine = cos_ref[...], sin_ref[...]
    kv = dot(xn_ref[...], wkv_ref[...].reshape(896, 256)) + vec_ref[2:3, :256]
    kv_ref[z, :rows, :128] = turn(kv[:, :128], cosine, sine).astype(BF)
    kv_ref[z, :rows, 128:] = kv[:, 128:].astype(BF)
    gk.start()

    gq.relay()
    go.start()

    mate = z + 1 - 2 * (z % 2)
    half_of = lambda k: pl.ds(pl.multiple_of(k * ff, 128), ff)
    taken, given = half_of(z % 2), half_of(1 - z % 2)
    send_z, recv_z = sems[15:17]

    def block_to(r):
        owner = peer(r)
        src, dst = wgu_out.at[owner, :, taken], wgu_ref.at[me, :, taken]
        return push(src, dst, send_u.at[r], recv_u.at[r], {"fsdp": owner})

    def block_from(r):
        src, dst = wgu_out.at[me, :, taken], wgu_ref.at[peer(r), :, taken]
        return push(src, dst, send_u.at[r], recv_u.at[r], {"fsdp": peer(r)})

    def hand_over(r):
        block = wgu_ref.at[peer(r), :, taken]
        return push(block, block, send_z.at[r], recv_z.at[r], {"ctx": mate})

    def handed(r):
        block = wgu_ref.at[peer(r), :, given]
        return push(block, block, send_z.at[r], recv_z.at[r], {"ctx": mate})

    @pl.loop(1, 8)
    def _(i):
        block_to(8 - i).start()

    wgu_ref[me] = wgu_out[me]
    gd.start()
    gk.collect(1)
    gq.relay_corner()
    for slot in (3, 5, 7, 1):
        gq.wait(slot)

    @pl.loop(0, 7)
    def _(i):
        at = pl.ds(pl.multiple_of(i * 128, 128), 128)
        q = dot(xn_ref[...], wq_all[:, :, at].reshape(896, 128)) + vec_ref[1:2, at]
        q_ref[:, at] = (turn(q, cosine, sine) * 0.125).astype(BF)

    gk.collect(2)

    gk.collect(3)
    for j in range(4):
        here = pl.ds(j * rows, rows)
        halves(kv_ref[j, :rows, :128].astype(F32), kk.at[:, :, here])
        halves_t(kv_ref[j, :rows, 128:].astype(F32), vvt, here)
    key_places(kv_ref, kcol)
    count = 4 * rows // 64

    @pl.loop(0, 7)
    def _(i):
        lanes = pl.ds(pl.multiple_of(i * 128, 128), 128)
        heads = (2 * i, 2 * i + 1)
        for half in range(2):
            score[half] = dot_t(kk[half, heads[half] // 7], q_ref[:, lanes])

        def find_top(at, tops):
            seen = kcol[at, :] <= place_row
            found = []
            for half in range(2):
                s = jnp.where(seen, score[half, at, :], NEGATIVE)
                score[half, at, :] = s
                found.append(jnp.maximum(tops[half], eights(s, jnp.maximum)))
            return tuple(found)

        start = jnp.full((8, rows), NEGATIVE, F32)
        tops = [jnp.max(top, axis=0, keepdims=True) for top in scan_rows(count, find_top, (start, start))]

        def soft(at, totals):
            found = []
            for half in range(2):
                e = jnp.exp(score[half, at, :] - tops[half])
                prob[half, at, :] = e.astype(BF)
                found.append(totals[half] + eights(e, jnp.add))
            return tuple(found)

        start = jnp.zeros((8, rows), F32)
        totals = [jnp.sum(total, axis=0, keepdims=True) for total in scan_rows(count, soft, (start, start))]
        o = None
        for half in range(2):
            lse_ref[pl.ds(heads[half], 1), :] = tops[half] + jnp.log(totals[half])
            part = dot(vvt[half, heads[half] // 7], prob[half]) * (1.0 / totals[half])
            o = part if o is None else o + part
        obt_ref[lanes, :] = o.astype(BF)

        block_from(7 - i).wait_recv()
        hand_over(7 - i).start()

        @pl.when(i == 0)
        def _():
            go.relay()

        @pl.when(i == 5)
        def _():
            go.relay_corner()
            gd.relay()

        @pl.when(i == 6)
        def _():
            gd.relay_corner()

    for slot in (3, 5, 7, 1):
        go.wait(slot)
    for lo in range(0, 896, 128):
        mid_ref[:, lo : lo + 128] = t_dot(obt_ref[...], wo_all[:, :, lo : lo + 128].reshape(896, 128))

    def norm_two(at):
        m = mid_ref[at, :] + x_ref[at, :].astype(F32)
        mid_ref[at, :] = m
        scale = lax.rsqrt(jnp.mean(m * m, axis=-1, keepdims=True) + EPSILON)
        xn2_ref[at, :] = (m * scale * vec_ref[3:4, :]).astype(BF)

    tiles(rows, 32, norm_two)

    @pl.loop(1, 8)
    def _(r):
        block_to(r).wait_send()
        hand_over(r).wait_send()
        handed(r).wait_recv()

    for slot in (1, 3, 5, 7):
        gd.wait(slot)
    for each in (gkv, gs, gq, go, gk, gd):
        each.finish()


def front(x, pos, cosine, sine, wq, wk, wv, wo, n1, bq, bk, bv, n2, wg, wu, cot):
    dma = pltpu.SemaphoreType.DMA
    vm = pl.BlockSpec(memory_space=pltpu.VMEM)
    vmem = pltpu.VMEM
    out = jax.ShapeDtypeStruct
    rows, width = x.shape
    own = wq.shape[0]
    ff = -(-(wg.shape[1] // 8) // 128) * 128
    tokens = 4 * rows
    return pl.pallas_call(
        front_kernel,
        out_shape=(
            out((rows, width), BF), out((rows, width), BF), out((4, rows + 16, 256), BF),
            out((16, rows), F32), out((width, rows), BF), out((rows, width), F32),
            out((rows, width), BF), out((8, own, 256), BF), out((8, own, width), BF),
            out((8, own, width), BF), out((16, width), F32), out((8, own, 2 * ff), BF),
            out((8, rows, width), BF),
        ),
        in_specs=[vm] * 16,
        out_specs=(vm,) * 13,
        scratch_shapes=[
            vmem((own, 256), BF), vmem((16, width), F32), vmem((16, width), BF), vmem((8, 16, width), BF),
            vmem((8, own, 2 * ff), BF), vmem((2, 2, tokens, 128), BF), vmem((2, 2, 128, tokens), BF),
            vmem((2, tokens, rows), F32), vmem((2, tokens, rows), BF), vmem((tokens, rows), F32),
            dma((7,)), dma((8,)), dma((7,)), dma((8,)), dma((7,)), dma((8,)), dma((7,)), dma((8,)),
            dma((8,)), dma((8,)), dma((4,)), dma((4,)), dma((4,)), dma((7,)), dma((8,)), dma((8,)), dma((8,)),
        ],
        compiler_params=pltpu.CompilerParams(collective_id=2, has_side_effects=True),
    )(x, pos, cosine, sine, wq, wk, wv, wo, n1, bq, bk, bv, n2, wg, wu, cot)


def middle_kernel(
    xn2_ref, pos_ref, cos_ref, sin_ref, kv_ref, lse_ref, vec_ref,
    df_hbm, wgu_hbm, wd_hbm, x_hbm, cot_hbm, mid_hbm, xn_hbm, q_hbm, obt_hbm, wkv_hbm, wq_hbm, wo_hbm,
    out_ref, gin_ref, pair_q, pair_o, pair_k, in_u, pair_d,
    x_all, part_out, core_in, tree_in, dx, core_f, tree_f, gwgu, gwd, mate_d, pair_u, mate_u,
    core_o, tree_o, core_q, tree_q, core_k, tree_k,
    own_o, mate_o, own_q, mate_q, own_k, mate_k, dkv_in, *sems,
):
    place = plane()
    me = lax.axis_index("fsdp")
    z = lax.axis_index("ctx")
    rows, width = xn2_ref.shape
    own = width // 8
    ff, ff_own = wgu_hbm.shape[1] // 2, wd_hbm.shape[0]
    tokens, keys = 8 * rows, 4 * rows
    piece = gwd.shape[1]
    loads = sems[38]
    greet_all()
    line_sems = sems[18:24]
    ld = Line(gwd, pair_d, mate_d, line_sems, 0)
    lu = Line(gwgu, pair_u, mate_u, line_sems, 4)
    lo = Line(own_o, pair_o, mate_o, line_sems, 12)
    lq = Line(own_q, pair_q, mate_q, line_sems, 13)
    lk = Line(own_k, pair_k, mate_k, line_sems, 14)
    send_all, recv_all, send_kv, recv_kv = sems[24:28]

    def feed_forward(df_ref, wgu_ref, wd, act_all, hid_all, dgu_all, dh, part, folded):
        gx = Gather(place, xn2_ref, x_all, sems[0], sems[1])
        rd = Scatter(place, part, core_in, tree_in, folded, *sems[2:6])
        gx.start()
        fetch = [
            pltpu.make_async_copy(wgu_hbm, wgu_ref, loads.at[0]),
            pltpu.make_async_copy(wd_hbm, wd.at[pl.ds(0, ff_own)], loads.at[1]),
            pltpu.make_async_copy(df_hbm, df_ref, loads.at[2]),
        ]
        for cp in fetch:
            cp.start()
        x_all[0] = xn2_ref[...]
        wd[ff_own:] = jnp.zeros((ff - ff_own, width), BF)
        fetch[0].wait()
        fetch[1].wait()
        both = lambda ref, p: ref[pl.ds(2 * p, 2)].reshape(2 * rows, ref.shape[2])

        @pl.loop(0, 4)
        def _(p):
            @pl.when(p == 1)
            def _():
                gx.relay()

            @pl.when(p == 3)
            def _():
                gx.relay_corner()

            gx.wait(2 * p + 1)
            x = both(x_all, p)
            for n in range(0, 2 * ff, 256):
                act_all[p, :, n : n + 256] = dot(x, wgu_ref[:, n : n + 256])

            def activate(at):
                gate, up = act_all[p, at, :ff], act_all[p, at, ff:]
                sig = 0.5 * jnp.tanh(0.5 * gate) + 0.5
                hid_all[p, at, :] = (gate * sig * up).astype(BF)

            tiles(2 * rows, 16, activate)
            out = dot(hid_all[p], wd[...]).astype(BF)
            part_out[pl.ds(2 * p, 2)] = out.reshape(2, rows, width)

        fetch[2].wait()
        for p in range(4):
            gwd[p] = t_dot(
                hid_all[:, :, p * piece : (p + 1) * piece].reshape(tokens, piece),
                df_ref[...].reshape(tokens, width),
            ).astype(BF)
            ld.start(p)

        @pl.loop(0, 4)
        def _(k):
            p = 3 - k
            dh[...] = dot_t(both(df_ref, p), wd[...])

            def activate(at):
                gate, up, d = act_all[p, at, :ff], act_all[p, at, ff:], dh[at, :]
                sig = 0.5 * jnp.tanh(0.5 * gate) + 0.5
                dgu_all[p, at, :ff] = (d * up * (sig * (1.0 + gate * (1.0 - sig)))).astype(BF)
                dgu_all[p, at, ff:] = (d * (gate * sig)).astype(BF)

            tiles(2 * rows, 16, activate)
            value = dot_t(dgu_all[p], wgu_ref[...]).astype(BF)
            part[pl.ds(2 * p, 2)] = value.reshape(2, rows, width)
            rd.to_twin(p).start()

            @pl.when(k == 1)
            def _():
                rd.start_corner()

            @pl.when(k == 2)
            def _():
                ld.meet(0)

        rd.start_far()
        ld.meet(1)
        rd.relay()

        @pl.loop(0, 2 * ff // 256)
        def _(n):
            at = pl.ds(pl.multiple_of(n * 256, 256), 256)
            value = t_dot(x_all[...].reshape(tokens, width), dgu_all[:, :, at].reshape(tokens, 256))
            gwgu[:, :, at] = value.astype(BF).reshape(8, own, 256)

            @pl.when(n == 1)
            def _():
                ld.meet(2)

            @pl.when(n == 3)
            def _():
                ld.settle(0)

        for r in (7, 6, 5):
            lu.start(peer(r))

        def store_dx(at, value):
            dx[at, :] = value

        rd.total(store_dx)
        gx.finish()
        rd.finish()

    pl.run_scoped(
        feed_forward,
        pltpu.VMEM((8, rows, width), BF), pltpu.VMEM((width, 2 * ff), BF), pltpu.VMEM((ff, width), BF),
        pltpu.VMEM((4, 2 * rows, 2 * ff), F32), pltpu.VMEM((4, 2 * rows, ff), BF),
        pltpu.VMEM((4, 2 * rows, 2 * ff), BF), pltpu.VMEM((2 * rows, ff), F32),
        pltpu.VMEM((8, rows, width), BF), pltpu.VMEM((3, rows, width), BF),
    )

    def attention_back(
        x_ref, cot_ref, mid_ref, xn_ref, q_ref, obt_ref, wkv_ref, wq_ref, wo_ref,
        dm, da, dob, kk, kkt, vv, kcol, score, dprob, prob, dscore, dk_acc, dv_acc,
        dq, dkv_own, dkv, dxn, small, part_o, fold_o, part_q, fold_q, part_k, fold_k, fold_f,
    ):
        ro = Scatter(place, part_o, core_o, tree_o, fold_o, *sems[6:10], by_owner=True)
        rq = Scatter(place, part_q, core_q, tree_q, fold_q, *sems[10:14], by_owner=True)
        rk = Scatter(place, part_k, core_k, tree_k, fold_k, *sems[14:18], by_owner=True)
        rf = Scatter(place, part_out, core_f, tree_f, fold_f, *sems[28:32])
        arrays = (
            (mid_hbm, mid_ref), (cot_hbm, cot_ref), (obt_hbm, obt_ref), (wo_hbm, wo_ref), (q_hbm, q_ref),
            (xn_hbm, xn_ref), (wq_hbm, wq_ref), (wkv_hbm, wkv_ref), (x_hbm, x_ref),
        )
        fetch = [pltpu.make_async_copy(src, dst, loads.at[3 + i]) for i, (src, dst) in enumerate(arrays)]
        for cp in fetch:
            cp.start()
        for k in (3, 2, 1, 0):
            rf.to_twin(k).start()
        ld.meet(3)
        ld.settle(1)
        fetch[0].wait()
        fetch[1].wait()

        small[...] = jnp.zeros_like(small)

        def norm_two(at):
            m, g = mid_ref[at, :], dx[at, :]
            scale = lax.rsqrt(jnp.mean(m * m, axis=-1, keepdims=True) + EPSILON)
            weighted = vec_ref[3:4, :] * g
            inner = jnp.mean(weighted * m, axis=-1, keepdims=True)
            d = cot_ref[at, :].astype(F32) + scale * weighted - m * (scale * scale * scale) * inner
            dm[at, :] = d
            da[at, :] = d.astype(BF)
            small[3:4, :] += jnp.sum(g * m * scale, axis=0, keepdims=True)

        tiles(rows, 32, norm_two)
        for i in range(2, 9):
            fetch[i].wait()

        @pl.loop(0, 7)
        def _(i):
            lanes = pl.ds(pl.multiple_of(i * 128, 128), 128)
            part_o[:, :, lanes] = dot(obt_ref[...], da[:, lanes]).astype(BF).reshape(8, own, 128)

        for k in (3, 2, 1, 0):
            ro.to_twin(k).start()
        dob[...] = dot_t(da[...], wo_ref[...].reshape(width, width)).astype(BF)
        for j in range(4):
            here = pl.ds(j * rows, rows)
            key, value = kv_ref[j, :rows, :128].astype(F32), kv_ref[j, :rows, 128:].astype(F32)
            halves(key, kk.at[:, :, here])
            halves(value, vv.at[:, :, here])
            halves_t(key, kkt, here)
        key_places(kv_ref, kcol)
        dk_acc[...] = jnp.zeros_like(dk_acc)
        dv_acc[...] = jnp.zeros_like(dv_acc)
        place_row = pos_ref[...].astype(F32)
        cosine, sine = cos_ref[...], -sin_ref[...]
        count = keys // 64

        def keep(total):
            def store(at, value):
                total[0, at, :] = value.astype(BF)

            return store

        def gather_to(r):
            owner = peer(r)
            return push(pair_u.at[owner], in_u.at[me], send_all.at[r], recv_all.at[me], {"fsdp": owner})

        def settle_u(r):
            lu.settle(peer(r))
            gather_to(r).start()

        ld.settle(2)

        @pl.loop(0, 7)
        def _(i):
            lanes = pl.ds(pl.multiple_of(i * 128, 128), 128)
            grad = None
            for half in range(2):
                head = 2 * i + half
                g = head // 7
                score[...] = dot_t(kk[half, g], q_ref[:, lanes])
                dprob[...] = dot_t(vv[half, g], dob[:, lanes])
                lse_row = lse_ref[pl.ds(head, 1), :]

                def find_delta(at, total):
                    s = jnp.where(kcol[at, :] <= place_row, score[at, :], NEGATIVE)
                    p = jnp.exp(s - lse_row)
                    score[at, :] = p
                    prob[at, :] = p.astype(BF)
                    return total + eights(p * dprob[at, :], jnp.add)

                delta = scan_rows(count, find_delta, jnp.zeros((8, rows), F32))
                delta = jnp.sum(delta, axis=0, keepdims=True)

                def find_score(at):
                    dscore[at, :] = (score[at, :] * (dprob[at, :] - delta)).astype(BF)

                tiles(keys, 64, find_score)
                dv_acc[half, g] += dot(prob[...], dob[:, lanes])
                dk_acc[half, g] += dot(dscore[...], q_ref[:, lanes])
                term = dot(kkt[half, g], dscore[...])
                grad = term if grad is None else grad + term
            dq[:, lanes] = turn(grad.T * 0.125, cosine, sine).astype(BF)

            @pl.when(i == 0)
            def _():
                ro.start()
                rf.start()
                lu.meet(peer(7))

            @pl.when(i == 1)
            def _():
                ld.settle(3)

            @pl.when(i == 2)
            def _():
                lu.meet(peer(6))

            @pl.when(i == 3)
            def _():
                ro.relay()
                rf.relay()
                settle_u(7)

            @pl.when(i == 4)
            def _():
                lu.meet(peer(5))

            @pl.when(i == 5)
            def _():
                settle_u(6)
                ro.total(keep(own_o))

        lane = lax.broadcasted_iota(jnp.int32, (64, 128), 1)

        def join(acc, at):
            first = jnp.where(lane < 64, acc[0, 0, at, :], acc[1, 1, at, :])
            second = jnp.where(lane < 64, acc[0, 1, at, :], acc[1, 0, at, :])
            return first + pltpu.roll(second, 64, 1)

        @pl.loop(0, 4)
        def _(j):
            for first in range(0, rows, 64):
                at = pl.ds(pl.multiple_of(j * rows + first, 64), 64)
                dkv_own[j, first : first + 64, :128] = join(dk_acc, at).astype(BF)
                dkv_own[j, first : first + 64, 128:] = join(dv_acc, at).astype(BF)

        def kv_to(d):
            other = (z + d) % 4
            return push(
                dkv_own.at[other], dkv_in.at[d - 1], send_kv.at[d - 1], recv_kv.at[d - 1], {"ctx": other}
            )

        for d in (2, 1, 3):
            kv_to(d).start()

        @pl.loop(3, 8)
        def _(i):
            lu.start(peer(7 - i))

        lo.start(0)
        settle_u(5)

        def weight_grads(grads, part, n):
            for at in range(0, n, 128):
                value = t_dot(xn_ref[...], grads[:, at : at + 128]).astype(BF)
                part[:, :, at : at + 128] = value.reshape(8, own, 128)

        weight_grads(dq, part_q, width)
        for k in (3, 2, 1, 0):
            rq.to_twin(k).start()
        for at in range(0, width, 128):
            wq_rows = wq_ref[...].reshape(width, width)
            dxn[:, at : at + 128] = dot_t(dq[...], wq_rows[at : at + 128])
        rq.start()

        def store_out(at, value):
            out_ref[at, :] = value + mid_ref[at, :]

        rf.total(store_out)
        for d in (1, 3, 2):
            kv_to(d).wait_recv()

        def sum_kv(at):
            value = dkv_own[z, at, :].astype(F32)
            for d in range(3):
                value = value + dkv_in[d, at, :].astype(F32)
            dkv[at, :128] = turn(value[:, :128], cos_ref[at, :], -sin_ref[at, :]).astype(BF)
            dkv[at, 128:] = value[:, 128:].astype(BF)

        tiles(rows, 32, sum_kv)
        weight_grads(dkv, part_k, 256)
        for at in range(0, width, 128):
            wkv_rows = wkv_ref[...].reshape(width, 256)
            dxn[:, at : at + 128] += dot_t(dkv[...], wkv_rows[at : at + 128])

        def norm_one(at):
            h, g = x_ref[at, :].astype(F32), dxn[at, :]
            scale = lax.rsqrt(jnp.mean(h * h, axis=-1, keepdims=True) + EPSILON)
            weighted = vec_ref[0:1, :] * g
            inner = jnp.mean(weighted * h, axis=-1, keepdims=True)
            gin_ref[at, :] = dm[at, :] + scale * weighted - h * (scale * scale * scale) * inner
            small[0:1, :] += jnp.sum(g * h * scale, axis=0, keepdims=True)
            small[1:2, :] += jnp.sum(dq[at, :].astype(F32), axis=0, keepdims=True)
            small[2:3, :256] += jnp.sum(dkv[at, :].astype(F32), axis=0, keepdims=True)

        tiles(rows, 32, norm_one)
        flat = small[...]
        line_of = lax.broadcasted_iota(jnp.int32, (16, 128), 0)
        for j in range(8):
            by_row = pltpu.roll(flat, (width - 112 * j) % width, 1)[:, :128]
            by_head = pltpu.roll(flat, (width - 16 * j) % width, 1)
            value = jnp.where(line_of == 2, by_head[:, :128], by_row)
            lifted = pltpu.roll(by_head[:, 128:256], 2, 0)
            value = jnp.where(line_of == 4, lifted, value)
            part_k[j, :16, 256:] = value.astype(BF)
            part_k[j, 16:, 256:] = jnp.zeros((own - 16, 128), BF)

        for k in (3, 2, 1, 0):
            rk.to_twin(k).start()
        lu.meet(peer(4))
        rk.start()
        rq.relay()
        lu.meet(peer(3))
        settle_u(4)
        rk.relay()
        rq.total(keep(own_q))
        lq.start(0)
        lu.meet(peer(2))
        settle_u(3)
        rk.total(keep(own_k))
        lk.start(0)
        lu.meet(peer(1))
        settle_u(2)
        lu.meet(me)
        settle_u(1)
        lo.meet(0)
        lu.settle(me)
        keep_own = pltpu.make_async_copy(pair_u.at[me], in_u.at[me], loads.at[12])
        keep_own.start()
        lq.meet(0)
        lo.settle(0)
        lk.meet(0)
        lq.settle(0)
        lk.settle(0)
        keep_own.wait()

        @pl.loop(1, 8)
        def _(r):
            other = peer(r)
            push(
                pair_u.at[me], in_u.at[other], send_all.at[r], recv_all.at[other], {"fsdp": other}
            ).wait_recv()
            gather_to(r).wait_send()

        for d in (1, 2, 3):
            kv_to(d).wait_send()
        for each in (ro, rq, rk, rf):
            each.finish()

    v = pltpu.VMEM
    pl.run_scoped(
        attention_back,
        v((rows, width), BF), v((rows, width), BF), v((rows, width), F32), v((rows, width), BF),
        v((rows, width), BF), v((width, rows), BF), v((8, own, 256), BF), v((8, own, width), BF),
        v((8, own, width), BF),
        v((rows, width), F32), v((rows, width), BF), v((rows, width), BF),
        v((2, 2, keys, 128), BF), v((2, 2, 128, keys), BF), v((2, 2, keys, 128), BF),
        v((keys, rows), F32), v((keys, rows), F32), v((keys, rows), F32),
        v((keys, rows), BF), v((keys, rows), BF),
        v((2, 2, keys, 128), F32), v((2, 2, keys, 128), F32),
        v((rows, width), BF), v((4, rows, 256), BF), v((rows, 256), BF), v((rows, width), F32),
        v((16, width), F32),
        v((8, own, width), BF), v((3, own, width), BF), v((8, own, width), BF), v((3, own, width), BF),
        v((8, own, 384), BF), v((3, own, 384), BF), v((3, rows, width), BF),
    )

    @pl.loop(0, 4)
    def _(p):
        ld.finish(p)

    @pl.loop(0, 8)
    def _(p):
        lu.finish(p)

    for each in (lo, lq, lk):
        each.finish(0)


def middle(xn2, pos, cosine, sine, kv, lse, vec, df_all, wgu, wd, x, cot, mid, xn, q, obt, wkv, wq, wo):
    dma = pltpu.SemaphoreType.DMA
    vm = pl.BlockSpec(memory_space=pltpu.VMEM)
    hbm = pl.BlockSpec(memory_space=pl.ANY)
    v = pltpu.VMEM
    out = jax.ShapeDtypeStruct
    rows, width = x.shape
    own = width // 8
    ff = wgu.shape[1] // 2
    gu, gd = (8, own, 2 * ff), (4, ff // 4, width)
    wide, narrow = (1, own, width), (1, own, 384)
    tree = [dma((4,)), dma((4,)), dma((3,)), dma((3,))]
    return pl.pallas_call(
        middle_kernel,
        out_shape=(
            out((rows, width), F32), out((rows, width), F32), out(wide, BF), out(wide, BF), out(narrow, BF),
            out(gu, BF), out(gd, BF),
        ),
        in_specs=[vm] * 7 + [hbm] * 12,
        out_specs=(vm, vm, vm, vm, vm, hbm, vm),
        scratch_shapes=[
            v((8, rows, width), BF), v((8, rows, width), BF), v((4, rows, width), BF), v((3, rows, width), BF),
            v((rows, width), F32), v((4, rows, width), BF), v((3, rows, width), BF),
            v(gu, BF), v(gd, BF), v(gd, BF), v(gu, BF), v(gu, BF),
            v((4, own, width), BF), v((3, own, width), BF), v((4, own, width), BF), v((3, own, width), BF),
            v((4, own, 384), BF), v((3, own, 384), BF),
            v(wide, BF), v(wide, BF), v(wide, BF), v(wide, BF), v(narrow, BF), v(narrow, BF),
            v((3, rows, 256), BF),
            dma((7,)), dma((8,)), *tree, *tree, *tree, *tree,
            *[dma((15,))] * 6,
            dma((8,)), dma((8,)), dma((3,)), dma((3,)), *tree,
            *[dma((1,))] * 6, dma((13,)),
        ],
        compiler_params=pltpu.CompilerParams(
            collective_id=0, has_side_effects=True, vmem_limit_bytes=67043328
        ),
    )(xn2, pos, cosine, sine, kv, lse, vec, df_all, wgu, wd, x, cot, mid, xn, q, obt, wkv, wq, wo)


def results_kernel(
    out_ref, gin_ref, tq_ref, to_ref, tk_ref, tu_ref, td_ref,
    o_ref, i_ref, n1_ref, q_ref, bq_ref, k_ref, bk_ref, v_ref, bv_ref, w_ref, n2_ref, g_ref, u_ref, d_ref,
):
    o_ref[...] = out_ref[...]
    i_ref[...] = gin_ref[...]
    q_ref[...] = tq_ref[0].astype(F32)
    w_ref[...] = to_ref[0].astype(F32)
    k_ref[...] = tk_ref[0, :, :128].astype(F32)
    v_ref[...] = tk_ref[0, :, 128:256].astype(F32)
    small = tk_ref[0, :16, 256:].astype(F32)
    for i, ref in enumerate((n1_ref, bq_ref, bk_ref, n2_ref, bv_ref)):
        ref[...] = small[i : i + 1, : ref.shape[1]]
    ff_own, ff = d_ref.shape[0], tu_ref.shape[2] // 2
    for j in range(8):
        def place_block(at):
            g_ref[at, j * ff_own : (j + 1) * ff_own] = tu_ref[j, at, :ff_own].astype(F32)
            u_ref[at, j * ff_own : (j + 1) * ff_own] = tu_ref[j, at, ff : ff + ff_own].astype(F32)

        tiles(tu_ref.shape[1], 16, place_block)
    rows = td_ref.shape[1]
    for p in range(4):
        count = min(rows, ff_own - p * rows)
        d_ref[p * rows : p * rows + count] = td_ref[p, :count].astype(F32)


def results(out, gin, tq, to, tk, tu, td, ff_own):
    vm = pl.BlockSpec(memory_space=pltpu.VMEM)
    rows, width = out.shape
    own = width // 8
    shapes = (
        (rows, width), (rows, width), (1, own), (own, 896), (1, own), (own, 128), (1, 16), (own, 128), (1, 16),
        (own, 896), (1, own), (own, 8 * ff_own), (own, 8 * ff_own), (ff_own, width),
    )
    return pl.pallas_call(
        results_kernel,
        out_shape=tuple(jax.ShapeDtypeStruct(shape, F32) for shape in shapes),
        in_specs=[vm] * 7,
        out_specs=(vm,) * 14,
    )(out, gin, tq, to, tk, tu, td)


def shards(
    inputs, positions, cotangent, norm_one, w_query, b_query, key_projection, b_key,
    value_projection, value_bias, w_out, norm_two, w_gate, w_up, w_down,
):
    places = positions[0]
    turned = angles_of(places)
    cosine, sine = jnp.cos(turned), jnp.sin(turned)
    sine = jnp.where(jnp.arange(128)[None, :] % 64 < 32, -sine, sine)
    own = w_query.shape[1]
    ff_own = w_down.shape[1]
    ff = -(-ff_own // 128) * 128
    x, cot = inputs[0], cotangent[0]
    xn, q, kv, lse, obt, mid, xn2, wkv, wq, wo, vec, wgu, df_all = front(
        x, positions, cosine, sine, w_query[0], key_projection[0], value_projection[0], w_out[0],
        norm_one, b_query, b_key, value_bias, norm_two, w_gate[0], w_up[0], cot,
    )
    totals = middle(
        xn2, positions, cosine, sine, kv, lse, vec, df_all, wgu.reshape(-1, 2 * ff), w_down[0],
        x, cot, mid, xn, q, obt, wkv, wq, wo,
    )
    matrix = lambda i: i in (0, 1, 3, 5, 7, 9, 11, 12, 13)
    return tuple(g[None] if matrix(i) else g for i, g in enumerate(results(*totals, ff_own)))


def angles_of(places):
    half = HEAD_SIZE // 2
    inverse = jnp.exp(jnp.arange(half, dtype=F32) * (-2.0 * math.log(ROPE_BASE) / HEAD_SIZE))
    return places.astype(F32)[:, None] * jnp.concatenate([inverse] * 4)[None, :]


def shards_general(
    inputs, positions, cotangent, norm_one, w_query, b_query, key_projection, b_key,
    value_projection, value_bias, w_out, norm_two, w_gate, w_up, w_down,
):
    rows = inputs.shape[1]
    width = inputs.shape[2]
    group = QUERY_HEADS // KEY_VALUE_HEADS
    q_cols = w_query.shape[2]
    kv_cols = key_projection.shape[2]
    score_scale = 1.0 / math.sqrt(HEAD_SIZE)

    places = positions[0]
    key_places = lax.all_gather(places, "ctx", axis=0, tiled=True)
    cosine, sine = angles(places)
    hidden = inputs[0].astype(F32)

    packed = jnp.concatenate([w_query[0], key_projection[0], value_projection[0], w_out[0]], axis=1)
    packed = lax.all_gather(packed, "fsdp", axis=0, tiled=True)
    w_qkv = packed[:, : q_cols + 2 * kv_cols]
    w_o = packed[:, q_cols + 2 * kv_cols :]
    small = jnp.concatenate([norm_one[0], b_query[0], b_key[0], value_bias[0], norm_two[0]])
    small = lax.all_gather(small, "fsdp", axis=0).astype(F32)
    cuts, at = [], 0
    for piece in (norm_one, b_query, b_key, value_bias, norm_two):
        n = piece.shape[1]
        cuts.append(small[:, at : at + n].reshape(-1))
        at += n
    gain_one, bias_q, bias_k, bias_v, gain_two = cuts
    bias = jnp.concatenate([bias_q, bias_k, bias_v])

    grad_branch = cotangent[0]
    df_all = lax.all_gather(grad_branch, "fsdp", axis=0, tiled=True)
    wg = lax.all_to_all(w_gate[0], "fsdp", split_axis=1, concat_axis=0, tiled=True)
    wu = lax.all_to_all(w_up[0], "fsdp", split_axis=1, concat_axis=0, tiled=True)
    wd = w_down[0]

    scale_one, normed = norm_rows(hidden, gain_one)
    qkv = dot(normed, w_qkv) + bias
    q = rotate(qkv[:, :q_cols].reshape(rows, QUERY_HEADS, HEAD_SIZE), cosine, sine).astype(BF)
    k = rotate(
        qkv[:, q_cols : q_cols + kv_cols].reshape(rows, KEY_VALUE_HEADS, HEAD_SIZE), cosine, sine
    ).astype(BF)
    v = qkv[:, q_cols + kv_cols :].astype(BF)
    kv = jnp.concatenate([k.reshape(rows, kv_cols), v], axis=1)
    kv = lax.all_gather(kv, "ctx", axis=0, tiled=True)
    total = kv.shape[0]
    k_all = kv[:, :kv_cols].reshape(total, KEY_VALUE_HEADS, HEAD_SIZE)
    v_all = kv[:, kv_cols:].reshape(total, KEY_VALUE_HEADS, HEAD_SIZE)
    q = q.reshape(rows, KEY_VALUE_HEADS, group, HEAD_SIZE)
    s = jnp.einsum("tgjd,ugd->gjtu", q, k_all, preferred_element_type=F32) * score_scale
    s = jnp.where(key_places[None, :] <= places[:, None], s, NEGATIVE)
    top = jnp.max(s, axis=-1, keepdims=True)
    lse = top + jnp.log(jnp.sum(jnp.exp(s - top), axis=-1, keepdims=True))
    pf = jnp.exp(s - lse)
    p = pf.astype(BF)
    o = jnp.einsum("gjtu,ugd->tgjd", p, v_all, preferred_element_type=F32)
    ob = o.reshape(rows, q_cols).astype(BF)
    middle = hidden + dot(ob, w_o)
    scale_two, normed_two = norm_rows(middle, gain_two)

    x_all = lax.all_gather(normed_two, "fsdp", axis=0, tiled=True)
    gate = dot(x_all, wg)
    up = dot(x_all, wu)
    sig = jax.nn.sigmoid(gate)
    hid = (gate * sig * up).astype(BF)
    out_part = dot(hid, wd).astype(BF)
    ffn_out = lax.psum_scatter(out_part, "fsdp", scatter_dimension=0, tiled=True)
    output = middle + ffn_out.astype(F32)

    dhid = dot_t(df_all, wd)
    dgate = (dhid * up * sig * (1.0 + gate * (1.0 - sig))).astype(BF)
    dup = (dhid * (gate * sig)).astype(BF)
    dx_part = (dot_t(dgate, wg) + dot_t(dup, wu)).astype(BF)
    dxn2 = lax.psum_scatter(dx_part, "fsdp", scatter_dimension=0, tiled=True).astype(F32)
    g_down = t_dot(hid, df_all)
    g_gate = t_dot(x_all, dgate)
    g_up = t_dot(x_all, dup)

    g_out = grad_branch.astype(F32)
    grad_gain_two, dmid = norm_back(middle, scale_two, gain_two, dxn2)
    dm = g_out + dmid
    da = dm.astype(BF)
    g_wo = t_dot(ob, da)
    dob = dot_t(da, w_o).astype(BF).reshape(rows, KEY_VALUE_HEADS, group, HEAD_SIZE)

    dp = jnp.einsum("tgjd,ugd->gjtu", dob, v_all, preferred_element_type=F32)
    delta = jnp.sum(pf * dp, axis=-1, keepdims=True)
    ds = (pf * (dp - delta)).astype(BF)
    dq = jnp.einsum("gjtu,ugd->tgjd", ds, k_all, preferred_element_type=F32) * score_scale
    dk = jnp.einsum("gjtu,tgjd->ugd", ds, q, preferred_element_type=F32) * score_scale
    dv = jnp.einsum("gjtu,tgjd->ugd", p, dob, preferred_element_type=F32)
    dkv = jnp.concatenate([dk.reshape(total, kv_cols), dv.reshape(total, kv_cols)], axis=1)
    dkv = lax.psum_scatter(dkv, "ctx", scatter_dimension=0, tiled=True)
    dq = rotate(dq.reshape(rows, QUERY_HEADS, HEAD_SIZE), cosine, -sine).astype(BF)
    dk = rotate(
        dkv[:, :kv_cols].reshape(rows, KEY_VALUE_HEADS, HEAD_SIZE), cosine, -sine
    ).astype(BF)
    dqkv = jnp.concatenate(
        [dq.reshape(rows, q_cols), dk.reshape(rows, kv_cols), dkv[:, kv_cols:].astype(BF)], axis=1
    )
    g_qkv = t_dot(normed, dqkv)
    g_bias = jnp.sum(dqkv.astype(F32), axis=0)
    dxn = dot_t(dqkv, w_qkv)
    grad_gain_one, dhidden = norm_back(hidden, scale_one, gain_one, dxn)
    grad_in = dm + dhidden

    g_attn = jnp.concatenate([g_qkv, g_wo], axis=1).astype(BF)
    g_attn = lax.psum_scatter(g_attn, "fsdp", scatter_dimension=0, tiled=True)
    back = [
        lax.all_to_all(g.astype(BF), "fsdp", split_axis=0, concat_axis=1, tiled=True)
        for g in (g_gate, g_up)
    ]
    g_attn, g_gate, g_up, g_down = lax.psum((g_attn, back[0], back[1], g_down.astype(BF)), "ctx")
    pieces = jnp.concatenate(
        [
            g.reshape(small.shape[0], -1)
            for g in (
                grad_gain_one, g_bias[:q_cols], g_bias[q_cols : q_cols + kv_cols],
                g_bias[q_cols + kv_cols :], grad_gain_two,
            )
        ],
        axis=1,
    )
    pieces = lax.psum(pieces, ("ctx", "fsdp"))
    mine = lax.dynamic_slice_in_dim(pieces, lax.axis_index("fsdp"), 1, axis=0)
    outs, at = [], 0
    for piece in (norm_one, b_query, b_key, value_bias, norm_two):
        n = piece.shape[1]
        outs.append(mine[:, at : at + n])
        at += n
    g_n1, g_bq, g_bk, g_bv, g_n2 = outs
    g_attn = g_attn.astype(F32)
    return (
        output[None], grad_in[None], g_n1,
        g_attn[None, :, :q_cols], g_bq,
        g_attn[None, :, q_cols : q_cols + kv_cols], g_bk,
        g_attn[None, :, q_cols + kv_cols : q_cols + 2 * kv_cols], g_bv,
        g_attn[None, :, q_cols + 2 * kv_cols :], g_n2,
        g_gate.astype(F32)[None], g_up.astype(F32)[None], g_down.astype(F32)[None],
    )


def solution(mesh):
    tok, row, vec = P("fsdp", "ctx", None), P(None, "fsdp", None), P(None, "fsdp")
    fast = mesh.shape["ctx"] == 4 and mesh.shape["fsdp"] == 8
    return jax.shard_map(
        shards if fast else shards_general,
        mesh=mesh,
        in_specs=(
            tok, P("fsdp", "ctx"), tok, vec, row, vec, row, vec, row, vec, row, vec, row, row, row,
        ),
        out_specs=(tok, tok, vec, row, vec, row, vec, row, vec, row, vec, row, row, row),
        check_vma=False,
    )
```

```python
import functools
import math

import jax
import jax.numpy as jnp
from jax import lax
from jax.experimental import pallas as pl
from jax.experimental.pallas import tpu as pltpu
from jax.sharding import PartitionSpec as P

QUERY_HEADS = 14
KEY_VALUE_HEADS = 2
HEAD_SIZE = 64
ROPE_BASE = 1000000.0
EPSILON = 1e-06
NEGATIVE = -1e30
BF = jnp.bfloat16
F32 = jnp.float32
MESH = pl.DeviceIdType.MESH


def angles(places):
    half = HEAD_SIZE // 2
    inverse = jnp.exp(jnp.arange(half, dtype=F32) * (-2.0 * math.log(ROPE_BASE) / HEAD_SIZE))
    turned = places.astype(F32)[:, None] * inverse[None, :]
    return jnp.cos(turned)[:, None, :], jnp.sin(turned)[:, None, :]


def rotate(u, cosine, sine):
    half = u.shape[-1] // 2
    a, b = u[..., :half], u[..., half:]
    return jnp.concatenate([a * cosine - b * sine, b * cosine + a * sine], axis=-1)


def norm_rows(hidden, gain):
    scale = lax.rsqrt(jnp.mean(hidden * hidden, axis=-1, keepdims=True) + EPSILON)
    return scale, (hidden * scale * gain).astype(BF)


def norm_back(hidden, scale, gain, grad):
    weighted = gain * grad
    grad_gain = jnp.sum(grad * hidden * scale, axis=0)
    inner = jnp.mean(weighted * hidden, axis=-1, keepdims=True)
    return grad_gain, scale * weighted - hidden * (scale * scale * scale) * inner


def dot(a, b):
    return jnp.dot(a, b, preferred_element_type=F32)


def dot_t(a, b):
    return lax.dot_general(a, b, (((1,), (1,)), ((), ())), preferred_element_type=F32)


def t_dot(a, b):
    return lax.dot_general(a, b, (((0,), (0,)), ((), ())), preferred_element_type=F32)


def plane():
    f = lax.axis_index("fsdp")
    core, x, y = f % 2, (f // 2) % 2, f // 4
    by_x, by_y = f + 2 - 4 * x, f + 4 - 8 * y
    twin = f + 1 - 2 * core
    near = by_x + core * (by_y - by_x)
    far = by_y + core * (by_x - by_y)
    return twin, near, far, 2 + 2 * core, 4 - 2 * core


def tiles(rows, step, body):
    count = rows // step
    unroll = count if count <= 10 else 4

    @pl.loop(0, count, unroll=unroll)
    def _(r):
        body(pl.ds(pl.multiple_of(r * step, step), step))


def peer(r):
    f = lax.axis_index("fsdp")
    core, x, y = f % 2, (f // 2) % 2, f // 4
    return f + (r % 2) * (1 - 2 * core) + ((r // 2) % 2) * (2 - 4 * x) + (r // 4) * (4 - 8 * y)


def greet(others):
    barrier = pltpu.get_barrier_semaphore()
    for other in others:
        pl.semaphore_signal(barrier, inc=1, device_id=other, device_id_type=MESH)
    pl.semaphore_wait(barrier, len(others))


def push(src, dst, send, recv, other):
    return pltpu.make_async_remote_copy(
        src_ref=src, dst_ref=dst, send_sem=send, recv_sem=recv, device_id=other, device_id_type=MESH
    )


class Gather:
    def __init__(self, place, mine, full, send, recv, by_owner=False):
        self.twin, self.near, self.far, self.s_near, self.s_far = place
        self.mine, self.full, self.send, self.recv = mine, full, send, recv
        self.by_owner = by_owner

    def copy(self, i):
        twin, near, far = self.twin, self.near, self.far
        here = (0, 0, 0, self.s_near, 2, 4, 6)[i]
        there, other = (
            (self.s_near, near), (self.s_far, far), (1, twin), (6, far), (3, twin), (5, twin), (7, twin)
        )[i]
        if self.by_owner:
            here = there = peer(here)
        src = self.mine if i < 3 else self.full.at[here]
        return push(src, self.full.at[there], self.send.at[i], self.recv.at[there], {"fsdp": other})

    def start(self):
        for i in range(3):
            self.copy(i).start()

    def wait(self, slot):
        slot = peer(slot) if self.by_owner else slot
        full = self.full.at[slot]
        push(full, full, self.send.at[0], self.recv.at[slot], {"fsdp": self.near}).wait_recv()

    def relay(self):
        self.wait(2)
        self.wait(4)
        for i in range(3, 6):
            self.copy(i).start()

    def relay_corner(self):
        self.wait(6)
        self.copy(6).start()

    def finish(self):
        for i in range(7):
            self.copy(i).wait_send()


class Scatter:
    def __init__(
        self, place, part, core_in, tree_in, folded, send_core, recv_core, send_tree, recv_tree,
        by_owner=False,
    ):
        self.twin, self.near, self.far, self.s_near, self.s_far = place
        self.at = peer if by_owner else lambda slot: slot
        self.part, self.core_in, self.tree_in, self.folded = part, core_in, tree_in, folded
        self.send_core, self.recv_core = send_core, recv_core
        self.send_tree, self.recv_tree = send_tree, recv_tree

    def to_twin(self, k):
        return push(
            self.part.at[self.at(2 * k + 1)], self.core_in.at[k], self.send_core.at[k], self.recv_core.at[k],
            {"fsdp": self.twin},
        )

    def tree(self, j):
        other = (self.far, self.near, self.far)[j]
        return push(
            self.folded.at[j], self.tree_in.at[j], self.send_tree.at[j], self.recv_tree.at[j],
            {"fsdp": other},
        )

    def fold(self, j, slot, corner=False):
        part, core_in, tree_in, folded = self.part, self.core_in, self.tree_in, self.folded
        k = slot // 2
        slot = self.at(slot)

        def add(at):
            value = part[slot, at, :].astype(F32) + core_in[k, at, :].astype(F32)
            if corner:
                value = value + tree_in[0, at, :].astype(F32)
            folded[j, at, :] = value.astype(BF)

        tiles(part.shape[1], 16, add)

    def start_corner(self):
        self.to_twin(3).wait_recv()
        self.fold(0, 6)
        self.tree(0).start()

    def start_far(self):
        self.to_twin(1).wait_recv()
        self.to_twin(2).wait_recv()
        self.fold(2, self.s_far)
        self.tree(2).start()

    def start(self):
        self.start_corner()
        self.start_far()

    def relay(self):
        self.tree(0).wait_recv()
        self.fold(1, self.s_near, True)
        self.tree(1).start()

    def total(self, store):
        part, core_in, tree_in = self.part, self.core_in, self.tree_in
        mine = self.at(0)
        self.to_twin(0).wait_recv()
        self.tree(1).wait_recv()
        self.tree(2).wait_recv()

        def add(at):
            value = part[mine, at, :].astype(F32) + core_in[0, at, :].astype(F32)
            store(at, value + tree_in[1, at, :].astype(F32) + tree_in[2, at, :].astype(F32))

        tiles(part.shape[1], 16, add)

    def finish(self):
        for k in range(4):
            self.to_twin(k).wait_send()
        for j in range(3):
            self.tree(j).wait_send()


def line():
    z = lax.axis_index("ctx")
    inner = (z == 1) | (z == 2)
    return z, inner, z + 1 - 2 * (z // 3), 3 * (z // 2), 3 - z


class Line:
    def __init__(self, own, pair, mate, sems, first=0):
        self.own, self.pair, self.mate = own, pair, mate
        self.sems, self.first = sems, first
        self.z, self.inner, self.to_inner, self.to_outer, self.to_mate = line()

    def _copy(self, k, p):
        src, dst, other = (
            (self.own, self.pair, self.to_inner),
            (self.pair, self.mate, self.to_mate),
            (self.pair, self.pair, self.to_outer),
        )[k]
        i = self.first + p
        return push(src.at[p], dst.at[p], self.sems[2 * k].at[i], self.sems[2 * k + 1].at[i], {"ctx": other})

    def _rows(self, body):
        tiles(self.own.shape[1], 16, body)

    def start(self, p):
        @pl.when(~self.inner)
        def _():
            self._copy(0, p).start()

    def meet(self, p):
        own, pair = self.own, self.pair

        @pl.when(self.inner)
        def _():
            self._copy(0, p).wait_recv()

            def add(at):
                pair[p, at, :] = (pair[p, at, :].astype(F32) + own[p, at, :].astype(F32)).astype(BF)

            self._rows(add)
            self._copy(1, p).start()

    def settle(self, p):
        pair, mate = self.pair, self.mate

        @pl.when(self.inner)
        def _():
            self._copy(1, p).wait_recv()
            self._copy(1, p).wait_send()

            def add(at):
                pair[p, at, :] = (pair[p, at, :].astype(F32) + mate[p, at, :].astype(F32)).astype(BF)

            self._rows(add)
            self._copy(2, p).start()

        @pl.when(~self.inner)
        def _():
            self._copy(2, p).wait_recv()

    def finish(self, p):
        @pl.when(self.inner)
        def _():
            self._copy(2, p).wait_send()

        @pl.when(~self.inner)
        def _():
            self._copy(0, p).wait_send()


def greet_all():
    z = lax.axis_index("ctx")
    barrier = pltpu.get_barrier_semaphore()
    for r in range(1, 8):
        pl.semaphore_signal(barrier, inc=1, device_id={"fsdp": peer(r)}, device_id_type=MESH)

    for d in range(1, 4):
        pl.semaphore_signal(barrier, inc=1, device_id={"ctx": (z + d) % 4}, device_id_type=MESH)
    pl.semaphore_wait(barrier, 10)


class LineGather:
    def __init__(self, full, send_up, send_down, recv):
        self.full, self.send_up, self.send_down, self.recv = full, send_up, send_down, recv
        self.z = lax.axis_index("ctx")

    def _copy(self, slot, up):
        send = (self.send_up if up else self.send_down).at[slot]
        full = self.full.at[slot]
        return push(full, full, send, self.recv.at[slot], {"ctx": self.z + 1 if up else self.z - 1})

    def _hand_up(self, slot):
        @pl.when(self.z < 3)
        def _():
            self._copy(slot, True).start()

    def _hand_down(self, slot):
        @pl.when(self.z > 0)
        def _():
            self._copy(slot, False).start()

    def start(self):
        self._hand_up(self.z)
        self._hand_down(self.z)

    def collect(self, d):
        @pl.when(self.z >= d)
        def _():
            self._copy(self.z - d, True).wait_recv()
            self._hand_up(self.z - d)

        @pl.when(self.z + d <= 3)
        def _():
            self._copy(self.z + d, False).wait_recv()
            self._hand_down(self.z + d)

    def finish(self):
        for slot in range(4):
            @pl.when((self.z < 3) & (slot <= self.z))
            def _():
                self._copy(slot, True).wait_send()

            @pl.when((self.z > 0) & (slot >= self.z))
            def _():
                self._copy(slot, False).wait_send()


def turn(u, cosine, sine):
    lane = lax.broadcasted_iota(jnp.int32, u.shape, 1)
    other = jnp.where(lane % 64 < 32, pltpu.roll(u, 96, 1), pltpu.roll(u, 32, 1))
    return u * cosine + other * sine


def halves(pair, out):
    lane = lax.broadcasted_iota(jnp.int32, pair.shape, 1)
    left = lane < 64
    swapped = pltpu.roll(pair, 64, 1)
    zero = jnp.zeros_like(pair)
    out[0, 0] = jnp.where(left, pair, zero).astype(BF)
    out[0, 1] = jnp.where(left, swapped, zero).astype(BF)
    out[1, 0] = jnp.where(left, zero, swapped).astype(BF)
    out[1, 1] = jnp.where(left, zero, pair).astype(BF)


def halves_t(pair, out, here):
    pair = pair.T
    zero = jnp.zeros((64, pair.shape[1]), BF)
    for g in range(2):
        head = pair[64 * g : 64 * g + 64].astype(BF)
        out[0, g, :64, here] = head
        out[0, g, 64:, here] = zero
        out[1, g, :64, here] = zero
        out[1, g, 64:, here] = head


def key_places(kv_ref, kcol):
    rows = kcol.shape[1]
    for j in range(4):
        digit = kv_ref[j, rows:, :].astype(F32)
        places = jnp.broadcast_to(digit[0:1] * 32.0 + digit[1:2], (128, rows))
        for lo in range(0, rows, 128):
            column = places[:, lo : lo + 128].T
            kcol[j * rows + lo : j * rows + lo + 128, :128] = column
            kcol[j * rows + lo : j * rows + lo + 128, 128:] = column


def scan_rows(count, body, init):
    return lax.fori_loop(
        0, count, lambda t, carry: body(pl.ds(pl.multiple_of(t * 64, 64), 64), carry), init, unroll=4
    )


def eights(value, op):
    parts = [value[8 * j : 8 * j + 8] for j in range(value.shape[0] // 8)]
    while len(parts) > 1:
        parts = [op(parts[j], parts[j + 1]) for j in range(0, len(parts), 2)]
    return parts[0]


def front_kernel(
    x_ref, pos_ref, cos_ref, sin_ref, wq_ref, wk_ref, wv_ref, wo_ref,
    n1_ref, bq_ref, bk_ref, bv_ref, n2_ref, wg_ref, wu_ref, cot_ref,
    xn_ref, q_ref, kv_ref, lse_ref, obt_ref, mid_ref, xn2_ref,
    wkv_ref, wq_all, wo_all, vec_ref, wgu_ref, df_ref,
    wkv_own, small_f, small_own, small_all, wgu_out, kk, vvt, score, prob, kcol, *sems,
):
    place = plane()
    me = lax.axis_index("fsdp")
    z = lax.axis_index("ctx")
    rows = x_ref.shape[0]
    ff_own, ff = wg_ref.shape[1] // 8, wgu_ref.shape[2] // 2
    greet_all()
    gkv = Gather(place, wkv_own, wkv_ref, sems[0], sems[1], by_owner=True)
    gs = Gather(place, small_own, small_all, sems[2], sems[3], by_owner=True)
    gq = Gather(place, wq_ref, wq_all, sems[4], sems[5], by_owner=True)
    go = Gather(place, wo_ref, wo_all, sems[6], sems[7], by_owner=True)
    send_u, recv_u = sems[8:10]
    gk = LineGather(kv_ref, *sems[10:13])
    gd = Gather(place, cot_ref, df_ref, sems[13], sems[14])

    wkv_own[:, :128] = wk_ref[...]
    wkv_own[:, 128:] = wv_ref[...]
    gkv.start()
    small_f[...] = jnp.zeros_like(small_f)
    small_f[0:1, :112] = n1_ref[...].astype(F32)
    small_f[1:2, :112] = bq_ref[...].astype(F32)
    small_f[2:3, :16] = bk_ref[...].astype(F32)
    small_f[2:3, 128:144] = bv_ref[...].astype(F32)
    small_f[3:4, :112] = n2_ref[...].astype(F32)
    flat = small_f[...]
    row = lax.broadcasted_iota(jnp.int32, flat.shape, 0)
    placed = jnp.where(row == 2, pltpu.roll(flat, me * 16, 1), pltpu.roll(flat, me * 112, 1))
    small_own[...] = placed.astype(BF)
    gs.start()
    gq.start()
    wkv_ref[me] = wkv_own[...]
    small_all[me] = small_own[...]
    wq_all[me] = wq_ref[...]
    wo_all[me] = wo_ref[...]
    for j in range(8):
        for half, src in ((0, wg_ref), (1, wu_ref)):
            block = src[:, j * ff_own : (j + 1) * ff_own]
            wgu_out[j, :, half * ff : half * ff + ff_own] = block
            wgu_out[j, :, half * ff + ff_own : (half + 1) * ff] = jnp.zeros(
                (src.shape[0], ff - ff_own), BF
            )
    df_ref[0] = cot_ref[...]
    place_row = pos_ref[...].astype(F32)
    high = jnp.floor(place_row * (1.0 / 32.0))
    kv_ref[z, rows : rows + 1, :] = high.astype(BF)
    kv_ref[z, rows + 1 : rows + 2, :] = (place_row - 32.0 * high).astype(BF)
    kv_ref[z, rows + 2 :, :] = jnp.zeros((14, 256), BF)

    gkv.relay()
    gs.relay()
    gkv.relay_corner()
    gs.relay_corner()
    for slot in (3, 5, 7, 1):
        gkv.wait(slot)
        gs.wait(slot)
    vec = small_all[0].astype(F32)
    for j in range(1, 8):
        vec = vec + small_all[j].astype(F32)
    vec_ref[...] = vec

    def norm_one(at):
        h = x_ref[at, :].astype(F32)
        scale = lax.rsqrt(jnp.mean(h * h, axis=-1, keepdims=True) + EPSILON)
        xn_ref[at, :] = (h * scale * vec_ref[0:1, :]).astype(BF)

    tiles(rows, 32, norm_one)
    cosine, sine = cos_ref[...], sin_ref[...]
    kv = dot(xn_ref[...], wkv_ref[...].reshape(896, 256)) + vec_ref[2:3, :256]
    kv_ref[z, :rows, :128] = turn(kv[:, :128], cosine, sine).astype(BF)
    kv_ref[z, :rows, 128:] = kv[:, 128:].astype(BF)
    gk.start()

    gq.relay()
    go.start()

    mate = z + 1 - 2 * (z % 2)
    half_of = lambda k: pl.ds(pl.multiple_of(k * ff, 128), ff)
    taken, given = half_of(z % 2), half_of(1 - z % 2)
    send_z, recv_z = sems[15:17]

    def block_to(r):
        owner = peer(r)
        src, dst = wgu_out.at[owner, :, taken], wgu_ref.at[me, :, taken]
        return push(src, dst, send_u.at[r], recv_u.at[r], {"fsdp": owner})

    def block_from(r):
        src, dst = wgu_out.at[me, :, taken], wgu_ref.at[peer(r), :, taken]
        return push(src, dst, send_u.at[r], recv_u.at[r], {"fsdp": peer(r)})

    def hand_over(r):
        block = wgu_ref.at[peer(r), :, taken]
        return push(block, block, send_z.at[r], recv_z.at[r], {"ctx": mate})

    def handed(r):
        block = wgu_ref.at[peer(r), :, given]
        return push(block, block, send_z.at[r], recv_z.at[r], {"ctx": mate})

    @pl.loop(1, 8)
    def _(i):
        block_to(8 - i).start()

    wgu_ref[me] = wgu_out[me]
    gd.start()
    gk.collect(1)
    gq.relay_corner()
    for slot in (3, 5, 7, 1):
        gq.wait(slot)

    @pl.loop(0, 7)
    def _(i):
        at = pl.ds(pl.multiple_of(i * 128, 128), 128)
        q = dot(xn_ref[...], wq_all[:, :, at].reshape(896, 128)) + vec_ref[1:2, at]
        q_ref[:, at] = (turn(q, cosine, sine) * 0.125).astype(BF)

    gk.collect(2)

    gk.collect(3)
    for j in range(4):
        here = pl.ds(j * rows, rows)
        halves(kv_ref[j, :rows, :128].astype(F32), kk.at[:, :, here])
        halves_t(kv_ref[j, :rows, 128:].astype(F32), vvt, here)
    key_places(kv_ref, kcol)
    count = 4 * rows // 64

    @pl.loop(0, 7)
    def _(i):
        lanes = pl.ds(pl.multiple_of(i * 128, 128), 128)
        heads = (2 * i, 2 * i + 1)
        for half in range(2):
            score[half] = dot_t(kk[half, heads[half] // 7], q_ref[:, lanes])

        def find_top(at, tops):
            seen = kcol[at, :] <= place_row
            found = []
            for half in range(2):
                s = jnp.where(seen, score[half, at, :], NEGATIVE)
                score[half, at, :] = s
                found.append(jnp.maximum(tops[half], eights(s, jnp.maximum)))
            return tuple(found)

        start = jnp.full((8, rows), NEGATIVE, F32)
        tops = [jnp.max(top, axis=0, keepdims=True) for top in scan_rows(count, find_top, (start, start))]

        def soft(at, totals):
            found = []
            for half in range(2):
                e = jnp.exp(score[half, at, :] - tops[half])
                prob[half, at, :] = e.astype(BF)
                found.append(totals[half] + eights(e, jnp.add))
            return tuple(found)

        start = jnp.zeros((8, rows), F32)
        totals = [jnp.sum(total, axis=0, keepdims=True) for total in scan_rows(count, soft, (start, start))]
        o = None
        for half in range(2):
            lse_ref[pl.ds(heads[half], 1), :] = tops[half] + jnp.log(totals[half])
            part = dot(vvt[half, heads[half] // 7], prob[half]) * (1.0 / totals[half])
            o = part if o is None else o + part
        obt_ref[lanes, :] = o.astype(BF)

        block_from(7 - i).wait_recv()
        hand_over(7 - i).start()

        @pl.when(i == 0)
        def _():
            go.relay()

        @pl.when(i == 5)
        def _():
            go.relay_corner()
            gd.relay()

        @pl.when(i == 6)
        def _():
            gd.relay_corner()

    for slot in (3, 5, 7, 1):
        go.wait(slot)
    for lo in range(0, 896, 128):
        mid_ref[:, lo : lo + 128] = t_dot(obt_ref[...], wo_all[:, :, lo : lo + 128].reshape(896, 128))

    def norm_two(at):
        m = mid_ref[at, :] + x_ref[at, :].astype(F32)
        mid_ref[at, :] = m
        scale = lax.rsqrt(jnp.mean(m * m, axis=-1, keepdims=True) + EPSILON)
        xn2_ref[at, :] = (m * scale * vec_ref[3:4, :]).astype(BF)

    tiles(rows, 32, norm_two)

    @pl.loop(1, 8)
    def _(r):
        block_to(r).wait_send()
        hand_over(r).wait_send()
        handed(r).wait_recv()

    for slot in (1, 3, 5, 7):
        gd.wait(slot)
    for each in (gkv, gs, gq, go, gk, gd):
        each.finish()


def front(x, pos, cosine, sine, wq, wk, wv, wo, n1, bq, bk, bv, n2, wg, wu, cot):
    dma = pltpu.SemaphoreType.DMA
    vm = pl.BlockSpec(memory_space=pltpu.VMEM)
    vmem = pltpu.VMEM
    out = jax.ShapeDtypeStruct
    rows, width = x.shape
    own = wq.shape[0]
    ff = -(-(wg.shape[1] // 8) // 128) * 128
    tokens = 4 * rows
    return pl.pallas_call(
        front_kernel,
        out_shape=(
            out((rows, width), BF), out((rows, width), BF), out((4, rows + 16, 256), BF),
            out((16, rows), F32), out((width, rows), BF), out((rows, width), F32),
            out((rows, width), BF), out((8, own, 256), BF), out((8, own, width), BF),
            out((8, own, width), BF), out((16, width), F32), out((8, own, 2 * ff), BF),
            out((8, rows, width), BF),
        ),
        in_specs=[vm] * 16,
        out_specs=(vm,) * 13,
        scratch_shapes=[
            vmem((own, 256), BF), vmem((16, width), F32), vmem((16, width), BF), vmem((8, 16, width), BF),
            vmem((8, own, 2 * ff), BF), vmem((2, 2, tokens, 128), BF), vmem((2, 2, 128, tokens), BF),
            vmem((2, tokens, rows), F32), vmem((2, tokens, rows), BF), vmem((tokens, rows), F32),
            dma((7,)), dma((8,)), dma((7,)), dma((8,)), dma((7,)), dma((8,)), dma((7,)), dma((8,)),
            dma((8,)), dma((8,)), dma((4,)), dma((4,)), dma((4,)), dma((7,)), dma((8,)), dma((8,)), dma((8,)),
        ],
        compiler_params=pltpu.CompilerParams(collective_id=2, has_side_effects=True),
    )(x, pos, cosine, sine, wq, wk, wv, wo, n1, bq, bk, bv, n2, wg, wu, cot)


def middle_kernel(
    xn2_ref, pos_ref, cos_ref, sin_ref, kv_ref, lse_ref, vec_ref,
    df_hbm, wgu_hbm, wd_hbm, x_hbm, cot_hbm, mid_hbm, xn_hbm, q_hbm, obt_hbm, wkv_hbm, wq_hbm, wo_hbm,
    out_ref, gin_ref, pair_q, pair_o, pair_k, in_u, pair_d,
    x_all, part_out, core_in, tree_in, dx, core_f, tree_f, gwgu, gwd, mate_d, pair_u, mate_u,
    core_o, tree_o, core_q, tree_q, core_k, tree_k,
    own_o, mate_o, own_q, mate_q, own_k, mate_k, dkv_in, *sems,
):
    place = plane()
    me = lax.axis_index("fsdp")
    z = lax.axis_index("ctx")
    rows, width = xn2_ref.shape
    own = width // 8
    ff, ff_own = wgu_hbm.shape[1] // 2, wd_hbm.shape[0]
    tokens, keys = 8 * rows, 4 * rows
    piece = gwd.shape[1]
    loads = sems[38]
    greet_all()
    line_sems = sems[18:24]
    ld = Line(gwd, pair_d, mate_d, line_sems, 0)
    lu = Line(gwgu, pair_u, mate_u, line_sems, 4)
    lo = Line(own_o, pair_o, mate_o, line_sems, 12)
    lq = Line(own_q, pair_q, mate_q, line_sems, 13)
    lk = Line(own_k, pair_k, mate_k, line_sems, 14)
    send_all, recv_all, send_kv, recv_kv = sems[24:28]

    def feed_forward(df_ref, wgu_ref, wd, act_all, hid_all, dgu_all, dh, part, folded):
        gx = Gather(place, xn2_ref, x_all, sems[0], sems[1])
        rd = Scatter(place, part, core_in, tree_in, folded, *sems[2:6])
        gx.start()
        fetch = [
            pltpu.make_async_copy(wgu_hbm, wgu_ref, loads.at[0]),
            pltpu.make_async_copy(wd_hbm, wd.at[pl.ds(0, ff_own)], loads.at[1]),
            pltpu.make_async_copy(df_hbm, df_ref, loads.at[2]),
        ]
        for cp in fetch:
            cp.start()
        x_all[0] = xn2_ref[...]
        wd[ff_own:] = jnp.zeros((ff - ff_own, width), BF)
        fetch[0].wait()
        fetch[1].wait()
        both = lambda ref, p: ref[pl.ds(2 * p, 2)].reshape(2 * rows, ref.shape[2])

        @pl.loop(0, 4)
        def _(p):
            @pl.when(p == 1)
            def _():
                gx.relay()

            @pl.when(p == 3)
            def _():
                gx.relay_corner()

            gx.wait(2 * p + 1)
            x = both(x_all, p)
            for n in range(0, 2 * ff, 256):
                act_all[p, :, n : n + 256] = dot(x, wgu_ref[:, n : n + 256])

            def activate(at):
                gate, up = act_all[p, at, :ff], act_all[p, at, ff:]
                sig = 0.5 * jnp.tanh(0.5 * gate) + 0.5
                hid_all[p, at, :] = (gate * sig * up).astype(BF)

            tiles(2 * rows, 16, activate)
            out = dot(hid_all[p], wd[...]).astype(BF)
            part_out[pl.ds(2 * p, 2)] = out.reshape(2, rows, width)

        fetch[2].wait()
        for p in range(4):
            gwd[p] = t_dot(
                hid_all[:, :, p * piece : (p + 1) * piece].reshape(tokens, piece),
                df_ref[...].reshape(tokens, width),
            ).astype(BF)
            ld.start(p)

        @pl.loop(0, 4)
        def _(k):
            p = 3 - k
            dh[...] = dot_t(both(df_ref, p), wd[...])

            def activate(at):
                gate, up, d = act_all[p, at, :ff], act_all[p, at, ff:], dh[at, :]
                sig = 0.5 * jnp.tanh(0.5 * gate) + 0.5
                dgu_all[p, at, :ff] = (d * up * (sig * (1.0 + gate * (1.0 - sig)))).astype(BF)
                dgu_all[p, at, ff:] = (d * (gate * sig)).astype(BF)

            tiles(2 * rows, 16, activate)
            value = dot_t(dgu_all[p], wgu_ref[...]).astype(BF)
            part[pl.ds(2 * p, 2)] = value.reshape(2, rows, width)
            rd.to_twin(p).start()

            @pl.when(k == 1)
            def _():
                rd.start_corner()

            @pl.when(k == 2)
            def _():
                ld.meet(0)

        rd.start_far()
        ld.meet(1)
        rd.relay()

        @pl.loop(0, 2 * ff // 256)
        def _(n):
            at = pl.ds(pl.multiple_of(n * 256, 256), 256)
            value = t_dot(x_all[...].reshape(tokens, width), dgu_all[:, :, at].reshape(tokens, 256))
            gwgu[:, :, at] = value.astype(BF).reshape(8, own, 256)

            @pl.when(n == 1)
            def _():
                ld.meet(2)

            @pl.when(n == 3)
            def _():
                ld.settle(0)

        for r in (7, 6, 5, 4):
            lu.start(peer(r))

        def store_dx(at, value):
            dx[at, :] = value

        rd.total(store_dx)
        gx.finish()
        rd.finish()

    pl.run_scoped(
        feed_forward,
        pltpu.VMEM((8, rows, width), BF), pltpu.VMEM((width, 2 * ff), BF), pltpu.VMEM((ff, width), BF),
        pltpu.VMEM((4, 2 * rows, 2 * ff), F32), pltpu.VMEM((4, 2 * rows, ff), BF),
        pltpu.VMEM((4, 2 * rows, 2 * ff), BF), pltpu.VMEM((2 * rows, ff), F32),
        pltpu.VMEM((8, rows, width), BF), pltpu.VMEM((3, rows, width), BF),
    )

    def attention_back(
        x_ref, cot_ref, mid_ref, xn_ref, q_ref, obt_ref, wkv_ref, wq_ref, wo_ref,
        dm, da, dob, kk, kkt, vv, kcol, score, dprob, prob, dscore, dk_acc, dv_acc,
        dq, dkv_own, dkv, dxn, small, part_o, fold_o, part_q, fold_q, part_k, fold_k, fold_f,
    ):
        ro = Scatter(place, part_o, core_o, tree_o, fold_o, *sems[6:10], by_owner=True)
        rq = Scatter(place, part_q, core_q, tree_q, fold_q, *sems[10:14], by_owner=True)
        rk = Scatter(place, part_k, core_k, tree_k, fold_k, *sems[14:18], by_owner=True)
        rf = Scatter(place, part_out, core_f, tree_f, fold_f, *sems[28:32])
        arrays = (
            (mid_hbm, mid_ref), (cot_hbm, cot_ref), (obt_hbm, obt_ref), (wo_hbm, wo_ref), (q_hbm, q_ref),
            (xn_hbm, xn_ref), (wq_hbm, wq_ref), (wkv_hbm, wkv_ref), (x_hbm, x_ref),
        )
        fetch = [pltpu.make_async_copy(src, dst, loads.at[3 + i]) for i, (src, dst) in enumerate(arrays)]
        for cp in fetch:
            cp.start()
        for k in (3, 2, 1, 0):
            rf.to_twin(k).start()
        ld.meet(3)
        ld.settle(1)
        fetch[0].wait()
        fetch[1].wait()

        small[...] = jnp.zeros_like(small)

        def norm_two(at):
            m, g = mid_ref[at, :], dx[at, :]
            scale = lax.rsqrt(jnp.mean(m * m, axis=-1, keepdims=True) + EPSILON)
            weighted = vec_ref[3:4, :] * g
            inner = jnp.mean(weighted * m, axis=-1, keepdims=True)
            d = cot_ref[at, :].astype(F32) + scale * weighted - m * (scale * scale * scale) * inner
            dm[at, :] = d
            da[at, :] = d.astype(BF)
            small[3:4, :] += jnp.sum(g * m * scale, axis=0, keepdims=True)

        tiles(rows, 32, norm_two)
        for i in range(2, 9):
            fetch[i].wait()

        @pl.loop(0, 7)
        def _(i):
            lanes = pl.ds(pl.multiple_of(i * 128, 128), 128)
            part_o[:, :, lanes] = dot(obt_ref[...], da[:, lanes]).astype(BF).reshape(8, own, 128)

        for k in (3, 2, 1, 0):
            ro.to_twin(k).start()
        dob[...] = dot_t(da[...], wo_ref[...].reshape(width, width)).astype(BF)
        for j in range(4):
            here = pl.ds(j * rows, rows)
            key, value = kv_ref[j, :rows, :128].astype(F32), kv_ref[j, :rows, 128:].astype(F32)
            halves(key, kk.at[:, :, here])
            halves(value, vv.at[:, :, here])
            halves_t(key, kkt, here)
        key_places(kv_ref, kcol)
        dk_acc[...] = jnp.zeros_like(dk_acc)
        dv_acc[...] = jnp.zeros_like(dv_acc)
        place_row = pos_ref[...].astype(F32)
        cosine, sine = cos_ref[...], -sin_ref[...]
        count = keys // 64

        def keep(total):
            def store(at, value):
                total[0, at, :] = value.astype(BF)

            return store

        def gather_to(r):
            owner = peer(r)
            return push(pair_u.at[owner], in_u.at[me], send_all.at[r], recv_all.at[me], {"fsdp": owner})

        def settle_u(r):
            lu.settle(peer(r))
            gather_to(r).start()

        ld.settle(2)

        @pl.loop(0, 7)
        def _(i):
            lanes = pl.ds(pl.multiple_of(i * 128, 128), 128)
            grad = None
            for half in range(2):
                head = 2 * i + half
                g = head // 7
                score[...] = dot_t(kk[half, g], q_ref[:, lanes])
                dprob[...] = dot_t(vv[half, g], dob[:, lanes])
                lse_row = lse_ref[pl.ds(head, 1), :]

                def find_delta(at, total):
                    s = jnp.where(kcol[at, :] <= place_row, score[at, :], NEGATIVE)
                    p = jnp.exp(s - lse_row)
                    score[at, :] = p
                    prob[at, :] = p.astype(BF)
                    return total + eights(p * dprob[at, :], jnp.add)

                delta = scan_rows(count, find_delta, jnp.zeros((8, rows), F32))
                delta = jnp.sum(delta, axis=0, keepdims=True)

                def find_score(at):
                    dscore[at, :] = (score[at, :] * (dprob[at, :] - delta)).astype(BF)

                tiles(keys, 64, find_score)
                dv_acc[half, g] += dot(prob[...], dob[:, lanes])
                dk_acc[half, g] += dot(dscore[...], q_ref[:, lanes])
                term = dot(kkt[half, g], dscore[...])
                grad = term if grad is None else grad + term
            dq[:, lanes] = turn(grad.T * 0.125, cosine, sine).astype(BF)

            @pl.when(i == 0)
            def _():
                ro.start()
                rf.start()

            @pl.when(i == 1)
            def _():
                lu.meet(peer(7))

            @pl.when(i == 2)
            def _():
                ld.settle(3)

            @pl.when(i == 3)
            def _():
                ro.relay()
                rf.relay()
                lu.meet(peer(6))

            @pl.when(i == 5)
            def _():
                lu.meet(peer(5))
                settle_u(7)
                ro.total(keep(own_o))

            @pl.when(i == 6)
            def _():
                lu.meet(peer(4))

        lane = lax.broadcasted_iota(jnp.int32, (64, 128), 1)

        def join(acc, at):
            first = jnp.where(lane < 64, acc[0, 0, at, :], acc[1, 1, at, :])
            second = jnp.where(lane < 64, acc[0, 1, at, :], acc[1, 0, at, :])
            return first + pltpu.roll(second, 64, 1)

        @pl.loop(0, 4)
        def _(j):
            for first in range(0, rows, 64):
                at = pl.ds(pl.multiple_of(j * rows + first, 64), 64)
                dkv_own[j, first : first + 64, :128] = join(dk_acc, at).astype(BF)
                dkv_own[j, first : first + 64, 128:] = join(dv_acc, at).astype(BF)

        def kv_to(d):
            other = (z + d) % 4
            return push(
                dkv_own.at[other], dkv_in.at[d - 1], send_kv.at[d - 1], recv_kv.at[d - 1], {"ctx": other}
            )

        for d in (2, 1, 3):
            kv_to(d).start()

        @pl.loop(4, 8)
        def _(i):
            lu.start(peer(7 - i))

        lo.start(0)
        settle_u(6)
        settle_u(5)

        def weight_grads(grads, part, n):
            for at in range(0, n, 128):
                value = t_dot(xn_ref[...], grads[:, at : at + 128]).astype(BF)
                part[:, :, at : at + 128] = value.reshape(8, own, 128)

        weight_grads(dq, part_q, width)
        for k in (3, 2, 1, 0):
            rq.to_twin(k).start()
        for at in range(0, width, 128):
            wq_rows = wq_ref[...].reshape(width, width)
            dxn[:, at : at + 128] = dot_t(dq[...], wq_rows[at : at + 128])
        rq.start()
        settle_u(4)

        def store_out(at, value):
            out_ref[at, :] = value + mid_ref[at, :]

        rf.total(store_out)
        for d in (1, 3, 2):
            kv_to(d).wait_recv()

        def sum_kv(at):
            value = dkv_own[z, at, :].astype(F32)
            for d in range(3):
                value = value + dkv_in[d, at, :].astype(F32)
            dkv[at, :128] = turn(value[:, :128], cos_ref[at, :], -sin_ref[at, :]).astype(BF)
            dkv[at, 128:] = value[:, 128:].astype(BF)

        tiles(rows, 32, sum_kv)
        weight_grads(dkv, part_k, 256)
        for at in range(0, width, 128):
            wkv_rows = wkv_ref[...].reshape(width, 256)
            dxn[:, at : at + 128] += dot_t(dkv[...], wkv_rows[at : at + 128])

        def norm_one(at):
            h, g = x_ref[at, :].astype(F32), dxn[at, :]
            scale = lax.rsqrt(jnp.mean(h * h, axis=-1, keepdims=True) + EPSILON)
            weighted = vec_ref[0:1, :] * g
            inner = jnp.mean(weighted * h, axis=-1, keepdims=True)
            gin_ref[at, :] = dm[at, :] + scale * weighted - h * (scale * scale * scale) * inner
            small[0:1, :] += jnp.sum(g * h * scale, axis=0, keepdims=True)
            small[1:2, :] += jnp.sum(dq[at, :].astype(F32), axis=0, keepdims=True)
            small[2:3, :256] += jnp.sum(dkv[at, :].astype(F32), axis=0, keepdims=True)

        tiles(rows, 32, norm_one)
        flat = small[...]
        line_of = lax.broadcasted_iota(jnp.int32, (16, 128), 0)
        for j in range(8):
            by_row = pltpu.roll(flat, (width - 112 * j) % width, 1)[:, :128]
            by_head = pltpu.roll(flat, (width - 16 * j) % width, 1)
            value = jnp.where(line_of == 2, by_head[:, :128], by_row)
            lifted = pltpu.roll(by_head[:, 128:256], 2, 0)
            value = jnp.where(line_of == 4, lifted, value)
            part_k[j, :16, 256:] = value.astype(BF)
            part_k[j, 16:, 256:] = jnp.zeros((own - 16, 128), BF)

        for k in (3, 2, 1, 0):
            rk.to_twin(k).start()
        lu.meet(peer(3))
        rk.start()
        rq.relay()
        lu.meet(peer(2))
        settle_u(3)
        rk.relay()
        rq.total(keep(own_q))
        lq.start(0)
        lu.meet(peer(1))
        rk.total(keep(own_k))
        lk.start(0)
        settle_u(2)
        lu.meet(me)
        settle_u(1)
        lo.meet(0)
        lu.settle(me)
        keep_own = pltpu.make_async_copy(pair_u.at[me], in_u.at[me], loads.at[12])
        keep_own.start()
        lq.meet(0)
        lo.settle(0)
        lk.meet(0)
        lq.settle(0)
        lk.settle(0)
        keep_own.wait()

        @pl.loop(1, 8)
        def _(r):
            other = peer(r)
            push(
                pair_u.at[me], in_u.at[other], send_all.at[r], recv_all.at[other], {"fsdp": other}
            ).wait_recv()
            gather_to(r).wait_send()

        for d in (1, 2, 3):
            kv_to(d).wait_send()
        for each in (ro, rq, rk, rf):
            each.finish()

    v = pltpu.VMEM
    pl.run_scoped(
        attention_back,
        v((rows, width), BF), v((rows, width), BF), v((rows, width), F32), v((rows, width), BF),
        v((rows, width), BF), v((width, rows), BF), v((8, own, 256), BF), v((8, own, width), BF),
        v((8, own, width), BF),
        v((rows, width), F32), v((rows, width), BF), v((rows, width), BF),
        v((2, 2, keys, 128), BF), v((2, 2, 128, keys), BF), v((2, 2, keys, 128), BF),
        v((keys, rows), F32), v((keys, rows), F32), v((keys, rows), F32),
        v((keys, rows), BF), v((keys, rows), BF),
        v((2, 2, keys, 128), F32), v((2, 2, keys, 128), F32),
        v((rows, width), BF), v((4, rows, 256), BF), v((rows, 256), BF), v((rows, width), F32),
        v((16, width), F32),
        v((8, own, width), BF), v((3, own, width), BF), v((8, own, width), BF), v((3, own, width), BF),
        v((8, own, 384), BF), v((3, own, 384), BF), v((3, rows, width), BF),
    )

    @pl.loop(0, 4)
    def _(p):
        ld.finish(p)

    @pl.loop(0, 8)
    def _(p):
        lu.finish(p)

    for each in (lo, lq, lk):
        each.finish(0)


def middle(xn2, pos, cosine, sine, kv, lse, vec, df_all, wgu, wd, x, cot, mid, xn, q, obt, wkv, wq, wo):
    dma = pltpu.SemaphoreType.DMA
    vm = pl.BlockSpec(memory_space=pltpu.VMEM)
    hbm = pl.BlockSpec(memory_space=pl.ANY)
    v = pltpu.VMEM
    out = jax.ShapeDtypeStruct
    rows, width = x.shape
    own = width // 8
    ff = wgu.shape[1] // 2
    gu, gd = (8, own, 2 * ff), (4, ff // 4, width)
    wide, narrow = (1, own, width), (1, own, 384)
    tree = [dma((4,)), dma((4,)), dma((3,)), dma((3,))]
    return pl.pallas_call(
        middle_kernel,
        out_shape=(
            out((rows, width), F32), out((rows, width), F32), out(wide, BF), out(wide, BF), out(narrow, BF),
            out(gu, BF), out(gd, BF),
        ),
        in_specs=[vm] * 7 + [hbm] * 12,
        out_specs=(vm, vm, vm, vm, vm, hbm, vm),
        scratch_shapes=[
            v((8, rows, width), BF), v((8, rows, width), BF), v((4, rows, width), BF), v((3, rows, width), BF),
            v((rows, width), F32), v((4, rows, width), BF), v((3, rows, width), BF),
            v(gu, BF), v(gd, BF), v(gd, BF), v(gu, BF), v(gu, BF),
            v((4, own, width), BF), v((3, own, width), BF), v((4, own, width), BF), v((3, own, width), BF),
            v((4, own, 384), BF), v((3, own, 384), BF),
            v(wide, BF), v(wide, BF), v(wide, BF), v(wide, BF), v(narrow, BF), v(narrow, BF),
            v((3, rows, 256), BF),
            dma((7,)), dma((8,)), *tree, *tree, *tree, *tree,
            *[dma((15,))] * 6,
            dma((8,)), dma((8,)), dma((3,)), dma((3,)), *tree,
            *[dma((1,))] * 6, dma((13,)),
        ],
        compiler_params=pltpu.CompilerParams(
            collective_id=0, has_side_effects=True, vmem_limit_bytes=67043328
        ),
    )(xn2, pos, cosine, sine, kv, lse, vec, df_all, wgu, wd, x, cot, mid, xn, q, obt, wkv, wq, wo)


def results_kernel(
    out_ref, gin_ref, tq_ref, to_ref, tk_ref, tu_ref, td_ref,
    o_ref, i_ref, n1_ref, q_ref, bq_ref, k_ref, bk_ref, v_ref, bv_ref, w_ref, n2_ref, g_ref, u_ref, d_ref,
):
    o_ref[...] = out_ref[...]
    i_ref[...] = gin_ref[...]
    q_ref[...] = tq_ref[0].astype(F32)
    w_ref[...] = to_ref[0].astype(F32)
    k_ref[...] = tk_ref[0, :, :128].astype(F32)
    v_ref[...] = tk_ref[0, :, 128:256].astype(F32)
    small = tk_ref[0, :16, 256:].astype(F32)
    for i, ref in enumerate((n1_ref, bq_ref, bk_ref, n2_ref, bv_ref)):
        ref[...] = small[i : i + 1, : ref.shape[1]]
    ff_own, ff = d_ref.shape[0], tu_ref.shape[2] // 2
    for j in range(8):
        def place_block(at):
            g_ref[at, j * ff_own : (j + 1) * ff_own] = tu_ref[j, at, :ff_own].astype(F32)
            u_ref[at, j * ff_own : (j + 1) * ff_own] = tu_ref[j, at, ff : ff + ff_own].astype(F32)

        tiles(tu_ref.shape[1], 16, place_block)
    rows = td_ref.shape[1]
    for p in range(4):
        count = min(rows, ff_own - p * rows)
        d_ref[p * rows : p * rows + count] = td_ref[p, :count].astype(F32)


def results(out, gin, tq, to, tk, tu, td, ff_own):
    vm = pl.BlockSpec(memory_space=pltpu.VMEM)
    rows, width = out.shape
    own = width // 8
    shapes = (
        (rows, width), (rows, width), (1, own), (own, 896), (1, own), (own, 128), (1, 16), (own, 128), (1, 16),
        (own, 896), (1, own), (own, 8 * ff_own), (own, 8 * ff_own), (ff_own, width),
    )
    return pl.pallas_call(
        results_kernel,
        out_shape=tuple(jax.ShapeDtypeStruct(shape, F32) for shape in shapes),
        in_specs=[vm] * 7,
        out_specs=(vm,) * 14,
    )(out, gin, tq, to, tk, tu, td)


def shards(
    inputs, positions, cotangent, norm_one, w_query, b_query, key_projection, b_key,
    value_projection, value_bias, w_out, norm_two, w_gate, w_up, w_down,
):
    places = positions[0]
    turned = angles_of(places)
    cosine, sine = jnp.cos(turned), jnp.sin(turned)
    sine = jnp.where(jnp.arange(128)[None, :] % 64 < 32, -sine, sine)
    own = w_query.shape[1]
    ff_own = w_down.shape[1]
    ff = -(-ff_own // 128) * 128
    x, cot = inputs[0], cotangent[0]
    xn, q, kv, lse, obt, mid, xn2, wkv, wq, wo, vec, wgu, df_all = front(
        x, positions, cosine, sine, w_query[0], key_projection[0], value_projection[0], w_out[0],
        norm_one, b_query, b_key, value_bias, norm_two, w_gate[0], w_up[0], cot,
    )
    totals = middle(
        xn2, positions, cosine, sine, kv, lse, vec, df_all, wgu.reshape(-1, 2 * ff), w_down[0],
        x, cot, mid, xn, q, obt, wkv, wq, wo,
    )
    matrix = lambda i: i in (0, 1, 3, 5, 7, 9, 11, 12, 13)
    return tuple(g[None] if matrix(i) else g for i, g in enumerate(results(*totals, ff_own)))


def angles_of(places):
    half = HEAD_SIZE // 2
    inverse = jnp.exp(jnp.arange(half, dtype=F32) * (-2.0 * math.log(ROPE_BASE) / HEAD_SIZE))
    return places.astype(F32)[:, None] * jnp.concatenate([inverse] * 4)[None, :]


def shards_general(
    inputs, positions, cotangent, norm_one, w_query, b_query, key_projection, b_key,
    value_projection, value_bias, w_out, norm_two, w_gate, w_up, w_down,
):
    rows = inputs.shape[1]
    width = inputs.shape[2]
    group = QUERY_HEADS // KEY_VALUE_HEADS
    q_cols = w_query.shape[2]
    kv_cols = key_projection.shape[2]
    score_scale = 1.0 / math.sqrt(HEAD_SIZE)

    places = positions[0]
    key_places = lax.all_gather(places, "ctx", axis=0, tiled=True)
    cosine, sine = angles(places)
    hidden = inputs[0].astype(F32)

    packed = jnp.concatenate([w_query[0], key_projection[0], value_projection[0], w_out[0]], axis=1)
    packed = lax.all_gather(packed, "fsdp", axis=0, tiled=True)
    w_qkv = packed[:, : q_cols + 2 * kv_cols]
    w_o = packed[:, q_cols + 2 * kv_cols :]
    small = jnp.concatenate([norm_one[0], b_query[0], b_key[0], value_bias[0], norm_two[0]])
    small = lax.all_gather(small, "fsdp", axis=0).astype(F32)
    cuts, at = [], 0
    for piece in (norm_one, b_query, b_key, value_bias, norm_two):
        n = piece.shape[1]
        cuts.append(small[:, at : at + n].reshape(-1))
        at += n
    gain_one, bias_q, bias_k, bias_v, gain_two = cuts
    bias = jnp.concatenate([bias_q, bias_k, bias_v])

    grad_branch = cotangent[0]
    df_all = lax.all_gather(grad_branch, "fsdp", axis=0, tiled=True)
    wg = lax.all_to_all(w_gate[0], "fsdp", split_axis=1, concat_axis=0, tiled=True)
    wu = lax.all_to_all(w_up[0], "fsdp", split_axis=1, concat_axis=0, tiled=True)
    wd = w_down[0]

    scale_one, normed = norm_rows(hidden, gain_one)
    qkv = dot(normed, w_qkv) + bias
    q = rotate(qkv[:, :q_cols].reshape(rows, QUERY_HEADS, HEAD_SIZE), cosine, sine).astype(BF)
    k = rotate(
        qkv[:, q_cols : q_cols + kv_cols].reshape(rows, KEY_VALUE_HEADS, HEAD_SIZE), cosine, sine
    ).astype(BF)
    v = qkv[:, q_cols + kv_cols :].astype(BF)
    kv = jnp.concatenate([k.reshape(rows, kv_cols), v], axis=1)
    kv = lax.all_gather(kv, "ctx", axis=0, tiled=True)
    total = kv.shape[0]
    k_all = kv[:, :kv_cols].reshape(total, KEY_VALUE_HEADS, HEAD_SIZE)
    v_all = kv[:, kv_cols:].reshape(total, KEY_VALUE_HEADS, HEAD_SIZE)
    q = q.reshape(rows, KEY_VALUE_HEADS, group, HEAD_SIZE)
    s = jnp.einsum("tgjd,ugd->gjtu", q, k_all, preferred_element_type=F32) * score_scale
    s = jnp.where(key_places[None, :] <= places[:, None], s, NEGATIVE)
    top = jnp.max(s, axis=-1, keepdims=True)
    lse = top + jnp.log(jnp.sum(jnp.exp(s - top), axis=-1, keepdims=True))
    pf = jnp.exp(s - lse)
    p = pf.astype(BF)
    o = jnp.einsum("gjtu,ugd->tgjd", p, v_all, preferred_element_type=F32)
    ob = o.reshape(rows, q_cols).astype(BF)
    middle = hidden + dot(ob, w_o)
    scale_two, normed_two = norm_rows(middle, gain_two)

    x_all = lax.all_gather(normed_two, "fsdp", axis=0, tiled=True)
    gate = dot(x_all, wg)
    up = dot(x_all, wu)
    sig = jax.nn.sigmoid(gate)
    hid = (gate * sig * up).astype(BF)
    out_part = dot(hid, wd).astype(BF)
    ffn_out = lax.psum_scatter(out_part, "fsdp", scatter_dimension=0, tiled=True)
    output = middle + ffn_out.astype(F32)

    dhid = dot_t(df_all, wd)
    dgate = (dhid * up * sig * (1.0 + gate * (1.0 - sig))).astype(BF)
    dup = (dhid * (gate * sig)).astype(BF)
    dx_part = (dot_t(dgate, wg) + dot_t(dup, wu)).astype(BF)
    dxn2 = lax.psum_scatter(dx_part, "fsdp", scatter_dimension=0, tiled=True).astype(F32)
    g_down = t_dot(hid, df_all)
    g_gate = t_dot(x_all, dgate)
    g_up = t_dot(x_all, dup)

    g_out = grad_branch.astype(F32)
    grad_gain_two, dmid = norm_back(middle, scale_two, gain_two, dxn2)
    dm = g_out + dmid
    da = dm.astype(BF)
    g_wo = t_dot(ob, da)
    dob = dot_t(da, w_o).astype(BF).reshape(rows, KEY_VALUE_HEADS, group, HEAD_SIZE)

    dp = jnp.einsum("tgjd,ugd->gjtu", dob, v_all, preferred_element_type=F32)
    delta = jnp.sum(pf * dp, axis=-1, keepdims=True)
    ds = (pf * (dp - delta)).astype(BF)
    dq = jnp.einsum("gjtu,ugd->tgjd", ds, k_all, preferred_element_type=F32) * score_scale
    dk = jnp.einsum("gjtu,tgjd->ugd", ds, q, preferred_element_type=F32) * score_scale
    dv = jnp.einsum("gjtu,tgjd->ugd", p, dob, preferred_element_type=F32)
    dkv = jnp.concatenate([dk.reshape(total, kv_cols), dv.reshape(total, kv_cols)], axis=1)
    dkv = lax.psum_scatter(dkv, "ctx", scatter_dimension=0, tiled=True)
    dq = rotate(dq.reshape(rows, QUERY_HEADS, HEAD_SIZE), cosine, -sine).astype(BF)
    dk = rotate(
        dkv[:, :kv_cols].reshape(rows, KEY_VALUE_HEADS, HEAD_SIZE), cosine, -sine
    ).astype(BF)
    dqkv = jnp.concatenate(
        [dq.reshape(rows, q_cols), dk.reshape(rows, kv_cols), dkv[:, kv_cols:].astype(BF)], axis=1
    )
    g_qkv = t_dot(normed, dqkv)
    g_bias = jnp.sum(dqkv.astype(F32), axis=0)
    dxn = dot_t(dqkv, w_qkv)
    grad_gain_one, dhidden = norm_back(hidden, scale_one, gain_one, dxn)
    grad_in = dm + dhidden

    g_attn = jnp.concatenate([g_qkv, g_wo], axis=1).astype(BF)
    g_attn = lax.psum_scatter(g_attn, "fsdp", scatter_dimension=0, tiled=True)
    back = [
        lax.all_to_all(g.astype(BF), "fsdp", split_axis=0, concat_axis=1, tiled=True)
        for g in (g_gate, g_up)
    ]
    g_attn, g_gate, g_up, g_down = lax.psum((g_attn, back[0], back[1], g_down.astype(BF)), "ctx")
    pieces = jnp.concatenate(
        [
            g.reshape(small.shape[0], -1)
            for g in (
                grad_gain_one, g_bias[:q_cols], g_bias[q_cols : q_cols + kv_cols],
                g_bias[q_cols + kv_cols :], grad_gain_two,
            )
        ],
        axis=1,
    )
    pieces = lax.psum(pieces, ("ctx", "fsdp"))
    mine = lax.dynamic_slice_in_dim(pieces, lax.axis_index("fsdp"), 1, axis=0)
    outs, at = [], 0
    for piece in (norm_one, b_query, b_key, value_bias, norm_two):
        n = piece.shape[1]
        outs.append(mine[:, at : at + n])
        at += n
    g_n1, g_bq, g_bk, g_bv, g_n2 = outs
    g_attn = g_attn.astype(F32)
    return (
        output[None], grad_in[None], g_n1,
        g_attn[None, :, :q_cols], g_bq,
        g_attn[None, :, q_cols : q_cols + kv_cols], g_bk,
        g_attn[None, :, q_cols + kv_cols : q_cols + 2 * kv_cols], g_bv,
        g_attn[None, :, q_cols + 2 * kv_cols :], g_n2,
        g_gate.astype(F32)[None], g_up.astype(F32)[None], g_down.astype(F32)[None],
    )


def solution(mesh):
    tok, row, vec = P("fsdp", "ctx", None), P(None, "fsdp", None), P(None, "fsdp")
    fast = mesh.shape["ctx"] == 4 and mesh.shape["fsdp"] == 8
    return jax.shard_map(
        shards if fast else shards_general,
        mesh=mesh,
        in_specs=(
            tok, P("fsdp", "ctx"), tok, vec, row, vec, row, vec, row, vec, row, vec, row, row, row,
        ),
        out_specs=(tok, tok, vec, row, vec, row, vec, row, vec, row, vec, row, row, row),
        check_vma=False,
    )
```

```python
import functools
import math

import jax
import jax.numpy as jnp
from jax import lax
from jax.experimental import pallas as pl
from jax.experimental.pallas import tpu as pltpu
from jax.sharding import PartitionSpec as P

QUERY_HEADS = 14
KEY_VALUE_HEADS = 2
HEAD_SIZE = 64
ROPE_BASE = 1000000.0
EPSILON = 1e-06
NEGATIVE = -1e30
BF = jnp.bfloat16
F32 = jnp.float32
MESH = pl.DeviceIdType.MESH


def angles(places):
    half = HEAD_SIZE // 2
    inverse = jnp.exp(jnp.arange(half, dtype=F32) * (-2.0 * math.log(ROPE_BASE) / HEAD_SIZE))
    turned = places.astype(F32)[:, None] * inverse[None, :]
    return jnp.cos(turned)[:, None, :], jnp.sin(turned)[:, None, :]


def rotate(u, cosine, sine):
    half = u.shape[-1] // 2
    a, b = u[..., :half], u[..., half:]
    return jnp.concatenate([a * cosine - b * sine, b * cosine + a * sine], axis=-1)


def norm_rows(hidden, gain):
    scale = lax.rsqrt(jnp.mean(hidden * hidden, axis=-1, keepdims=True) + EPSILON)
    return scale, (hidden * scale * gain).astype(BF)


def norm_back(hidden, scale, gain, grad):
    weighted = gain * grad
    grad_gain = jnp.sum(grad * hidden * scale, axis=0)
    inner = jnp.mean(weighted * hidden, axis=-1, keepdims=True)
    return grad_gain, scale * weighted - hidden * (scale * scale * scale) * inner


def dot(a, b):
    return jnp.dot(a, b, preferred_element_type=F32)


def dot_t(a, b):
    return lax.dot_general(a, b, (((1,), (1,)), ((), ())), preferred_element_type=F32)


def t_dot(a, b):
    return lax.dot_general(a, b, (((0,), (0,)), ((), ())), preferred_element_type=F32)


def plane():
    f = lax.axis_index("fsdp")
    core, x, y = f % 2, (f // 2) % 2, f // 4
    by_x, by_y = f + 2 - 4 * x, f + 4 - 8 * y
    twin = f + 1 - 2 * core
    near = by_x + core * (by_y - by_x)
    far = by_y + core * (by_x - by_y)
    return twin, near, far, 2 + 2 * core, 4 - 2 * core


def tiles(rows, step, body):
    count = rows // step
    unroll = count if count <= 10 else 4

    @pl.loop(0, count, unroll=unroll)
    def _(r):
        body(pl.ds(pl.multiple_of(r * step, step), step))


def peer(r):
    f = lax.axis_index("fsdp")
    core, x, y = f % 2, (f // 2) % 2, f // 4
    return f + (r % 2) * (1 - 2 * core) + ((r // 2) % 2) * (2 - 4 * x) + (r // 4) * (4 - 8 * y)


def greet(others):
    barrier = pltpu.get_barrier_semaphore()
    for other in others:
        pl.semaphore_signal(barrier, inc=1, device_id=other, device_id_type=MESH)
    pl.semaphore_wait(barrier, len(others))


def push(src, dst, send, recv, other):
    return pltpu.make_async_remote_copy(
        src_ref=src, dst_ref=dst, send_sem=send, recv_sem=recv, device_id=other, device_id_type=MESH
    )


class Gather:
    def __init__(self, place, mine, full, send, recv, by_owner=False):
        self.twin, self.near, self.far, self.s_near, self.s_far = place
        self.mine, self.full, self.send, self.recv = mine, full, send, recv
        self.by_owner = by_owner

    def copy(self, i):
        twin, near, far = self.twin, self.near, self.far
        here = (0, 0, 0, self.s_near, 2, 4, 6)[i]
        there, other = (
            (self.s_near, near), (self.s_far, far), (1, twin), (6, far), (3, twin), (5, twin), (7, twin)
        )[i]
        if self.by_owner:
            here = there = peer(here)
        src = self.mine if i < 3 else self.full.at[here]
        return push(src, self.full.at[there], self.send.at[i], self.recv.at[there], {"fsdp": other})

    def start(self):
        for i in range(3):
            self.copy(i).start()

    def wait(self, slot):
        slot = peer(slot) if self.by_owner else slot
        full = self.full.at[slot]
        push(full, full, self.send.at[0], self.recv.at[slot], {"fsdp": self.near}).wait_recv()

    def relay(self):
        self.wait(2)
        self.wait(4)
        for i in range(3, 6):
            self.copy(i).start()

    def relay_corner(self):
        self.wait(6)
        self.copy(6).start()

    def finish(self):
        for i in range(7):
            self.copy(i).wait_send()


class Scatter:
    def __init__(
        self, place, part, core_in, tree_in, folded, send_core, recv_core, send_tree, recv_tree,
        by_owner=False,
    ):
        self.twin, self.near, self.far, self.s_near, self.s_far = place
        self.at = peer if by_owner else lambda slot: slot
        self.part, self.core_in, self.tree_in, self.folded = part, core_in, tree_in, folded
        self.send_core, self.recv_core = send_core, recv_core
        self.send_tree, self.recv_tree = send_tree, recv_tree

    def to_twin(self, k):
        return push(
            self.part.at[self.at(2 * k + 1)], self.core_in.at[k], self.send_core.at[k], self.recv_core.at[k],
            {"fsdp": self.twin},
        )

    def tree(self, j):
        other = (self.far, self.near, self.far)[j]
        return push(
            self.folded.at[j], self.tree_in.at[j], self.send_tree.at[j], self.recv_tree.at[j],
            {"fsdp": other},
        )

    def fold(self, j, slot, corner=False):
        part, core_in, tree_in, folded = self.part, self.core_in, self.tree_in, self.folded
        k = slot // 2
        slot = self.at(slot)

        def add(at):
            value = part[slot, at, :].astype(F32) + core_in[k, at, :].astype(F32)
            if corner:
                value = value + tree_in[0, at, :].astype(F32)
            folded[j, at, :] = value.astype(BF)

        tiles(part.shape[1], 16, add)

    def start_corner(self):
        self.to_twin(3).wait_recv()
        self.fold(0, 6)
        self.tree(0).start()

    def start_far(self):
        self.to_twin(1).wait_recv()
        self.to_twin(2).wait_recv()
        self.fold(2, self.s_far)
        self.tree(2).start()

    def start(self):
        self.start_corner()
        self.start_far()

    def relay(self):
        self.tree(0).wait_recv()
        self.fold(1, self.s_near, True)
        self.tree(1).start()

    def total(self, store):
        part, core_in, tree_in = self.part, self.core_in, self.tree_in
        mine = self.at(0)
        self.to_twin(0).wait_recv()
        self.tree(1).wait_recv()
        self.tree(2).wait_recv()

        def add(at):
            value = part[mine, at, :].astype(F32) + core_in[0, at, :].astype(F32)
            store(at, value + tree_in[1, at, :].astype(F32) + tree_in[2, at, :].astype(F32))

        tiles(part.shape[1], 16, add)

    def finish(self):
        for k in range(4):
            self.to_twin(k).wait_send()
        for j in range(3):
            self.tree(j).wait_send()


def line():
    z = lax.axis_index("ctx")
    inner = (z == 1) | (z == 2)
    return z, inner, z + 1 - 2 * (z // 3), 3 * (z // 2), 3 - z


class Line:
    def __init__(self, own, pair, mate, sems, first=0):
        self.own, self.pair, self.mate = own, pair, mate
        self.sems, self.first = sems, first
        self.z, self.inner, self.to_inner, self.to_outer, self.to_mate = line()

    def _copy(self, k, p):
        src, dst, other = (
            (self.own, self.pair, self.to_inner),
            (self.pair, self.mate, self.to_mate),
            (self.pair, self.pair, self.to_outer),
        )[k]
        i = self.first + p
        return push(src.at[p], dst.at[p], self.sems[2 * k].at[i], self.sems[2 * k + 1].at[i], {"ctx": other})

    def _rows(self, body):
        tiles(self.own.shape[1], 16, body)

    def start(self, p):
        @pl.when(~self.inner)
        def _():
            self._copy(0, p).start()

    def meet(self, p):
        own, pair = self.own, self.pair

        @pl.when(self.inner)
        def _():
            self._copy(0, p).wait_recv()

            def add(at):
                pair[p, at, :] = (pair[p, at, :].astype(F32) + own[p, at, :].astype(F32)).astype(BF)

            self._rows(add)
            self._copy(1, p).start()

    def settle(self, p):
        pair, mate = self.pair, self.mate

        @pl.when(self.inner)
        def _():
            self._copy(1, p).wait_recv()
            self._copy(1, p).wait_send()

            def add(at):
                pair[p, at, :] = (pair[p, at, :].astype(F32) + mate[p, at, :].astype(F32)).astype(BF)

            self._rows(add)
            self._copy(2, p).start()

        @pl.when(~self.inner)
        def _():
            self._copy(2, p).wait_recv()

    def finish(self, p):
        @pl.when(self.inner)
        def _():
            self._copy(2, p).wait_send()

        @pl.when(~self.inner)
        def _():
            self._copy(0, p).wait_send()


def greet_all():
    z = lax.axis_index("ctx")
    barrier = pltpu.get_barrier_semaphore()
    for r in range(1, 8):
        pl.semaphore_signal(barrier, inc=1, device_id={"fsdp": peer(r)}, device_id_type=MESH)

    for d in range(1, 4):
        pl.semaphore_signal(barrier, inc=1, device_id={"ctx": (z + d) % 4}, device_id_type=MESH)
    pl.semaphore_wait(barrier, 10)


class LineGather:
    def __init__(self, full, send_up, send_down, recv):
        self.full, self.send_up, self.send_down, self.recv = full, send_up, send_down, recv
        self.z = lax.axis_index("ctx")

    def _copy(self, slot, up):
        send = (self.send_up if up else self.send_down).at[slot]
        full = self.full.at[slot]
        return push(full, full, send, self.recv.at[slot], {"ctx": self.z + 1 if up else self.z - 1})

    def _hand_up(self, slot):
        @pl.when(self.z < 3)
        def _():
            self._copy(slot, True).start()

    def _hand_down(self, slot):
        @pl.when(self.z > 0)
        def _():
            self._copy(slot, False).start()

    def start(self):
        self._hand_up(self.z)
        self._hand_down(self.z)

    def collect(self, d):
        @pl.when(self.z >= d)
        def _():
            self._copy(self.z - d, True).wait_recv()
            self._hand_up(self.z - d)

        @pl.when(self.z + d <= 3)
        def _():
            self._copy(self.z + d, False).wait_recv()
            self._hand_down(self.z + d)

    def finish(self):
        for slot in range(4):
            @pl.when((self.z < 3) & (slot <= self.z))
            def _():
                self._copy(slot, True).wait_send()

            @pl.when((self.z > 0) & (slot >= self.z))
            def _():
                self._copy(slot, False).wait_send()


def turn(u, cosine, sine):
    lane = lax.broadcasted_iota(jnp.int32, u.shape, 1)
    other = jnp.where(lane % 64 < 32, pltpu.roll(u, 96, 1), pltpu.roll(u, 32, 1))
    return u * cosine + other * sine


def halves(pair, out):
    lane = lax.broadcasted_iota(jnp.int32, pair.shape, 1)
    left = lane < 64
    swapped = pltpu.roll(pair, 64, 1)
    zero = jnp.zeros_like(pair)
    out[0, 0] = jnp.where(left, pair, zero).astype(BF)
    out[0, 1] = jnp.where(left, swapped, zero).astype(BF)
    out[1, 0] = jnp.where(left, zero, swapped).astype(BF)
    out[1, 1] = jnp.where(left, zero, pair).astype(BF)


def halves_t(pair, out, here):
    pair = pair.T
    zero = jnp.zeros((64, pair.shape[1]), BF)
    for g in range(2):
        head = pair[64 * g : 64 * g + 64].astype(BF)
        out[0, g, :64, here] = head
        out[0, g, 64:, here] = zero
        out[1, g, :64, here] = zero
        out[1, g, 64:, here] = head


def key_places(kv_ref, kcol):
    rows = kcol.shape[1]
    for j in range(4):
        digit = kv_ref[j, rows:, :].astype(F32)
        places = jnp.broadcast_to(digit[0:1] * 32.0 + digit[1:2], (128, rows))
        for lo in range(0, rows, 128):
            column = places[:, lo : lo + 128].T
            kcol[j * rows + lo : j * rows + lo + 128, :128] = column
            kcol[j * rows + lo : j * rows + lo + 128, 128:] = column


def scan_rows(count, body, init):
    return lax.fori_loop(
        0, count, lambda t, carry: body(pl.ds(pl.multiple_of(t * 64, 64), 64), carry), init, unroll=4
    )


def eights(value, op):
    parts = [value[8 * j : 8 * j + 8] for j in range(value.shape[0] // 8)]
    while len(parts) > 1:
        parts = [op(parts[j], parts[j + 1]) for j in range(0, len(parts), 2)]
    return parts[0]


def front_kernel(
    x_ref, pos_ref, cos_ref, sin_ref, wq_ref, wk_ref, wv_ref, wo_ref,
    n1_ref, bq_ref, bk_ref, bv_ref, n2_ref, wg_ref, wu_ref, cot_ref,
    xn_ref, q_ref, kv_ref, lse_ref, obt_ref, mid_ref, xn2_ref,
    wkv_ref, wq_all, wo_all, vec_ref, wgu_ref, df_ref,
    wkv_own, small_f, small_own, small_all, wgu_out, kk, vvt, score, prob, kcol, *sems,
):
    place = plane()
    me = lax.axis_index("fsdp")
    z = lax.axis_index("ctx")
    rows = x_ref.shape[0]
    ff_own, ff = wg_ref.shape[1] // 8, wgu_ref.shape[2] // 2
    greet_all()
    gkv = Gather(place, wkv_own, wkv_ref, sems[0], sems[1], by_owner=True)
    gs = Gather(place, small_own, small_all, sems[2], sems[3], by_owner=True)
    gq = Gather(place, wq_ref, wq_all, sems[4], sems[5], by_owner=True)
    go = Gather(place, wo_ref, wo_all, sems[6], sems[7], by_owner=True)
    send_u, recv_u = sems[8:10]
    gk = LineGather(kv_ref, *sems[10:13])
    gd = Gather(place, cot_ref, df_ref, sems[13], sems[14])

    wkv_own[:, :128] = wk_ref[...]
    wkv_own[:, 128:] = wv_ref[...]
    gkv.start()
    small_f[...] = jnp.zeros_like(small_f)
    small_f[0:1, :112] = n1_ref[...].astype(F32)
    small_f[1:2, :112] = bq_ref[...].astype(F32)
    small_f[2:3, :16] = bk_ref[...].astype(F32)
    small_f[2:3, 128:144] = bv_ref[...].astype(F32)
    small_f[3:4, :112] = n2_ref[...].astype(F32)
    flat = small_f[...]
    row = lax.broadcasted_iota(jnp.int32, flat.shape, 0)
    placed = jnp.where(row == 2, pltpu.roll(flat, me * 16, 1), pltpu.roll(flat, me * 112, 1))
    small_own[...] = placed.astype(BF)
    gs.start()
    gq.start()
    wkv_ref[me] = wkv_own[...]
    small_all[me] = small_own[...]
    wq_all[me] = wq_ref[...]
    wo_all[me] = wo_ref[...]
    for j in range(8):
        for half, src in ((0, wg_ref), (1, wu_ref)):
            block = src[:, j * ff_own : (j + 1) * ff_own]
            wgu_out[j, :, half * ff : half * ff + ff_own] = block
            wgu_out[j, :, half * ff + ff_own : (half + 1) * ff] = jnp.zeros(
                (src.shape[0], ff - ff_own), BF
            )
    df_ref[0] = cot_ref[...]
    place_row = pos_ref[...].astype(F32)
    high = jnp.floor(place_row * (1.0 / 32.0))
    kv_ref[z, rows : rows + 1, :] = high.astype(BF)
    kv_ref[z, rows + 1 : rows + 2, :] = (place_row - 32.0 * high).astype(BF)
    kv_ref[z, rows + 2 :, :] = jnp.zeros((14, 256), BF)

    gkv.relay()
    gs.relay()
    gkv.relay_corner()
    gs.relay_corner()
    for slot in (3, 5, 7, 1):
        gkv.wait(slot)
        gs.wait(slot)
    vec = small_all[0].astype(F32)
    for j in range(1, 8):
        vec = vec + small_all[j].astype(F32)
    vec_ref[...] = vec

    def norm_one(at):
        h = x_ref[at, :].astype(F32)
        scale = lax.rsqrt(jnp.mean(h * h, axis=-1, keepdims=True) + EPSILON)
        xn_ref[at, :] = (h * scale * vec_ref[0:1, :]).astype(BF)

    tiles(rows, 32, norm_one)
    cosine, sine = cos_ref[...], sin_ref[...]
    kv = dot(xn_ref[...], wkv_ref[...].reshape(896, 256)) + vec_ref[2:3, :256]
    kv_ref[z, :rows, :128] = turn(kv[:, :128], cosine, sine).astype(BF)
    kv_ref[z, :rows, 128:] = kv[:, 128:].astype(BF)
    gk.start()

    gq.relay()
    go.start()

    mate = z + 1 - 2 * (z % 2)
    half_of = lambda k: pl.ds(pl.multiple_of(k * ff, 128), ff)
    taken, given = half_of(z % 2), half_of(1 - z % 2)
    send_z, recv_z = sems[15:17]

    def block_to(r):
        owner = peer(r)
        src, dst = wgu_out.at[owner, :, taken], wgu_ref.at[me, :, taken]
        return push(src, dst, send_u.at[r], recv_u.at[r], {"fsdp": owner})

    def block_from(r):
        src, dst = wgu_out.at[me, :, taken], wgu_ref.at[peer(r), :, taken]
        return push(src, dst, send_u.at[r], recv_u.at[r], {"fsdp": peer(r)})

    def hand_over(r):
        block = wgu_ref.at[peer(r), :, taken]
        return push(block, block, send_z.at[r], recv_z.at[r], {"ctx": mate})

    def handed(r):
        block = wgu_ref.at[peer(r), :, given]
        return push(block, block, send_z.at[r], recv_z.at[r], {"ctx": mate})

    @pl.loop(1, 8)
    def _(i):
        block_to(8 - i).start()

    wgu_ref[me] = wgu_out[me]
    gd.start()
    gk.collect(1)
    gq.relay_corner()
    for slot in (3, 5, 7, 1):
        gq.wait(slot)

    @pl.loop(0, 7)
    def _(i):
        at = pl.ds(pl.multiple_of(i * 128, 128), 128)
        q = dot(xn_ref[...], wq_all[:, :, at].reshape(896, 128)) + vec_ref[1:2, at]
        q_ref[:, at] = (turn(q, cosine, sine) * 0.125).astype(BF)

    gk.collect(2)

    gk.collect(3)
    for j in range(4):
        here = pl.ds(j * rows, rows)
        halves(kv_ref[j, :rows, :128].astype(F32), kk.at[:, :, here])
        halves_t(kv_ref[j, :rows, 128:].astype(F32), vvt, here)
    key_places(kv_ref, kcol)
    count = 4 * rows // 64

    @pl.loop(0, 7)
    def _(i):
        lanes = pl.ds(pl.multiple_of(i * 128, 128), 128)
        heads = (2 * i, 2 * i + 1)
        for half in range(2):
            score[half] = dot_t(kk[half, heads[half] // 7], q_ref[:, lanes])

        def find_top(at, tops):
            seen = kcol[at, :] <= place_row
            found = []
            for half in range(2):
                s = jnp.where(seen, score[half, at, :], NEGATIVE)
                score[half, at, :] = s
                found.append(jnp.maximum(tops[half], eights(s, jnp.maximum)))
            return tuple(found)

        start = jnp.full((8, rows), NEGATIVE, F32)
        tops = [jnp.max(top, axis=0, keepdims=True) for top in scan_rows(count, find_top, (start, start))]

        def soft(at, totals):
            found = []
            for half in range(2):
                e = jnp.exp(score[half, at, :] - tops[half])
                prob[half, at, :] = e.astype(BF)
                found.append(totals[half] + eights(e, jnp.add))
            return tuple(found)

        start = jnp.zeros((8, rows), F32)
        totals = [jnp.sum(total, axis=0, keepdims=True) for total in scan_rows(count, soft, (start, start))]
        o = None
        for half in range(2):
            lse_ref[pl.ds(heads[half], 1), :] = tops[half] + jnp.log(totals[half])
            part = dot(vvt[half, heads[half] // 7], prob[half]) * (1.0 / totals[half])
            o = part if o is None else o + part
        obt_ref[lanes, :] = o.astype(BF)

        block_from(7 - i).wait_recv()
        hand_over(7 - i).start()

        @pl.when(i == 0)
        def _():
            go.relay()

        @pl.when(i == 5)
        def _():
            go.relay_corner()
            gd.relay()

        @pl.when(i == 6)
        def _():
            gd.relay_corner()

    for slot in (3, 5, 7, 1):
        go.wait(slot)
    for lo in range(0, 896, 128):
        mid_ref[:, lo : lo + 128] = t_dot(obt_ref[...], wo_all[:, :, lo : lo + 128].reshape(896, 128))

    def norm_two(at):
        m = mid_ref[at, :] + x_ref[at, :].astype(F32)
        mid_ref[at, :] = m
        scale = lax.rsqrt(jnp.mean(m * m, axis=-1, keepdims=True) + EPSILON)
        xn2_ref[at, :] = (m * scale * vec_ref[3:4, :]).astype(BF)

    tiles(rows, 32, norm_two)

    @pl.loop(1, 8)
    def _(r):
        block_to(r).wait_send()
        hand_over(r).wait_send()
        handed(r).wait_recv()

    for slot in (1, 3, 5, 7):
        gd.wait(slot)
    for each in (gkv, gs, gq, go, gk, gd):
        each.finish()


def front(x, pos, cosine, sine, wq, wk, wv, wo, n1, bq, bk, bv, n2, wg, wu, cot):
    dma = pltpu.SemaphoreType.DMA
    vm = pl.BlockSpec(memory_space=pltpu.VMEM)
    vmem = pltpu.VMEM
    out = jax.ShapeDtypeStruct
    rows, width = x.shape
    own = wq.shape[0]
    ff = -(-(wg.shape[1] // 8) // 128) * 128
    tokens = 4 * rows
    return pl.pallas_call(
        front_kernel,
        out_shape=(
            out((rows, width), BF), out((rows, width), BF), out((4, rows + 16, 256), BF),
            out((16, rows), F32), out((width, rows), BF), out((rows, width), F32),
            out((rows, width), BF), out((8, own, 256), BF), out((8, own, width), BF),
            out((8, own, width), BF), out((16, width), F32), out((8, own, 2 * ff), BF),
            out((8, rows, width), BF),
        ),
        in_specs=[vm] * 16,
        out_specs=(vm,) * 13,
        scratch_shapes=[
            vmem((own, 256), BF), vmem((16, width), F32), vmem((16, width), BF), vmem((8, 16, width), BF),
            vmem((8, own, 2 * ff), BF), vmem((2, 2, tokens, 128), BF), vmem((2, 2, 128, tokens), BF),
            vmem((2, tokens, rows), F32), vmem((2, tokens, rows), BF), vmem((tokens, rows), F32),
            dma((7,)), dma((8,)), dma((7,)), dma((8,)), dma((7,)), dma((8,)), dma((7,)), dma((8,)),
            dma((8,)), dma((8,)), dma((4,)), dma((4,)), dma((4,)), dma((7,)), dma((8,)), dma((8,)), dma((8,)),
        ],
        compiler_params=pltpu.CompilerParams(collective_id=2, has_side_effects=True),
    )(x, pos, cosine, sine, wq, wk, wv, wo, n1, bq, bk, bv, n2, wg, wu, cot)


def middle_kernel(
    xn2_ref, pos_ref, cos_ref, sin_ref, kv_ref, lse_ref, vec_ref,
    df_hbm, wgu_hbm, wd_hbm, x_hbm, cot_hbm, mid_hbm, xn_hbm, q_hbm, obt_hbm, wkv_hbm, wq_hbm, wo_hbm,
    out_ref, gin_ref, pair_q, pair_o, pair_k, in_u, pair_d,
    x_all, part_out, core_in, tree_in, dx, core_f, tree_f, gwgu, gwd, mate_d, pair_u, mate_u,
    core_o, tree_o, core_q, tree_q, core_k, tree_k,
    own_o, mate_o, own_q, mate_q, own_k, mate_k, dkv_in, *sems,
):
    place = plane()
    me = lax.axis_index("fsdp")
    z = lax.axis_index("ctx")
    rows, width = xn2_ref.shape
    own = width // 8
    ff, ff_own = wgu_hbm.shape[1] // 2, wd_hbm.shape[0]
    tokens, keys = 8 * rows, 4 * rows
    piece = gwd.shape[1]
    loads = sems[38]
    greet_all()
    line_sems = sems[18:24]
    ld = Line(gwd, pair_d, mate_d, line_sems, 0)
    lu = Line(gwgu, pair_u, mate_u, line_sems, 4)
    lo = Line(own_o, pair_o, mate_o, line_sems, 12)
    lq = Line(own_q, pair_q, mate_q, line_sems, 13)
    lk = Line(own_k, pair_k, mate_k, line_sems, 14)
    send_all, recv_all, send_kv, recv_kv = sems[24:28]

    def feed_forward(df_ref, wgu_ref, wd, act_all, hid_all, dgu_all, dh, part, folded):
        gx = Gather(place, xn2_ref, x_all, sems[0], sems[1])
        rd = Scatter(place, part, core_in, tree_in, folded, *sems[2:6])
        gx.start()
        fetch = [
            pltpu.make_async_copy(wgu_hbm, wgu_ref, loads.at[0]),
            pltpu.make_async_copy(wd_hbm, wd.at[pl.ds(0, ff_own)], loads.at[1]),
            pltpu.make_async_copy(df_hbm, df_ref, loads.at[2]),
        ]
        for cp in fetch:
            cp.start()
        x_all[0] = xn2_ref[...]
        wd[ff_own:] = jnp.zeros((ff - ff_own, width), BF)
        fetch[0].wait()
        fetch[1].wait()
        both = lambda ref, p: ref[pl.ds(2 * p, 2)].reshape(2 * rows, ref.shape[2])

        @pl.loop(0, 4)
        def _(p):
            @pl.when(p == 1)
            def _():
                gx.relay()

            @pl.when(p == 3)
            def _():
                gx.relay_corner()

            gx.wait(2 * p + 1)
            x = both(x_all, p)
            for n in range(0, 2 * ff, 256):
                act_all[p, :, n : n + 256] = dot(x, wgu_ref[:, n : n + 256])

            def activate(at):
                gate, up = act_all[p, at, :ff], act_all[p, at, ff:]
                sig = 0.5 * jnp.tanh(0.5 * gate) + 0.5
                hid_all[p, at, :] = (gate * sig * up).astype(BF)

            tiles(2 * rows, 16, activate)
            out = dot(hid_all[p], wd[...]).astype(BF)
            part_out[pl.ds(2 * p, 2)] = out.reshape(2, rows, width)

        fetch[2].wait()
        for p in range(4):
            gwd[p] = t_dot(
                hid_all[:, :, p * piece : (p + 1) * piece].reshape(tokens, piece),
                df_ref[...].reshape(tokens, width),
            ).astype(BF)
            ld.start(p)

        @pl.loop(0, 4)
        def _(k):
            p = 3 - k
            dh[...] = dot_t(both(df_ref, p), wd[...])

            def activate(at):
                gate, up, d = act_all[p, at, :ff], act_all[p, at, ff:], dh[at, :]
                sig = 0.5 * jnp.tanh(0.5 * gate) + 0.5
                dgu_all[p, at, :ff] = (d * up * (sig * (1.0 + gate * (1.0 - sig)))).astype(BF)
                dgu_all[p, at, ff:] = (d * (gate * sig)).astype(BF)

            tiles(2 * rows, 16, activate)
            value = dot_t(dgu_all[p], wgu_ref[...]).astype(BF)
            part[pl.ds(2 * p, 2)] = value.reshape(2, rows, width)
            rd.to_twin(p).start()

            @pl.when(k == 1)
            def _():
                rd.start_corner()

            @pl.when(k == 2)
            def _():
                ld.meet(0)

        rd.start_far()
        ld.meet(1)
        rd.relay()

        @pl.loop(0, 2 * ff // 256)
        def _(n):
            at = pl.ds(pl.multiple_of(n * 256, 256), 256)
            value = t_dot(x_all[...].reshape(tokens, width), dgu_all[:, :, at].reshape(tokens, 256))
            gwgu[:, :, at] = value.astype(BF).reshape(8, own, 256)

            @pl.when(n == 1)
            def _():
                ld.meet(2)

            @pl.when(n == 3)
            def _():
                ld.settle(0)

        for r in (7, 6, 5, 4):
            lu.start(peer(r))

        def store_dx(at, value):
            dx[at, :] = value

        rd.total(store_dx)
        gx.finish()
        rd.finish()

    pl.run_scoped(
        feed_forward,
        pltpu.VMEM((8, rows, width), BF), pltpu.VMEM((width, 2 * ff), BF), pltpu.VMEM((ff, width), BF),
        pltpu.VMEM((4, 2 * rows, 2 * ff), F32), pltpu.VMEM((4, 2 * rows, ff), BF),
        pltpu.VMEM((4, 2 * rows, 2 * ff), BF), pltpu.VMEM((2 * rows, ff), F32),
        pltpu.VMEM((8, rows, width), BF), pltpu.VMEM((3, rows, width), BF),
    )

    def attention_back(
        x_ref, cot_ref, mid_ref, xn_ref, q_ref, obt_ref, wkv_ref, wq_ref, wo_ref,
        dm, da, dob, kk, kkt, vv, kcol, score, dprob, prob, dscore, dk_acc, dv_acc,
        dq, dkv_own, dkv, dxn, small, part_o, fold_o, part_q, fold_q, part_k, fold_k, fold_f,
    ):
        ro = Scatter(place, part_o, core_o, tree_o, fold_o, *sems[6:10], by_owner=True)
        rq = Scatter(place, part_q, core_q, tree_q, fold_q, *sems[10:14], by_owner=True)
        rk = Scatter(place, part_k, core_k, tree_k, fold_k, *sems[14:18], by_owner=True)
        rf = Scatter(place, part_out, core_f, tree_f, fold_f, *sems[28:32])
        arrays = (
            (mid_hbm, mid_ref), (cot_hbm, cot_ref), (obt_hbm, obt_ref), (wo_hbm, wo_ref), (q_hbm, q_ref),
            (xn_hbm, xn_ref), (wq_hbm, wq_ref), (wkv_hbm, wkv_ref), (x_hbm, x_ref),
        )
        fetch = [pltpu.make_async_copy(src, dst, loads.at[3 + i]) for i, (src, dst) in enumerate(arrays)]
        for cp in fetch:
            cp.start()
        for k in (3, 2, 1, 0):
            rf.to_twin(k).start()
        ld.meet(3)
        fetch[0].wait()
        fetch[1].wait()

        small[...] = jnp.zeros_like(small)

        def norm_two(at):
            m, g = mid_ref[at, :], dx[at, :]
            scale = lax.rsqrt(jnp.mean(m * m, axis=-1, keepdims=True) + EPSILON)
            weighted = vec_ref[3:4, :] * g
            inner = jnp.mean(weighted * m, axis=-1, keepdims=True)
            d = cot_ref[at, :].astype(F32) + scale * weighted - m * (scale * scale * scale) * inner
            dm[at, :] = d
            da[at, :] = d.astype(BF)
            small[3:4, :] += jnp.sum(g * m * scale, axis=0, keepdims=True)

        tiles(rows, 32, norm_two)
        for i in range(2, 9):
            fetch[i].wait()

        @pl.loop(0, 7)
        def _(i):
            lanes = pl.ds(pl.multiple_of(i * 128, 128), 128)
            part_o[:, :, lanes] = dot(obt_ref[...], da[:, lanes]).astype(BF).reshape(8, own, 128)

        for k in (3, 2, 1, 0):
            ro.to_twin(k).start()
        dob[...] = dot_t(da[...], wo_ref[...].reshape(width, width)).astype(BF)
        for j in range(4):
            here = pl.ds(j * rows, rows)
            key, value = kv_ref[j, :rows, :128].astype(F32), kv_ref[j, :rows, 128:].astype(F32)
            halves(key, kk.at[:, :, here])
            halves(value, vv.at[:, :, here])
            halves_t(key, kkt, here)
        key_places(kv_ref, kcol)
        dk_acc[...] = jnp.zeros_like(dk_acc)
        dv_acc[...] = jnp.zeros_like(dv_acc)
        place_row = pos_ref[...].astype(F32)
        cosine, sine = cos_ref[...], -sin_ref[...]
        count = keys // 64

        def keep(total):
            def store(at, value):
                total[0, at, :] = value.astype(BF)

            return store

        def gather_to(r):
            owner = peer(r)
            return push(pair_u.at[owner], in_u.at[me], send_all.at[r], recv_all.at[me], {"fsdp": owner})

        def settle_u(r):
            lu.settle(peer(r))
            gather_to(r).start()

        ld.settle(1)

        @pl.loop(0, 7)
        def _(i):
            lanes = pl.ds(pl.multiple_of(i * 128, 128), 128)
            grad = None
            for half in range(2):
                head = 2 * i + half
                g = head // 7
                score[...] = dot_t(kk[half, g], q_ref[:, lanes])
                dprob[...] = dot_t(vv[half, g], dob[:, lanes])
                lse_row = lse_ref[pl.ds(head, 1), :]

                def find_delta(at, total):
                    s = jnp.where(kcol[at, :] <= place_row, score[at, :], NEGATIVE)
                    p = jnp.exp(s - lse_row)
                    score[at, :] = p
                    prob[at, :] = p.astype(BF)
                    return total + eights(p * dprob[at, :], jnp.add)

                delta = scan_rows(count, find_delta, jnp.zeros((8, rows), F32))
                delta = jnp.sum(delta, axis=0, keepdims=True)

                def find_score(at):
                    dscore[at, :] = (score[at, :] * (dprob[at, :] - delta)).astype(BF)

                tiles(keys, 64, find_score)
                dv_acc[half, g] += dot(prob[...], dob[:, lanes])
                dk_acc[half, g] += dot(dscore[...], q_ref[:, lanes])
                term = dot(kkt[half, g], dscore[...])
                grad = term if grad is None else grad + term
            dq[:, lanes] = turn(grad.T * 0.125, cosine, sine).astype(BF)

            @pl.when(i == 0)
            def _():
                ro.start()
                rf.start()
                ld.settle(2)

            @pl.when(i == 1)
            def _():
                lu.meet(peer(7))

            @pl.when(i == 2)
            def _():
                ld.settle(3)

            @pl.when(i == 3)
            def _():
                ro.relay()
                rf.relay()
                lu.meet(peer(6))

            @pl.when(i == 5)
            def _():
                lu.meet(peer(5))
                settle_u(7)
                ro.total(keep(own_o))

            @pl.when(i == 6)
            def _():
                lu.meet(peer(4))

        lane = lax.broadcasted_iota(jnp.int32, (64, 128), 1)

        def join(acc, at):
            first = jnp.where(lane < 64, acc[0, 0, at, :], acc[1, 1, at, :])
            second = jnp.where(lane < 64, acc[0, 1, at, :], acc[1, 0, at, :])
            return first + pltpu.roll(second, 64, 1)

        @pl.loop(0, 4)
        def _(j):
            for first in range(0, rows, 64):
                at = pl.ds(pl.multiple_of(j * rows + first, 64), 64)
                dkv_own[j, first : first + 64, :128] = join(dk_acc, at).astype(BF)
                dkv_own[j, first : first + 64, 128:] = join(dv_acc, at).astype(BF)

        def kv_to(d):
            other = (z + d) % 4
            return push(
                dkv_own.at[other], dkv_in.at[d - 1], send_kv.at[d - 1], recv_kv.at[d - 1], {"ctx": other}
            )

        for d in (2, 1, 3):
            kv_to(d).start()

        @pl.loop(4, 8)
        def _(i):
            lu.start(peer(7 - i))

        lo.start(0)
        settle_u(6)
        settle_u(5)

        def weight_grads(grads, part, n):
            for at in range(0, n, 128):
                value = t_dot(xn_ref[...], grads[:, at : at + 128]).astype(BF)
                part[:, :, at : at + 128] = value.reshape(8, own, 128)

        weight_grads(dq, part_q, width)
        for k in (3, 2, 1, 0):
            rq.to_twin(k).start()
        for at in range(0, width, 128):
            wq_rows = wq_ref[...].reshape(width, width)
            dxn[:, at : at + 128] = dot_t(dq[...], wq_rows[at : at + 128])
        rq.start()
        settle_u(4)

        def store_out(at, value):
            out_ref[at, :] = value + mid_ref[at, :]

        rf.total(store_out)
        for d in (1, 3, 2):
            kv_to(d).wait_recv()

        def sum_kv(at):
            value = dkv_own[z, at, :].astype(F32)
            for d in range(3):
                value = value + dkv_in[d, at, :].astype(F32)
            dkv[at, :128] = turn(value[:, :128], cos_ref[at, :], -sin_ref[at, :]).astype(BF)
            dkv[at, 128:] = value[:, 128:].astype(BF)

        tiles(rows, 32, sum_kv)
        weight_grads(dkv, part_k, 256)
        for at in range(0, width, 128):
            wkv_rows = wkv_ref[...].reshape(width, 256)
            dxn[:, at : at + 128] += dot_t(dkv[...], wkv_rows[at : at + 128])

        def norm_one(at):
            h, g = x_ref[at, :].astype(F32), dxn[at, :]
            scale = lax.rsqrt(jnp.mean(h * h, axis=-1, keepdims=True) + EPSILON)
            weighted = vec_ref[0:1, :] * g
            inner = jnp.mean(weighted * h, axis=-1, keepdims=True)
            gin_ref[at, :] = dm[at, :] + scale * weighted - h * (scale * scale * scale) * inner
            small[0:1, :] += jnp.sum(g * h * scale, axis=0, keepdims=True)
            small[1:2, :] += jnp.sum(dq[at, :].astype(F32), axis=0, keepdims=True)
            small[2:3, :256] += jnp.sum(dkv[at, :].astype(F32), axis=0, keepdims=True)

        tiles(rows, 32, norm_one)
        flat = small[...]
        line_of = lax.broadcasted_iota(jnp.int32, (16, 128), 0)
        for j in range(8):
            by_row = pltpu.roll(flat, (width - 112 * j) % width, 1)[:, :128]
            by_head = pltpu.roll(flat, (width - 16 * j) % width, 1)
            value = jnp.where(line_of == 2, by_head[:, :128], by_row)
            lifted = pltpu.roll(by_head[:, 128:256], 2, 0)
            value = jnp.where(line_of == 4, lifted, value)
            part_k[j, :16, 256:] = value.astype(BF)
            part_k[j, 16:, 256:] = jnp.zeros((own - 16, 128), BF)

        for k in (3, 2, 1, 0):
            rk.to_twin(k).start()
        lu.meet(peer(3))
        rk.start()
        rq.relay()
        lu.meet(peer(2))
        settle_u(3)
        rk.relay()
        rq.total(keep(own_q))
        lq.start(0)
        lu.meet(peer(1))
        rk.total(keep(own_k))
        lk.start(0)
        settle_u(2)
        lu.meet(me)
        settle_u(1)
        lo.meet(0)
        lu.settle(me)
        keep_own = pltpu.make_async_copy(pair_u.at[me], in_u.at[me], loads.at[12])
        keep_own.start()
        lq.meet(0)
        lo.settle(0)
        lk.meet(0)
        lq.settle(0)
        lk.settle(0)
        keep_own.wait()

        @pl.loop(1, 8)
        def _(r):
            other = peer(r)
            push(
                pair_u.at[me], in_u.at[other], send_all.at[r], recv_all.at[other], {"fsdp": other}
            ).wait_recv()
            gather_to(r).wait_send()

        for d in (1, 2, 3):
            kv_to(d).wait_send()
        for each in (ro, rq, rk, rf):
            each.finish()

    v = pltpu.VMEM
    pl.run_scoped(
        attention_back,
        v((rows, width), BF), v((rows, width), BF), v((rows, width), F32), v((rows, width), BF),
        v((rows, width), BF), v((width, rows), BF), v((8, own, 256), BF), v((8, own, width), BF),
        v((8, own, width), BF),
        v((rows, width), F32), v((rows, width), BF), v((rows, width), BF),
        v((2, 2, keys, 128), BF), v((2, 2, 128, keys), BF), v((2, 2, keys, 128), BF),
        v((keys, rows), F32), v((keys, rows), F32), v((keys, rows), F32),
        v((keys, rows), BF), v((keys, rows), BF),
        v((2, 2, keys, 128), F32), v((2, 2, keys, 128), F32),
        v((rows, width), BF), v((4, rows, 256), BF), v((rows, 256), BF), v((rows, width), F32),
        v((16, width), F32),
        v((8, own, width), BF), v((3, own, width), BF), v((8, own, width), BF), v((3, own, width), BF),
        v((8, own, 384), BF), v((3, own, 384), BF), v((3, rows, width), BF),
    )

    @pl.loop(0, 4)
    def _(p):
        ld.finish(p)

    @pl.loop(0, 8)
    def _(p):
        lu.finish(p)

    for each in (lo, lq, lk):
        each.finish(0)


def middle(xn2, pos, cosine, sine, kv, lse, vec, df_all, wgu, wd, x, cot, mid, xn, q, obt, wkv, wq, wo):
    dma = pltpu.SemaphoreType.DMA
    vm = pl.BlockSpec(memory_space=pltpu.VMEM)
    hbm = pl.BlockSpec(memory_space=pl.ANY)
    v = pltpu.VMEM
    out = jax.ShapeDtypeStruct
    rows, width = x.shape
    own = width // 8
    ff = wgu.shape[1] // 2
    gu, gd = (8, own, 2 * ff), (4, ff // 4, width)
    wide, narrow = (1, own, width), (1, own, 384)
    tree = [dma((4,)), dma((4,)), dma((3,)), dma((3,))]
    return pl.pallas_call(
        middle_kernel,
        out_shape=(
            out((rows, width), F32), out((rows, width), F32), out(wide, BF), out(wide, BF), out(narrow, BF),
            out(gu, BF), out(gd, BF),
        ),
        in_specs=[vm] * 7 + [hbm] * 12,
        out_specs=(vm, vm, vm, vm, vm, hbm, vm),
        scratch_shapes=[
            v((8, rows, width), BF), v((8, rows, width), BF), v((4, rows, width), BF), v((3, rows, width), BF),
            v((rows, width), F32), v((4, rows, width), BF), v((3, rows, width), BF),
            v(gu, BF), v(gd, BF), v(gd, BF), v(gu, BF), v(gu, BF),
            v((4, own, width), BF), v((3, own, width), BF), v((4, own, width), BF), v((3, own, width), BF),
            v((4, own, 384), BF), v((3, own, 384), BF),
            v(wide, BF), v(wide, BF), v(wide, BF), v(wide, BF), v(narrow, BF), v(narrow, BF),
            v((3, rows, 256), BF),
            dma((7,)), dma((8,)), *tree, *tree, *tree, *tree,
            *[dma((15,))] * 6,
            dma((8,)), dma((8,)), dma((3,)), dma((3,)), *tree,
            *[dma((1,))] * 6, dma((13,)),
        ],
        compiler_params=pltpu.CompilerParams(
            collective_id=0, has_side_effects=True, vmem_limit_bytes=67043328
        ),
    )(xn2, pos, cosine, sine, kv, lse, vec, df_all, wgu, wd, x, cot, mid, xn, q, obt, wkv, wq, wo)


def results_kernel(
    out_ref, gin_ref, tq_ref, to_ref, tk_ref, tu_ref, td_ref,
    o_ref, i_ref, n1_ref, q_ref, bq_ref, k_ref, bk_ref, v_ref, bv_ref, w_ref, n2_ref, g_ref, u_ref, d_ref,
):
    o_ref[...] = out_ref[...]
    i_ref[...] = gin_ref[...]
    q_ref[...] = tq_ref[0].astype(F32)
    w_ref[...] = to_ref[0].astype(F32)
    k_ref[...] = tk_ref[0, :, :128].astype(F32)
    v_ref[...] = tk_ref[0, :, 128:256].astype(F32)
    small = tk_ref[0, :16, 256:].astype(F32)
    for i, ref in enumerate((n1_ref, bq_ref, bk_ref, n2_ref, bv_ref)):
        ref[...] = small[i : i + 1, : ref.shape[1]]
    ff_own, ff = d_ref.shape[0], tu_ref.shape[2] // 2
    for j in range(8):
        def place_block(at):
            g_ref[at, j * ff_own : (j + 1) * ff_own] = tu_ref[j, at, :ff_own].astype(F32)
            u_ref[at, j * ff_own : (j + 1) * ff_own] = tu_ref[j, at, ff : ff + ff_own].astype(F32)

        tiles(tu_ref.shape[1], 16, place_block)
    rows = td_ref.shape[1]
    for p in range(4):
        count = min(rows, ff_own - p * rows)
        d_ref[p * rows : p * rows + count] = td_ref[p, :count].astype(F32)


def results(out, gin, tq, to, tk, tu, td, ff_own):
    vm = pl.BlockSpec(memory_space=pltpu.VMEM)
    rows, width = out.shape
    own = width // 8
    shapes = (
        (rows, width), (rows, width), (1, own), (own, 896), (1, own), (own, 128), (1, 16), (own, 128), (1, 16),
        (own, 896), (1, own), (own, 8 * ff_own), (own, 8 * ff_own), (ff_own, width),
    )
    return pl.pallas_call(
        results_kernel,
        out_shape=tuple(jax.ShapeDtypeStruct(shape, F32) for shape in shapes),
        in_specs=[vm] * 7,
        out_specs=(vm,) * 14,
    )(out, gin, tq, to, tk, tu, td)


def shards(
    inputs, positions, cotangent, norm_one, w_query, b_query, key_projection, b_key,
    value_projection, value_bias, w_out, norm_two, w_gate, w_up, w_down,
):
    places = positions[0]
    turned = angles_of(places)
    cosine, sine = jnp.cos(turned), jnp.sin(turned)
    sine = jnp.where(jnp.arange(128)[None, :] % 64 < 32, -sine, sine)
    own = w_query.shape[1]
    ff_own = w_down.shape[1]
    ff = -(-ff_own // 128) * 128
    x, cot = inputs[0], cotangent[0]
    xn, q, kv, lse, obt, mid, xn2, wkv, wq, wo, vec, wgu, df_all = front(
        x, positions, cosine, sine, w_query[0], key_projection[0], value_projection[0], w_out[0],
        norm_one, b_query, b_key, value_bias, norm_two, w_gate[0], w_up[0], cot,
    )
    totals = middle(
        xn2, positions, cosine, sine, kv, lse, vec, df_all, wgu.reshape(-1, 2 * ff), w_down[0],
        x, cot, mid, xn, q, obt, wkv, wq, wo,
    )
    matrix = lambda i: i in (0, 1, 3, 5, 7, 9, 11, 12, 13)
    return tuple(g[None] if matrix(i) else g for i, g in enumerate(results(*totals, ff_own)))


def angles_of(places):
    half = HEAD_SIZE // 2
    inverse = jnp.exp(jnp.arange(half, dtype=F32) * (-2.0 * math.log(ROPE_BASE) / HEAD_SIZE))
    return places.astype(F32)[:, None] * jnp.concatenate([inverse] * 4)[None, :]


def shards_general(
    inputs, positions, cotangent, norm_one, w_query, b_query, key_projection, b_key,
    value_projection, value_bias, w_out, norm_two, w_gate, w_up, w_down,
):
    rows = inputs.shape[1]
    width = inputs.shape[2]
    group = QUERY_HEADS // KEY_VALUE_HEADS
    q_cols = w_query.shape[2]
    kv_cols = key_projection.shape[2]
    score_scale = 1.0 / math.sqrt(HEAD_SIZE)

    places = positions[0]
    key_places = lax.all_gather(places, "ctx", axis=0, tiled=True)
    cosine, sine = angles(places)
    hidden = inputs[0].astype(F32)

    packed = jnp.concatenate([w_query[0], key_projection[0], value_projection[0], w_out[0]], axis=1)
    packed = lax.all_gather(packed, "fsdp", axis=0, tiled=True)
    w_qkv = packed[:, : q_cols + 2 * kv_cols]
    w_o = packed[:, q_cols + 2 * kv_cols :]
    small = jnp.concatenate([norm_one[0], b_query[0], b_key[0], value_bias[0], norm_two[0]])
    small = lax.all_gather(small, "fsdp", axis=0).astype(F32)
    cuts, at = [], 0
    for piece in (norm_one, b_query, b_key, value_bias, norm_two):
        n = piece.shape[1]
        cuts.append(small[:, at : at + n].reshape(-1))
        at += n
    gain_one, bias_q, bias_k, bias_v, gain_two = cuts
    bias = jnp.concatenate([bias_q, bias_k, bias_v])

    grad_branch = cotangent[0]
    df_all = lax.all_gather(grad_branch, "fsdp", axis=0, tiled=True)
    wg = lax.all_to_all(w_gate[0], "fsdp", split_axis=1, concat_axis=0, tiled=True)
    wu = lax.all_to_all(w_up[0], "fsdp", split_axis=1, concat_axis=0, tiled=True)
    wd = w_down[0]

    scale_one, normed = norm_rows(hidden, gain_one)
    qkv = dot(normed, w_qkv) + bias
    q = rotate(qkv[:, :q_cols].reshape(rows, QUERY_HEADS, HEAD_SIZE), cosine, sine).astype(BF)
    k = rotate(
        qkv[:, q_cols : q_cols + kv_cols].reshape(rows, KEY_VALUE_HEADS, HEAD_SIZE), cosine, sine
    ).astype(BF)
    v = qkv[:, q_cols + kv_cols :].astype(BF)
    kv = jnp.concatenate([k.reshape(rows, kv_cols), v], axis=1)
    kv = lax.all_gather(kv, "ctx", axis=0, tiled=True)
    total = kv.shape[0]
    k_all = kv[:, :kv_cols].reshape(total, KEY_VALUE_HEADS, HEAD_SIZE)
    v_all = kv[:, kv_cols:].reshape(total, KEY_VALUE_HEADS, HEAD_SIZE)
    q = q.reshape(rows, KEY_VALUE_HEADS, group, HEAD_SIZE)
    s = jnp.einsum("tgjd,ugd->gjtu", q, k_all, preferred_element_type=F32) * score_scale
    s = jnp.where(key_places[None, :] <= places[:, None], s, NEGATIVE)
    top = jnp.max(s, axis=-1, keepdims=True)
    lse = top + jnp.log(jnp.sum(jnp.exp(s - top), axis=-1, keepdims=True))
    pf = jnp.exp(s - lse)
    p = pf.astype(BF)
    o = jnp.einsum("gjtu,ugd->tgjd", p, v_all, preferred_element_type=F32)
    ob = o.reshape(rows, q_cols).astype(BF)
    middle = hidden + dot(ob, w_o)
    scale_two, normed_two = norm_rows(middle, gain_two)

    x_all = lax.all_gather(normed_two, "fsdp", axis=0, tiled=True)
    gate = dot(x_all, wg)
    up = dot(x_all, wu)
    sig = jax.nn.sigmoid(gate)
    hid = (gate * sig * up).astype(BF)
    out_part = dot(hid, wd).astype(BF)
    ffn_out = lax.psum_scatter(out_part, "fsdp", scatter_dimension=0, tiled=True)
    output = middle + ffn_out.astype(F32)

    dhid = dot_t(df_all, wd)
    dgate = (dhid * up * sig * (1.0 + gate * (1.0 - sig))).astype(BF)
    dup = (dhid * (gate * sig)).astype(BF)
    dx_part = (dot_t(dgate, wg) + dot_t(dup, wu)).astype(BF)
    dxn2 = lax.psum_scatter(dx_part, "fsdp", scatter_dimension=0, tiled=True).astype(F32)
    g_down = t_dot(hid, df_all)
    g_gate = t_dot(x_all, dgate)
    g_up = t_dot(x_all, dup)

    g_out = grad_branch.astype(F32)
    grad_gain_two, dmid = norm_back(middle, scale_two, gain_two, dxn2)
    dm = g_out + dmid
    da = dm.astype(BF)
    g_wo = t_dot(ob, da)
    dob = dot_t(da, w_o).astype(BF).reshape(rows, KEY_VALUE_HEADS, group, HEAD_SIZE)

    dp = jnp.einsum("tgjd,ugd->gjtu", dob, v_all, preferred_element_type=F32)
    delta = jnp.sum(pf * dp, axis=-1, keepdims=True)
    ds = (pf * (dp - delta)).astype(BF)
    dq = jnp.einsum("gjtu,ugd->tgjd", ds, k_all, preferred_element_type=F32) * score_scale
    dk = jnp.einsum("gjtu,tgjd->ugd", ds, q, preferred_element_type=F32) * score_scale
    dv = jnp.einsum("gjtu,tgjd->ugd", p, dob, preferred_element_type=F32)
    dkv = jnp.concatenate([dk.reshape(total, kv_cols), dv.reshape(total, kv_cols)], axis=1)
    dkv = lax.psum_scatter(dkv, "ctx", scatter_dimension=0, tiled=True)
    dq = rotate(dq.reshape(rows, QUERY_HEADS, HEAD_SIZE), cosine, -sine).astype(BF)
    dk = rotate(
        dkv[:, :kv_cols].reshape(rows, KEY_VALUE_HEADS, HEAD_SIZE), cosine, -sine
    ).astype(BF)
    dqkv = jnp.concatenate(
        [dq.reshape(rows, q_cols), dk.reshape(rows, kv_cols), dkv[:, kv_cols:].astype(BF)], axis=1
    )
    g_qkv = t_dot(normed, dqkv)
    g_bias = jnp.sum(dqkv.astype(F32), axis=0)
    dxn = dot_t(dqkv, w_qkv)
    grad_gain_one, dhidden = norm_back(hidden, scale_one, gain_one, dxn)
    grad_in = dm + dhidden

    g_attn = jnp.concatenate([g_qkv, g_wo], axis=1).astype(BF)
    g_attn = lax.psum_scatter(g_attn, "fsdp", scatter_dimension=0, tiled=True)
    back = [
        lax.all_to_all(g.astype(BF), "fsdp", split_axis=0, concat_axis=1, tiled=True)
        for g in (g_gate, g_up)
    ]
    g_attn, g_gate, g_up, g_down = lax.psum((g_attn, back[0], back[1], g_down.astype(BF)), "ctx")
    pieces = jnp.concatenate(
        [
            g.reshape(small.shape[0], -1)
            for g in (
                grad_gain_one, g_bias[:q_cols], g_bias[q_cols : q_cols + kv_cols],
                g_bias[q_cols + kv_cols :], grad_gain_two,
            )
        ],
        axis=1,
    )
    pieces = lax.psum(pieces, ("ctx", "fsdp"))
    mine = lax.dynamic_slice_in_dim(pieces, lax.axis_index("fsdp"), 1, axis=0)
    outs, at = [], 0
    for piece in (norm_one, b_query, b_key, value_bias, norm_two):
        n = piece.shape[1]
        outs.append(mine[:, at : at + n])
        at += n
    g_n1, g_bq, g_bk, g_bv, g_n2 = outs
    g_attn = g_attn.astype(F32)
    return (
        output[None], grad_in[None], g_n1,
        g_attn[None, :, :q_cols], g_bq,
        g_attn[None, :, q_cols : q_cols + kv_cols], g_bk,
        g_attn[None, :, q_cols + kv_cols : q_cols + 2 * kv_cols], g_bv,
        g_attn[None, :, q_cols + 2 * kv_cols :], g_n2,
        g_gate.astype(F32)[None], g_up.astype(F32)[None], g_down.astype(F32)[None],
    )


def solution(mesh):
    tok, row, vec = P("fsdp", "ctx", None), P(None, "fsdp", None), P(None, "fsdp")
    fast = mesh.shape["ctx"] == 4 and mesh.shape["fsdp"] == 8
    return jax.shard_map(
        shards if fast else shards_general,
        mesh=mesh,
        in_specs=(
            tok, P("fsdp", "ctx"), tok, vec, row, vec, row, vec, row, vec, row, vec, row, row, row,
        ),
        out_specs=(tok, tok, vec, row, vec, row, vec, row, vec, row, vec, row, row, row),
        check_vma=False,
    )
```
